512 devices in a mesh: gx: 16 (over y, core), gy: 4 (over z_lo), gz: 8 (over z_hi, x).
Axes of the slice: x: 4, y: 8, z: 8 (z_hi: 2, z_lo: 4; z = z_hi * 4 + z_lo), core: 2. Of those that a mesh axis runs over, the one named last changes fastest.
Arguments:
- positions: float32 [3, 16, 32, 8, 128], P(None, 'gx', ('gy', 'gz')), may hold values from 0 to 3
- velocities: float32 [3, 16, 32, 8, 128], P(None, 'gx', ('gy', 'gz')), may hold values from -6 to 6
- bead_keys: int32 [16, 32, 8, 128], P('gx', ('gy', 'gz')), may hold values from 0 to 1073741823
- counts: int32 [16, 32, 8], P('gx', ('gy', 'gz')), may hold values from 64 to 128
Outputs:
- half_kick: float32 [3, 16, 32, 8, 128], P(None, 'gx', 'gy', 'gz')
The draws below stay inside these ranges and needn't reach their ends.
Inputs may be any that keep to these rules, and one draw needn't show every extreme that they name: Slots from counts of a tile on are padding and take no part. `bead_keys`: the lowest bit of a key names the bead type, 0 water and 1 polymer.
All inputs are finite; a program needn't handle non-finite values.
Results may differ from the reference program's by a relative error of at most 0.0003.
Values sent between devices are 32-bit elements; how exact they have to be, the bound alone decides.
A program may use at most 64 MiB of HBM per device.

```python
import jax
import jax.numpy as jnp
from jax import lax

SLOTS = 128
SIDE = 3
NTX = 16
NTY = 32
NTZ = 8


def place_ends(values, own_key, smallest, top_value):
    index_at = [jax.random.randint(jax.random.fold_in(own_key, axis), (), 0, length) for axis, length in enumerate(values.shape)]
    main_axis = values.shape.index(max(values.shape))
    next_to = index_at[:main_axis] + [(index_at[main_axis] + 1) % values.shape[main_axis]] + index_at[main_axis + 1:]
    return values.at[tuple(index_at)].set(smallest).at[tuple(next_to)].set(top_value)


def levels(stream_key, shape, split, low, largest):
    def one(axis_at, blocks):
        heights = jax.random.uniform(jax.random.fold_in(jax.random.fold_in(stream_key, 6), axis_at), (blocks,), jnp.float32, low / len(split), largest / len(split))
        return jnp.repeat(jnp.exp(heights), shape[axis_at] // blocks).reshape((-1,) + (1,) * (len(shape) - axis_at - 1))

    factor_of = one(*split[0])
    for cut in split[1:]:
        factor_of = factor_of * one(*cut)
    return factor_of


def bell_draw(rng, extent, width, reach, split=(), kind=jnp.bfloat16):
    result = jax.random.normal(rng, extent, jnp.float32) * width
    if len(split) > 0:
        result = levels(rng, extent, split, -0.22, 0.18) * result
    return jnp.clip(result, min=-reach, max=reach).astype(kind)


def setup_inputs(seed: int = 0) -> dict:
    streams_of = jax.random.split(jax.random.key(seed), 5)
    return {
        "positions": jnp.clip(3.0 * jax.random.uniform(streams_of[0], (3, NTX, NTY, NTZ, SLOTS), jnp.float32) ** levels(streams_of[0], (3, NTX, NTY, NTZ, SLOTS), ((1, 16), (2, 32)), -0.2, 0.2), 0.0, 3.0),
        "velocities": bell_draw(streams_of[1], (3, NTX, NTY, NTZ, SLOTS), 1.0, 6.0, ((1, 16), (2, 32)), jnp.float32),
        "bead_keys": place_ends(jax.random.randint(streams_of[2], (NTX, NTY, NTZ, SLOTS), 0, 1073741824), jax.random.fold_in(streams_of[2], 1), 0, 1073741823).astype(jnp.int32),
        "counts": place_ends(jax.random.randint(streams_of[3], (NTX, NTY, NTZ), SLOTS // 2, SLOTS + 1), jax.random.fold_in(streams_of[3], 1), SLOTS // 2, SLOTS).astype(jnp.int32),
    }


soft_radius = 0.05
friction = 4.5
noise_amplitude = 15.0
like_repulsion = 25.0
unlike_extra = 15.0
kick_scale = 0.02
root_twelve = 3.4641016151377544

def pair_noise(first_keys, second_keys):
    hashed = (first_keys ^ second_keys) * 1103515245 + (first_keys + second_keys) * 12345
    hashed = hashed ^ hashed >> 15 & 131071
    hashed = hashed * 747796405
    hashed = hashed ^ hashed >> 13 & 524287
    fraction = (hashed >> 7 & 16777215).astype(jnp.float32) * (1.0 / 16777216.0)
    return root_twelve * (fraction - 0.5)

def pair_forces(own_motion, own_keys, other_motion, other_keys, other_counts, displace):
    slot_index = lax.broadcasted_iota(jnp.int32, other_keys.shape, 1)
    present = (slot_index < other_counts[:, None]).astype(jnp.float32)
    separation = [own_motion[component][:, :, None] - (other_motion[component][:, None, :] + displace[component]) for component in range(3)]
    squared = separation[0] * separation[0] + separation[1] * separation[1] + separation[2] * separation[2]
    distance = jnp.sqrt(squared)
    weight = jnp.maximum(1.0 - distance, 0.0) * present[:, None, :]
    inverse = 1.0 / jnp.maximum(distance, soft_radius)
    approach = separation[0] * (own_motion[3][:, :, None] - other_motion[3][:, None, :])
    approach = approach + separation[1] * (own_motion[4][:, :, None] - other_motion[4][:, None, :])
    approach = approach + separation[2] * (own_motion[5][:, :, None] - other_motion[5][:, None, :])
    approach = approach * inverse
    first_keys = own_keys[:, :, None]
    second_keys = other_keys[:, None, :]
    random_pair = pair_noise(first_keys, second_keys)
    repulsion = like_repulsion + unlike_extra * ((first_keys ^ second_keys) & 1).astype(jnp.float32)
    strength = (repulsion * weight - friction * weight * weight * approach + noise_amplitude * weight * random_pair) * inverse
    return jnp.stack([lax.optimization_barrier(jnp.sum(strength * part, axis=2)) for part in separation])

def reference(positions, velocities, bead_keys, counts):
    motion = jnp.concatenate([positions, velocities], axis=0)
    size_x, size_y, size_z, slots = bead_keys.shape
    plane = size_y * size_z
    own_motion = jnp.moveaxis(motion, 1, 0).reshape(size_x, 6, plane, slots)
    own_keys = bead_keys.reshape(size_x, plane, slots)
    summed = jnp.zeros((size_x, 3, plane, slots), jnp.float32)
    for off_x in range(3):
        for off_y in range(3):
            for off_z in range(3):
                moved = (1 - off_x, 1 - off_y, 1 - off_z)
                other_motion = jnp.moveaxis(jnp.roll(motion, moved, axis=(1, 2, 3)), 1, 0).reshape(size_x, 6, plane, slots)
                other_keys = jnp.roll(bead_keys, moved, axis=(0, 1, 2)).reshape(size_x, plane, slots)
                other_counts = jnp.roll(counts, moved, axis=(0, 1, 2)).reshape(size_x, plane)
                displace = jnp.array([SIDE * (off_x - 1), SIDE * (off_y - 1), SIDE * (off_z - 1)], jnp.float32)

                def one_plane(items, displace=displace):
                    return pair_forces(items[0], items[1], items[2], items[3], items[4], displace)
                summed = summed + lax.map(one_plane, (own_motion, own_keys, other_motion, other_keys, other_counts))
    slot_index = lax.broadcasted_iota(jnp.int32, bead_keys.shape, 3)
    occupied = (slot_index < counts[:, :, :, None]).astype(jnp.float32)
    force = jnp.moveaxis(summed, 1, 0).reshape(3, size_x, size_y, size_z, slots)
    return kick_scale * force * occupied[None]
```

```python
import functools

import jax
import jax.numpy as jnp
from jax import lax
from jax.experimental import pallas as pl
from jax.experimental.pallas import tpu as pltpu
from jax.sharding import PartitionSpec as P

MESH = pl.DeviceIdType.MESH
SIDE = 3.0
SLOTS = 128
FAR = 4096.0
HALF = 64

soft_radius = 0.05
friction = 4.5
noise_amplitude = 15.0
like_repulsion = 25.0
unlike_extra = 15.0
kick_scale = 0.02
root_twelve = 3.4641016151377544


def take(values, index):
    return jnp.take_along_axis(values, index, axis=1, mode="promise_in_bounds")


def cell_of(part):
    return jnp.where(part >= 2.0, 2, jnp.where(part >= 1.0, 1, 0))


def exchange_kernel(
    groups, pos_ref, vel_ref, key_ref, count_ref, tiles_ref, order_ref,
    stage, ranks, local_sem, send_sem, recv_sem, rank_send, rank_recv,
):
    n_x, n_y, n_z = groups
    gx, gy, gz = lax.axis_index("gx"), lax.axis_index("gy"), lax.axis_index("gz")
    first, last = gz == 0, gz == n_z - 1
    above, below = lax.rem(gy + 1, n_y), lax.rem(gy + n_y - 1, n_y)
    columns = [lax.rem(gx + n_x + dx, n_x) for dx in (-1, 0, 1)]
    peers = [lax.rem(gz + k, n_z) for k in (4, 5, 3, 6, 2, 7, 1)]

    barrier = pltpu.get_barrier_semaphore()

    def ready(x, y, z):
        pl.semaphore_signal(
            barrier, inc=1, device_id={"gx": x, "gy": y, "gz": z}, device_id_type=MESH
        )

    for x in columns:
        for z in peers:
            ready(x, gy, z)
        ready(x, below, jnp.int32(n_z - 1))
        ready(x, above, jnp.int32(0))
    ready(columns[0], gy, gz)
    ready(columns[2], gy, gz)

    lane = lax.broadcasted_iota(jnp.int32, (n_z, SLOTS), 1)
    row = lax.broadcasted_iota(jnp.int32, (n_z, SLOTS), 0)
    occupancy = jnp.zeros((n_z, SLOTS), jnp.int32)
    for z in range(n_z):
        occupancy = jnp.where(row == z, count_ref[z], occupancy)
    px, py, pz = pos_ref[0], pos_ref[1], pos_ref[2]
    cell = cell_of(px) * 9 + cell_of(py) * 3 + cell_of(pz)
    cell = jnp.where(lane < occupancy, cell, 27)
    order = cell * SLOTS + lane
    rank = jnp.zeros((n_z, SLOTS), jnp.int32)
    for m in range(SLOTS):
        rank = rank + jnp.where(order[:, m : m + 1] < order, 1, 0)
    source = jnp.zeros((n_z, SLOTS), jnp.int32)
    for m in range(SLOTS):
        source = jnp.where(rank[:, m : m + 1] == lane, m, source)
    real = lane < occupancy
    key = key_ref[...]
    fields = [
        jnp.where(real, take(px, source), FAR),
        take(py, source),
        take(pz, source),
        take(vel_ref[0], source),
        take(vel_ref[1], source),
        take(vel_ref[2], source),
        take(lax.shift_right_logical(key, 15).astype(jnp.float32), source),
        take((key & 32767).astype(jnp.float32), source),
    ]
    for f, field in enumerate(fields):
        stage[pl.ds(8 + f, n_z, stride=8), :] = field
        stage[pl.ds(f, 1), :] = field[n_z - 1 : n_z]
        stage[pl.ds(8 * (n_z + 1) + f, 1), :] = field[0:1]
    masked = jnp.where(lane < occupancy, rank, rank + SLOTS)
    for z in range(n_z):
        ranks[z] = masked[z : z + 1]

    edge = jnp.logical_or(first, last)
    pl.semaphore_wait(barrier, jnp.where(edge, 6 * n_z - 1, 3 * n_z - 1))

    def block(z):
        return stage.at[pl.ds(pl.multiple_of(8 * z, 8), 24), :]

    def send(x, y, z, slot, sem=0):
        pltpu.make_async_remote_copy(
            src_ref=block(z),
            dst_ref=tiles_ref.at[slot],
            send_sem=send_sem.at[sem],
            recv_sem=recv_sem.at[0],
            device_id={"gx": x, "gy": y, "gz": z},
            device_id_type=MESH,
        ).start()

    def slot_of(dx, row_at):
        return (1 - dx) * (n_z + 2) + row_at

    @pl.when(first)
    def _():
        for z in [gz] + peers:
            for dx in (-1, 0, 1):
                send(columns[dx + 1], below, z, slot_of(dx, n_z + 1), 1)

    @pl.when(last)
    def _():
        for z in [gz] + peers:
            for dx in (-1, 0, 1):
                send(columns[dx + 1], above, z, slot_of(dx, 0), 1)

    for z in peers:
        for dx in (-1, 0, 1):
            send(columns[dx + 1], gy, z, slot_of(dx, gz + 1))
    for dx in (-1, 1):
        send(columns[dx + 1], gy, gz, slot_of(dx, gz + 1))
    for z in peers:
        pltpu.make_async_remote_copy(
            src_ref=ranks.at[z],
            dst_ref=order_ref.at[gz],
            send_sem=rank_send.at[0],
            recv_sem=rank_recv.at[0],
            device_id={"gx": gx, "gy": gy, "gz": z},
            device_id_type=MESH,
        ).start()
    own = pltpu.make_async_copy(block(gz), tiles_ref.at[slot_of(0, gz + 1)], local_sem.at[0])
    own_rank = pltpu.make_async_copy(ranks.at[gz], order_ref.at[gz], local_sem.at[1])
    own.start()
    own_rank.start()
    own.wait()
    own_rank.wait()

    def bulk(count, sem=0):
        part = tiles_ref.at[pl.ds(0, count)]
        return pltpu.make_async_remote_copy(
            src_ref=part, dst_ref=part, send_sem=send_sem.at[sem], recv_sem=recv_sem.at[0],
            device_id={"gx": gx, "gy": gy, "gz": peers[0]}, device_id_type=MESH,
        )

    def bulk_rank(count):
        part = order_ref.at[pl.ds(0, count)]
        return pltpu.make_async_remote_copy(
            src_ref=part, dst_ref=part, send_sem=rank_send.at[0], recv_sem=rank_recv.at[0],
            device_id={"gx": gx, "gy": gy, "gz": peers[0]}, device_id_type=MESH,
        )

    bulk(3 * (n_z + 2) - 1).wait_recv()
    bulk_rank(n_z - 1).wait_recv()
    bulk_rank(n_z - 1).wait_send()

    @pl.when(edge)
    def _():
        bulk(3 * n_z, 1).wait_send()

    bulk(3 * n_z - 1).wait_send()


def exchange(groups, positions, velocities, keys, counts):
    n_z = groups[2]
    vmem = pl.BlockSpec(memory_space=pltpu.VMEM)
    return pl.pallas_call(
        functools.partial(exchange_kernel, groups),
        out_shape=[
            jax.ShapeDtypeStruct((3 * (n_z + 2), 24, SLOTS), jnp.float32),
            jax.ShapeDtypeStruct((n_z, 1, SLOTS), jnp.int32),
        ],
        in_specs=[vmem, vmem, vmem, pl.BlockSpec(memory_space=pltpu.SMEM)],
        out_specs=[pl.BlockSpec(memory_space=pl.ANY)] * 2,
        scratch_shapes=[
            pltpu.VMEM((8 * (n_z + 2), SLOTS), jnp.float32),
            pltpu.VMEM((n_z, 1, SLOTS), jnp.int32),
            pltpu.SemaphoreType.DMA((2,)),
            pltpu.SemaphoreType.DMA((2,)),
            pltpu.SemaphoreType.DMA((1,)),
            pltpu.SemaphoreType.DMA((1,)),
            pltpu.SemaphoreType.DMA((1,)),
        ],
        compiler_params=pltpu.CompilerParams(collective_id=0, has_side_effects=True),
        name="sort_exchange",
    )(positions, velocities, keys, counts)


def runs_of(offset):
    spans = [{-1: (2, 3), 0: (0, 3), 1: (0, 1)}[o] for o in offset]
    runs = []
    for a in range(*spans[0]):
        for b in range(*spans[1]):
            low, high = a * 9 + b * 3 + spans[2][0], a * 9 + b * 3 + spans[2][1]
            if runs and runs[-1][1] == low:
                runs[-1] = (runs[-1][0], high)
            else:
                runs.append((low, high))
    return runs


def force_kernel(rows, tiles_ref, order_ref, out_ref):
    lane = lax.broadcasted_iota(jnp.int32, (rows, SLOTS), 1)
    left_half = lane < HALF
    position = lane & (HALF - 1)

    def load(offset, f):
        ox, oy, oz = offset
        start = (((1 + ox) * (rows + 2) + 1 + oy) * 3 + 1 + oz) * 8 + f
        return tiles_ref[pl.ds(start, rows, stride=24), :]

    def join(high, low):
        return high.astype(jnp.int32) * 32768 + low.astype(jnp.int32)

    home = (0, 0, 0)
    own = [load(home, f) for f in range(6)]
    own_key = join(load(home, 6), load(home, 7))

    def pair(other, other_key, summed):
        sep = [own[c] - other[c] for c in range(3)]
        squared = sep[0] * sep[0] + sep[1] * sep[1] + sep[2] * sep[2]
        root = lax.rsqrt(jnp.maximum(squared, 1e-30))
        distance = squared * root
        inverse = jnp.minimum(root, 1.0 / soft_radius)
        weight = jnp.maximum(1.0 - distance, 0.0) * inverse
        along = sep[0] * (own[3] - other[3])
        along = along + sep[1] * (own[4] - other[4])
        along = along + sep[2] * (own[5] - other[5])
        mixed = own_key ^ other_key
        hashed = mixed * 1103515245 + (own_key + other_key) * 12345
        hashed = hashed ^ lax.shift_right_logical(hashed, 15)
        hashed = hashed * 747796405
        hashed = hashed ^ lax.shift_right_logical(hashed, 13)
        fraction = lax.shift_right_logical(hashed << 1, 8).astype(jnp.float32)
        scale = noise_amplitude * root_twelve / 16777216.0
        base = like_repulsion - 0.5 * noise_amplitude * root_twelve
        level = jnp.where((mixed & 1) == 0, base, base + unlike_extra)
        strength = weight * (fraction * scale + level - friction * (weight * along))
        return tuple(summed[c] + strength * sep[c] for c in range(3))

    zero = jnp.zeros((rows, SLOTS), jnp.float32)
    summed = (zero, zero, zero)

    def count_cells(cells, low, high):
        inside = jnp.logical_and(cells >= low, cells < high)
        return jnp.sum(jnp.where(inside, 1.0, 0.0), axis=1, keepdims=True).astype(jnp.int32)

    def cells_of(x, y, z):
        cells = cell_of(x) * 9 + cell_of(y) * 3 + cell_of(z)
        return jnp.where(x > 0.5 * FAR, 27, cells)

    def group(axis, summed):
        sides = []
        longest = None
        for side in (-1, 1):
            tiles = []
            ranges = [(0,)] * axis + [(side,)] + [(-1, 0, 1)] * (2 - axis)
            total = jnp.zeros((rows, 1), jnp.int32)
            for ox in ranges[0]:
                for oy in ranges[1]:
                    for oz in ranges[2]:
                        offset = (ox, oy, oz)
                        cells = cells_of(*(load(offset, f) for f in range(3)))
                        table = []
                        for low, high in runs_of(offset):
                            begin = count_cells(cells, 0, low) if low else jnp.zeros_like(total)
                            length = count_cells(cells, low, high)
                            table.append((total, begin - total))
                            total = total + length
                        tiles.append((offset, table))
            sides.append((tiles, total))
            peak = jnp.max(total)
            longest = peak if longest is None else jnp.maximum(longest, peak)
        side_at = jnp.where(own[axis] < 1.5, 0, HALF)

        def one_pass(p, summed):
            at = position + p * HALF
            packed = [jnp.full((rows, SLOTS), FAR, jnp.float32)] + [zero] * 7
            for half, (tiles, total) in enumerate(sides):
                mine = left_half if half == 0 else jnp.logical_not(left_half)
                alive = jnp.logical_and(mine, at < total)
                for offset, table in tiles:
                    index = at
                    for base, shift in table:
                        index = jnp.where(at >= base, at + shift, index)
                    index = index & (SLOTS - 1)
                    taken = jnp.logical_and(alive, at >= table[0][0])
                    for f in range(8):
                        value = load(offset, f)
                        if f < 3 and offset[f]:
                            value = value + SIDE * offset[f]
                        packed[f] = jnp.where(taken, take(value, index), packed[f])
            packed_key = join(packed[6], packed[7])

            def some_steps(s, summed):
                for u in range(4):
                    index = side_at + (s * 4 + u)
                    other = [take(packed[f], index) for f in range(6)]
                    summed = pair(other, take(packed_key, index), summed)
                return summed

            steps = jnp.minimum(longest - p * HALF, HALF)
            return lax.fori_loop(0, (steps + 3) // 4, some_steps, summed)

        return lax.fori_loop(0, (longest + HALF - 1) // HALF, one_pass, summed)

    occupied = own[0] < 0.5 * FAR
    count = jnp.max(jnp.sum(jnp.where(occupied, 1.0, 0.0), axis=1, keepdims=True)).astype(jnp.int32)

    def own_steps(s, summed):
        for u in range(4):
            index = jnp.zeros_like(lane) + (s * 4 + u)
            other = [take(own[f], index) for f in range(6)]
            summed = pair(other, take(own_key, index), summed)
        return summed

    summed = lax.fori_loop(0, (count + 3) // 4, own_steps, summed)
    for axis in range(3):
        summed = group(axis, summed)

    order = order_ref[:, 0, :]
    scale = jnp.where(order < SLOTS, kick_scale, 0.0)
    order = order & (SLOTS - 1)
    for c in range(3):
        out_ref[c] = scale * take(summed[c], order)


def forces(n_z, tiles, order):
    vmem = pl.BlockSpec(memory_space=pltpu.VMEM)
    return pl.pallas_call(
        functools.partial(force_kernel, n_z),
        out_shape=jax.ShapeDtypeStruct((3, n_z, SLOTS), jnp.float32),
        in_specs=[vmem, vmem],
        out_specs=vmem,
        name="pair_forces",
    )(tiles, order)


def solution(mesh):
    groups = tuple(mesh.shape[a] for a in ("gx", "gy", "gz"))
    n_z = groups[2]

    def on_device(positions, velocities, bead_keys, counts):
        tiles, order = exchange(
            groups,
            positions.reshape(3, n_z, SLOTS),
            velocities.reshape(3, n_z, SLOTS),
            bead_keys.reshape(n_z, SLOTS),
            counts.reshape(n_z),
        )
        kick = forces(n_z, tiles.reshape(-1, SLOTS), order)
        return kick.reshape(3, 1, n_z, 1, SLOTS)

    in_specs = (
        P(None, "gx", ("gy", "gz"), None, None),
        P(None, "gx", ("gy", "gz"), None, None),
        P("gx", ("gy", "gz"), None, None),
        P("gx", ("gy", "gz"), None),
    )
    out_specs = P(None, "gx", "gy", "gz", None)
    return jax.shard_map(
        on_device, mesh=mesh, in_specs=in_specs, out_specs=out_specs, check_vma=False
    )
```

```python
import functools

import jax
import jax.numpy as jnp
from jax import lax
from jax.experimental import pallas as pl
from jax.experimental.pallas import tpu as pltpu
from jax.sharding import PartitionSpec as P

MESH = pl.DeviceIdType.MESH
SIDE = 3.0
SLOTS = 128
FAR = 4096.0
HALF = 64

soft_radius = 0.05
friction = 4.5
noise_amplitude = 15.0
like_repulsion = 25.0
unlike_extra = 15.0
kick_scale = 0.02
root_twelve = 3.4641016151377544


def take(values, index):
    return jnp.take_along_axis(values, index, axis=1, mode="promise_in_bounds")


def cell_of(part):
    return jnp.where(part >= 2.0, 2, jnp.where(part >= 1.0, 1, 0))


def exchange_kernel(
    groups, pos_ref, vel_ref, key_ref, count_ref, tiles_ref, order_ref,
    stage, ranks, local_sem, send_sem, recv_sem, rank_send, rank_recv,
):
    n_x, n_y, n_z = groups
    gx, gy, gz = lax.axis_index("gx"), lax.axis_index("gy"), lax.axis_index("gz")
    first, last = gz == 0, gz == n_z - 1
    above, below = lax.rem(gy + 1, n_y), lax.rem(gy + n_y - 1, n_y)
    columns = [lax.rem(gx + n_x + dx, n_x) for dx in (-1, 0, 1)]
    peers = [lax.rem(gz + k, n_z) for k in (4, 5, 3, 6, 2, 7, 1)]

    barrier = pltpu.get_barrier_semaphore()

    def ready(x, y, z):
        pl.semaphore_signal(
            barrier, inc=1, device_id={"gx": x, "gy": y, "gz": z}, device_id_type=MESH
        )

    for x in columns:
        for z in peers:
            ready(x, gy, z)
        ready(x, below, jnp.int32(n_z - 1))
        ready(x, above, jnp.int32(0))
    ready(columns[0], gy, gz)
    ready(columns[2], gy, gz)

    lane = lax.broadcasted_iota(jnp.int32, (n_z, SLOTS), 1)
    row = lax.broadcasted_iota(jnp.int32, (n_z, SLOTS), 0)
    occupancy = jnp.zeros((n_z, SLOTS), jnp.int32)
    for z in range(n_z):
        occupancy = jnp.where(row == z, count_ref[z], occupancy)
    px, py, pz = pos_ref[0], pos_ref[1], pos_ref[2]
    cell = cell_of(px) * 9 + cell_of(py) * 3 + cell_of(pz)
    cell = jnp.where(lane < occupancy, cell, 27)
    order = cell * SLOTS + lane
    rank = jnp.zeros((n_z, SLOTS), jnp.int32)
    for m in range(SLOTS):
        rank = rank + jnp.where(order[:, m : m + 1] < order, 1, 0)
    source = jnp.zeros((n_z, SLOTS), jnp.int32)
    for m in range(SLOTS):
        source = jnp.where(rank[:, m : m + 1] == lane, m, source)
    real = lane < occupancy
    key = key_ref[...]
    fields = [
        jnp.where(real, take(px, source), FAR),
        take(py, source),
        take(pz, source),
        take(vel_ref[0], source),
        take(vel_ref[1], source),
        take(vel_ref[2], source),
        take(lax.shift_right_logical(key, 15).astype(jnp.float32), source),
        take((key & 32767).astype(jnp.float32), source),
    ]
    for f, field in enumerate(fields):
        stage[pl.ds(8 + f, n_z, stride=8), :] = field
        stage[pl.ds(f, 1), :] = field[n_z - 1 : n_z]
        stage[pl.ds(8 * (n_z + 1) + f, 1), :] = field[0:1]
    masked = jnp.where(lane < occupancy, rank, rank + SLOTS)
    for z in range(n_z):
        ranks[z] = masked[z : z + 1]

    edge = jnp.logical_or(first, last)
    pl.semaphore_wait(barrier, jnp.where(edge, 6 * n_z - 1, 3 * n_z - 1))

    def block(z):
        return stage.at[pl.ds(pl.multiple_of(8 * z, 8), 24), :]

    def send(x, y, z, slot, sem=0):
        pltpu.make_async_remote_copy(
            src_ref=block(z),
            dst_ref=tiles_ref.at[slot],
            send_sem=send_sem.at[sem],
            recv_sem=recv_sem.at[0],
            device_id={"gx": x, "gy": y, "gz": z},
            device_id_type=MESH,
        ).start()

    def slot_of(dx, row_at):
        return (1 - dx) * (n_z + 2) + row_at

    @pl.when(first)
    def _():
        for z in [gz] + peers:
            for dx in (-1, 0, 1):
                send(columns[dx + 1], below, z, slot_of(dx, n_z + 1), 1)

    @pl.when(last)
    def _():
        for z in [gz] + peers:
            for dx in (-1, 0, 1):
                send(columns[dx + 1], above, z, slot_of(dx, 0), 1)

    for z in peers:
        for dx in (-1, 0, 1):
            send(columns[dx + 1], gy, z, slot_of(dx, gz + 1))
    for dx in (-1, 1):
        send(columns[dx + 1], gy, gz, slot_of(dx, gz + 1))
    for z in peers:
        pltpu.make_async_remote_copy(
            src_ref=ranks.at[z],
            dst_ref=order_ref.at[gz],
            send_sem=rank_send.at[0],
            recv_sem=rank_recv.at[0],
            device_id={"gx": gx, "gy": gy, "gz": z},
            device_id_type=MESH,
        ).start()
    own = pltpu.make_async_copy(block(gz), tiles_ref.at[slot_of(0, gz + 1)], local_sem.at[0])
    own_rank = pltpu.make_async_copy(ranks.at[gz], order_ref.at[gz], local_sem.at[1])
    own.start()
    own_rank.start()
    own.wait()
    own_rank.wait()

    def bulk(count, sem=0):
        part = tiles_ref.at[pl.ds(0, count)]
        return pltpu.make_async_remote_copy(
            src_ref=part, dst_ref=part, send_sem=send_sem.at[sem], recv_sem=recv_sem.at[0],
            device_id={"gx": gx, "gy": gy, "gz": peers[0]}, device_id_type=MESH,
        )

    def bulk_rank(count):
        part = order_ref.at[pl.ds(0, count)]
        return pltpu.make_async_remote_copy(
            src_ref=part, dst_ref=part, send_sem=rank_send.at[0], recv_sem=rank_recv.at[0],
            device_id={"gx": gx, "gy": gy, "gz": peers[0]}, device_id_type=MESH,
        )

    bulk(3 * (n_z + 2) - 1).wait_recv()
    bulk_rank(n_z - 1).wait_recv()
    bulk_rank(n_z - 1).wait_send()

    @pl.when(edge)
    def _():
        bulk(3 * n_z, 1).wait_send()

    bulk(3 * n_z - 1).wait_send()


def exchange(groups, positions, velocities, keys, counts):
    n_z = groups[2]
    vmem = pl.BlockSpec(memory_space=pltpu.VMEM)
    return pl.pallas_call(
        functools.partial(exchange_kernel, groups),
        out_shape=[
            jax.ShapeDtypeStruct((3 * (n_z + 2), 24, SLOTS), jnp.float32),
            jax.ShapeDtypeStruct((n_z, 1, SLOTS), jnp.int32),
        ],
        in_specs=[vmem, vmem, vmem, pl.BlockSpec(memory_space=pltpu.SMEM)],
        out_specs=[pl.BlockSpec(memory_space=pl.ANY)] * 2,
        scratch_shapes=[
            pltpu.VMEM((8 * (n_z + 2), SLOTS), jnp.float32),
            pltpu.VMEM((n_z, 1, SLOTS), jnp.int32),
            pltpu.SemaphoreType.DMA((2,)),
            pltpu.SemaphoreType.DMA((2,)),
            pltpu.SemaphoreType.DMA((1,)),
            pltpu.SemaphoreType.DMA((1,)),
            pltpu.SemaphoreType.DMA((1,)),
        ],
        compiler_params=pltpu.CompilerParams(collective_id=0, has_side_effects=True),
        name="sort_exchange",
    )(positions, velocities, keys, counts)


def runs_of(offset):
    spans = [{-1: (2, 3), 0: (0, 3), 1: (0, 1)}[o] for o in offset]
    runs = []
    for a in range(*spans[0]):
        for b in range(*spans[1]):
            low, high = a * 9 + b * 3 + spans[2][0], a * 9 + b * 3 + spans[2][1]
            if runs and runs[-1][1] == low:
                runs[-1] = (runs[-1][0], high)
            else:
                runs.append((low, high))
    return runs


def force_kernel(rows, tiles_ref, order_ref, out_ref):
    lane = lax.broadcasted_iota(jnp.int32, (rows, SLOTS), 1)
    left_half = lane < HALF
    position = lane & (HALF - 1)

    def load(offset, f):
        ox, oy, oz = offset
        start = (((1 + ox) * (rows + 2) + 1 + oy) * 3 + 1 + oz) * 8 + f
        return tiles_ref[pl.ds(start, rows, stride=24), :]

    def join(high, low):
        return high.astype(jnp.int32) * 32768 + low.astype(jnp.int32)

    home = (0, 0, 0)
    own = [load(home, f) for f in range(6)]
    own_key = join(load(home, 6), load(home, 7))

    def pair(other, other_key, summed):
        sep = [own[c] - other[c] for c in range(3)]
        squared = sep[0] * sep[0] + sep[1] * sep[1] + sep[2] * sep[2]
        root = lax.rsqrt(jnp.maximum(squared, 1e-30))
        distance = squared * root
        inverse = jnp.minimum(root, 1.0 / soft_radius)
        weight = jnp.maximum(1.0 - distance, 0.0) * inverse
        along = sep[0] * (own[3] - other[3])
        along = along + sep[1] * (own[4] - other[4])
        along = along + sep[2] * (own[5] - other[5])
        mixed = own_key ^ other_key
        hashed = mixed * 1103515245 + (own_key + other_key) * 12345
        hashed = hashed ^ lax.shift_right_logical(hashed, 15)
        hashed = hashed * 747796405
        hashed = hashed ^ lax.shift_right_logical(hashed, 13)
        fraction = lax.shift_right_logical(hashed << 1, 8).astype(jnp.float32)
        scale = noise_amplitude * root_twelve / 16777216.0
        base = like_repulsion - 0.5 * noise_amplitude * root_twelve
        level = jnp.where((mixed & 1) == 0, base, base + unlike_extra)
        strength = weight * (fraction * scale + level - friction * (weight * along))
        return tuple(summed[c] + strength * sep[c] for c in range(3))

    zero = jnp.zeros((rows, SLOTS), jnp.float32)
    summed = (zero, zero, zero)

    def count_cells(cells, low, high):
        inside = jnp.logical_and(cells >= low, cells < high)
        return jnp.sum(jnp.where(inside, 1.0, 0.0), axis=1, keepdims=True).astype(jnp.int32)

    def cells_of(x, y, z):
        cells = cell_of(x) * 9 + cell_of(y) * 3 + cell_of(z)
        return jnp.where(x > 0.5 * FAR, 27, cells)

    def group(axis, summed):
        sides = []
        longest = None
        for side in (-1, 1):
            tiles = []
            ranges = [(0,)] * axis + [(side,)] + [(-1, 0, 1)] * (2 - axis)
            total = jnp.zeros((rows, 1), jnp.int32)
            for ox in ranges[0]:
                for oy in ranges[1]:
                    for oz in ranges[2]:
                        offset = (ox, oy, oz)
                        cells = cells_of(*(load(offset, f) for f in range(3)))
                        table = []
                        for low, high in runs_of(offset):
                            begin = count_cells(cells, 0, low) if low else jnp.zeros_like(total)
                            length = count_cells(cells, low, high)
                            table.append((total, begin - total))
                            total = total + length
                        tiles.append((offset, table))
            sides.append((tiles, total))
            peak = jnp.max(total)
            longest = peak if longest is None else jnp.maximum(longest, peak)
        side_at = jnp.where(own[axis] < 1.5, 0, HALF)

        def one_pass(p, summed):
            at = position + p * HALF
            packed = [jnp.full((rows, SLOTS), FAR, jnp.float32)] + [zero] * 7
            for half, (tiles, total) in enumerate(sides):
                mine = left_half if half == 0 else jnp.logical_not(left_half)
                alive = jnp.logical_and(mine, at < total)
                for offset, table in tiles:
                    index = at
                    for base, shift in table:
                        index = jnp.where(at >= base, at + shift, index)
                    index = index & (SLOTS - 1)
                    taken = jnp.logical_and(alive, at >= table[0][0])
                    for f in range(8):
                        value = load(offset, f)
                        if f < 3 and offset[f]:
                            value = value + SIDE * offset[f]
                        packed[f] = jnp.where(taken, take(value, index), packed[f])
            packed_key = join(packed[6], packed[7])

            def some_steps(s, summed):
                for u in range(16):
                    index = side_at + (s * 16 + u)
                    other = [take(packed[f], index) for f in range(6)]
                    summed = pair(other, take(packed_key, index), summed)
                return summed

            steps = jnp.minimum(longest - p * HALF, HALF)
            return lax.fori_loop(0, (steps + 16 - 1) // 16, some_steps, summed)

        return lax.fori_loop(0, (longest + HALF - 1) // HALF, one_pass, summed)

    occupied = own[0] < 0.5 * FAR
    count = jnp.max(jnp.sum(jnp.where(occupied, 1.0, 0.0), axis=1, keepdims=True)).astype(jnp.int32)

    def own_steps(s, summed):
        for u in range(16):
            index = jnp.zeros_like(lane) + (s * 16 + u)
            other = [take(own[f], index) for f in range(6)]
            summed = pair(other, take(own_key, index), summed)
        return summed

    summed = lax.fori_loop(0, (count + 16 - 1) // 16, own_steps, summed)
    for axis in range(3):
        summed = group(axis, summed)

    order = order_ref[:, 0, :]
    scale = jnp.where(order < SLOTS, kick_scale, 0.0)
    order = order & (SLOTS - 1)
    for c in range(3):
        out_ref[c] = scale * take(summed[c], order)


def forces(n_z, tiles, order):
    vmem = pl.BlockSpec(memory_space=pltpu.VMEM)
    return pl.pallas_call(
        functools.partial(force_kernel, n_z),
        out_shape=jax.ShapeDtypeStruct((3, n_z, SLOTS), jnp.float32),
        in_specs=[vmem, vmem],
        out_specs=vmem,
        name="pair_forces",
    )(tiles, order)


def solution(mesh):
    groups = tuple(mesh.shape[a] for a in ("gx", "gy", "gz"))
    n_z = groups[2]

    def on_device(positions, velocities, bead_keys, counts):
        tiles, order = exchange(
            groups,
            positions.reshape(3, n_z, SLOTS),
            velocities.reshape(3, n_z, SLOTS),
            bead_keys.reshape(n_z, SLOTS),
            counts.reshape(n_z),
        )
        kick = forces(n_z, tiles.reshape(-1, SLOTS), order)
        return kick.reshape(3, 1, n_z, 1, SLOTS)

    in_specs = (
        P(None, "gx", ("gy", "gz"), None, None),
        P(None, "gx", ("gy", "gz"), None, None),
        P("gx", ("gy", "gz"), None, None),
        P("gx", ("gy", "gz"), None),
    )
    out_specs = P(None, "gx", "gy", "gz", None)
    return jax.shard_map(
        on_device, mesh=mesh, in_specs=in_specs, out_specs=out_specs, check_vma=False
    )
```

```python
import functools

import jax
import jax.numpy as jnp
from jax import lax
from jax.experimental import pallas as pl
from jax.experimental.pallas import tpu as pltpu
from jax.sharding import PartitionSpec as P

MESH = pl.DeviceIdType.MESH
SIDE = 3.0
SLOTS = 128
FAR = 4096.0
HALF = 64

soft_radius = 0.05
friction = 4.5
noise_amplitude = 15.0
like_repulsion = 25.0
unlike_extra = 15.0
kick_scale = 0.02
root_twelve = 3.4641016151377544


def take(values, index):
    return jnp.take_along_axis(values, index, axis=1, mode="promise_in_bounds")


def cell_of(part):
    return jnp.where(part >= 2.0, 2, jnp.where(part >= 1.0, 1, 0))


def exchange_kernel(
    groups, pos_ref, vel_ref, key_ref, count_ref, tiles_ref, order_ref,
    stage, ranks, mirrored, mirrored_ranks, edged, send_sem, recv_sem, rank_send, rank_recv,
):
    n_x, n_y, n_z = groups
    n_half = n_z // 2
    gx, gy, gz = lax.axis_index("gx"), lax.axis_index("gy"), lax.axis_index("gz")
    half, along = gz // n_half, lax.rem(gz, n_half)
    mirror = lax.rem(gz + n_half, n_z)
    first, last = gz == 0, gz == n_z - 1
    start, end = along == 0, along == n_half - 1
    above, below = lax.rem(gy + 1, n_y), lax.rem(gy + n_y - 1, n_y)
    columns = [lax.rem(gx + n_x + dx, n_x) for dx in (-1, 0, 1)]
    peers = [(k, dx) for k in (2, 1, 3, 0) for dx in (-1, 0, 1) if (k, dx) != (0, 0)]

    def slot_at(k):
        return lax.rem(along + k, n_half)

    def device(x, y, z):
        return {"gx": x, "gy": y, "gz": z}

    barrier = pltpu.get_barrier_semaphore()

    def ready(target):
        pl.semaphore_signal(barrier, inc=1, device_id=target, device_id_type=MESH)

    ready(device(gx, gy, mirror))
    for k, dx in peers:
        ready(device(columns[dx + 1], gy, half * n_half + slot_at(k)))

    @pl.when(start)
    def _():
        ready(device(gx, above, jnp.int32(0)))

    @pl.when(end)
    def _():
        ready(device(gx, below, jnp.int32(n_z - 1)))

    lane = lax.broadcasted_iota(jnp.int32, (n_z, SLOTS), 1)
    row = lax.broadcasted_iota(jnp.int32, (n_z, SLOTS), 0)
    occupancy = jnp.zeros((n_z, SLOTS), jnp.int32)
    for z in range(n_z):
        occupancy = jnp.where(row == z, count_ref[z], occupancy)
    px, py, pz = pos_ref[0], pos_ref[1], pos_ref[2]
    cell = cell_of(px) * 9 + cell_of(py) * 3 + cell_of(pz)
    cell = jnp.where(lane < occupancy, cell, 27)
    order = cell * SLOTS + lane
    rank = jnp.zeros((n_z, SLOTS), jnp.int32)
    for m in range(SLOTS):
        rank = rank + jnp.where(order[:, m : m + 1] < order, 1, 0)
    source = jnp.zeros((n_z, SLOTS), jnp.int32)
    for m in range(SLOTS):
        source = jnp.where(rank[:, m : m + 1] == lane, m, source)
    real = lane < occupancy
    key = key_ref[...]
    fields = [
        jnp.where(real, take(px, source), FAR),
        take(py, source),
        take(pz, source),
        take(vel_ref[0], source),
        take(vel_ref[1], source),
        take(vel_ref[2], source),
        take(lax.shift_right_logical(key, 15).astype(jnp.float32), source),
        take((key & 32767).astype(jnp.float32), source),
    ]
    for f, field in enumerate(fields):
        stage[pl.ds(8 + f, n_z, stride=8), :] = field
        stage[pl.ds(f, 1), :] = field[n_z - 1 : n_z]
        stage[pl.ds(8 * (n_z + 1) + f, 1), :] = field[0:1]
    masked = jnp.where(lane < occupancy, rank, rank + SLOTS)
    for z in range(n_z):
        ranks[z] = masked[z : z + 1]

    edge = jnp.logical_or(first, last)
    n_peers = len(peers)
    pl.semaphore_wait(barrier, jnp.where(edge, n_peers + 3, n_peers + 1))

    def copy(source, target, send, recv, to):
        return pltpu.make_async_remote_copy(
            src_ref=source, dst_ref=target, send_sem=send, recv_sem=recv,
            device_id=to, device_id_type=MESH,
        )

    def slab(h):
        return stage.at[pl.ds(pl.multiple_of(8 * n_half * h, 8), 8 * (n_half + 2)), :]

    across = copy(slab(1 - half), mirrored, send_sem.at[0], recv_sem.at[0], device(gx, gy, mirror))
    across.start()
    rank_across = copy(
        ranks.at[pl.ds(n_half * (1 - half), n_half)], mirrored_ranks,
        rank_send.at[0], rank_recv.at[0], device(gx, gy, mirror),
    )
    rank_across.start()

    def to_edge(h, y, position):
        return copy(
            slab(h), edged, send_sem.at[1 + h], recv_sem.at[1], device(gx, y, n_half * h + position)
        )

    @pl.when(first)
    def _():
        for h in (0, 1):
            to_edge(h, below, 0).start()

    @pl.when(last)
    def _():
        for h in (0, 1):
            to_edge(h, above, n_half - 1).start()

    def spread(buffer, offset, row_at, sem):
        def block(position):
            at = pl.multiple_of(8 * (offset + position), 8)
            return buffer.at[pl.ds(at, 24), :]

        for k, dx in peers:
            copy(
                block(slot_at(k)), tiles_ref.at[(1 - dx) * (n_z + 2) + row_at],
                send_sem.at[sem], recv_sem.at[2],
                device(columns[dx + 1], gy, half * n_half + slot_at(k)),
            ).start()
        pltpu.make_async_copy(
            block(along), tiles_ref.at[n_z + 2 + row_at], recv_sem.at[2]
        ).start()

    def spread_ranks(buffer, offset, row_at, sem):
        for k in (2, 1, 3):
            copy(
                buffer.at[offset + slot_at(k)], order_ref.at[row_at],
                rank_send.at[sem], rank_recv.at[1],
                device(gx, gy, half * n_half + slot_at(k)),
            ).start()
        pltpu.make_async_copy(
            buffer.at[offset + along], order_ref.at[row_at], rank_recv.at[1]
        ).start()

    spread(stage, half * n_half, gz + 1, 3)
    spread_ranks(ranks, half * n_half, gz, 1)
    across.wait_recv()
    spread(mirrored, 0, mirror + 1, 4)
    rank_across.wait_recv()
    spread_ranks(mirrored_ranks, 0, mirror, 2)
    relay = jnp.logical_or(start, end)

    @pl.when(relay)
    def _():
        copy(
            edged, edged, send_sem.at[1], recv_sem.at[1], device(gx, gy, mirror)
        ).wait_recv()
        spread(edged, 0, jnp.where(start, n_z + 1, 0), 5)

    def bulk(count, sem):
        part = tiles_ref.at[pl.ds(0, count)]
        return copy(part, part, send_sem.at[sem], recv_sem.at[2], device(gx, gy, mirror))

    def bulk_rank(count, sem):
        part = order_ref.at[pl.ds(0, count)]
        return copy(part, part, rank_send.at[sem], rank_recv.at[1], device(gx, gy, mirror))

    bulk(3 * (n_z + 2), 3).wait_recv()
    bulk_rank(n_z, 1).wait_recv()
    across.wait_send()
    rank_across.wait_send()
    for sem in (3, 4):
        bulk(n_peers, sem).wait_send()
    for sem in (1, 2):
        bulk_rank(n_half - 1, sem).wait_send()

    @pl.when(relay)
    def _():
        bulk(n_peers, 5).wait_send()

    @pl.when(edge)
    def _():
        for h in (0, 1):
            to_edge(h, gy, 0).wait_send()


def exchange(groups, positions, velocities, keys, counts):
    n_z = groups[2]
    vmem = pl.BlockSpec(memory_space=pltpu.VMEM)
    return pl.pallas_call(
        functools.partial(exchange_kernel, groups),
        out_shape=[
            jax.ShapeDtypeStruct((3 * (n_z + 2), 24, SLOTS), jnp.float32),
            jax.ShapeDtypeStruct((n_z, 1, SLOTS), jnp.int32),
        ],
        in_specs=[vmem, vmem, vmem, pl.BlockSpec(memory_space=pltpu.SMEM)],
        out_specs=[pl.BlockSpec(memory_space=pl.ANY)] * 2,
        scratch_shapes=[
            pltpu.VMEM((8 * (n_z + 2), SLOTS), jnp.float32),
            pltpu.VMEM((n_z, 1, SLOTS), jnp.int32),
            pltpu.VMEM((8 * (n_z // 2 + 2), SLOTS), jnp.float32),
            pltpu.VMEM((n_z // 2, 1, SLOTS), jnp.int32),
            pltpu.VMEM((8 * (n_z // 2 + 2), SLOTS), jnp.float32),
            pltpu.SemaphoreType.DMA((6,)),
            pltpu.SemaphoreType.DMA((3,)),
            pltpu.SemaphoreType.DMA((3,)),
            pltpu.SemaphoreType.DMA((2,)),
        ],
        compiler_params=pltpu.CompilerParams(collective_id=0, has_side_effects=True),
        name="sort_exchange",
    )(positions, velocities, keys, counts)


def runs_of(offset):
    spans = [{-1: (2, 3), 0: (0, 3), 1: (0, 1)}[o] for o in offset]
    runs = []
    for a in range(*spans[0]):
        for b in range(*spans[1]):
            low, high = a * 9 + b * 3 + spans[2][0], a * 9 + b * 3 + spans[2][1]
            if runs and runs[-1][1] == low:
                runs[-1] = (runs[-1][0], high)
            else:
                runs.append((low, high))
    return runs


def force_kernel(rows, tiles_ref, order_ref, out_ref):
    lane = lax.broadcasted_iota(jnp.int32, (rows, SLOTS), 1)
    left_half = lane < HALF
    position = lane & (HALF - 1)

    def load(offset, f):
        ox, oy, oz = offset
        start = (((1 + ox) * (rows + 2) + 1 + oy) * 3 + 1 + oz) * 8 + f
        return tiles_ref[pl.ds(start, rows, stride=24), :]

    def join(high, low):
        return high.astype(jnp.int32) * 32768 + low.astype(jnp.int32)

    home = (0, 0, 0)
    own = [load(home, f) for f in range(6)]
    own_key = join(load(home, 6), load(home, 7))

    def pair(other, other_key, summed):
        sep = [own[c] - other[c] for c in range(3)]
        squared = sep[0] * sep[0] + sep[1] * sep[1] + sep[2] * sep[2]
        root = lax.rsqrt(jnp.maximum(squared, 1e-30))
        distance = squared * root
        inverse = jnp.minimum(root, 1.0 / soft_radius)
        weight = jnp.maximum(1.0 - distance, 0.0) * inverse
        along = sep[0] * (own[3] - other[3])
        along = along + sep[1] * (own[4] - other[4])
        along = along + sep[2] * (own[5] - other[5])
        mixed = own_key ^ other_key
        hashed = mixed * 1103515245 + (own_key + other_key) * 12345
        hashed = hashed ^ lax.shift_right_logical(hashed, 15)
        hashed = hashed * 747796405
        hashed = hashed ^ lax.shift_right_logical(hashed, 13)
        fraction = lax.shift_right_logical(hashed << 1, 8).astype(jnp.float32)
        scale = noise_amplitude * root_twelve / 16777216.0
        base = like_repulsion - 0.5 * noise_amplitude * root_twelve
        level = jnp.where((mixed & 1) == 0, base, base + unlike_extra)
        strength = weight * (fraction * scale + level - friction * (weight * along))
        return tuple(summed[c] + strength * sep[c] for c in range(3))

    zero = jnp.zeros((rows, SLOTS), jnp.float32)
    summed = (zero, zero, zero)

    def count_cells(cells, low, high):
        inside = jnp.logical_and(cells >= low, cells < high)
        return jnp.sum(jnp.where(inside, 1.0, 0.0), axis=1, keepdims=True).astype(jnp.int32)

    def cells_of(x, y, z):
        cells = cell_of(x) * 9 + cell_of(y) * 3 + cell_of(z)
        return jnp.where(x > 0.5 * FAR, 27, cells)

    def group(axis, summed):
        sides = []
        longest = None
        for side in (-1, 1):
            tiles = []
            ranges = [(0,)] * axis + [(side,)] + [(-1, 0, 1)] * (2 - axis)
            total = jnp.zeros((rows, 1), jnp.int32)
            for ox in ranges[0]:
                for oy in ranges[1]:
                    for oz in ranges[2]:
                        offset = (ox, oy, oz)
                        cells = cells_of(*(load(offset, f) for f in range(3)))
                        table = []
                        for low, high in runs_of(offset):
                            begin = count_cells(cells, 0, low) if low else jnp.zeros_like(total)
                            length = count_cells(cells, low, high)
                            table.append((total, begin - total))
                            total = total + length
                        tiles.append((offset, table))
            sides.append((tiles, total))
            peak = jnp.max(total)
            longest = peak if longest is None else jnp.maximum(longest, peak)
        side_at = jnp.where(own[axis] < 1.5, 0, HALF)

        def one_pass(p, summed):
            at = position + p * HALF
            packed = [jnp.full((rows, SLOTS), FAR, jnp.float32)] + [zero] * 7
            for half, (tiles, total) in enumerate(sides):
                mine = left_half if half == 0 else jnp.logical_not(left_half)
                alive = jnp.logical_and(mine, at < total)
                for offset, table in tiles:
                    index = at
                    for base, shift in table:
                        index = jnp.where(at >= base, at + shift, index)
                    index = index & (SLOTS - 1)
                    taken = jnp.logical_and(alive, at >= table[0][0])
                    for f in range(8):
                        value = load(offset, f)
                        if f < 3 and offset[f]:
                            value = value + SIDE * offset[f]
                        packed[f] = jnp.where(taken, take(value, index), packed[f])
            packed_key = join(packed[6], packed[7])

            def some_steps(s, summed):
                for u in range(16):
                    index = side_at + (s * 16 + u)
                    other = [take(packed[f], index) for f in range(6)]
                    summed = pair(other, take(packed_key, index), summed)
                return summed

            steps = jnp.minimum(longest - p * HALF, HALF)
            return lax.fori_loop(0, (steps + 16 - 1) // 16, some_steps, summed)

        return lax.fori_loop(0, (longest + HALF - 1) // HALF, one_pass, summed)

    occupied = own[0] < 0.5 * FAR
    count = jnp.max(jnp.sum(jnp.where(occupied, 1.0, 0.0), axis=1, keepdims=True)).astype(jnp.int32)

    def own_steps(s, summed):
        for u in range(16):
            index = jnp.zeros_like(lane) + (s * 16 + u)
            other = [take(own[f], index) for f in range(6)]
            summed = pair(other, take(own_key, index), summed)
        return summed

    summed = lax.fori_loop(0, (count + 16 - 1) // 16, own_steps, summed)
    for axis in range(3):
        summed = group(axis, summed)

    order = order_ref[:, 0, :]
    scale = jnp.where(order < SLOTS, kick_scale, 0.0)
    order = order & (SLOTS - 1)
    for c in range(3):
        out_ref[c] = scale * take(summed[c], order)


def forces(n_z, tiles, order):
    vmem = pl.BlockSpec(memory_space=pltpu.VMEM)
    return pl.pallas_call(
        functools.partial(force_kernel, n_z),
        out_shape=jax.ShapeDtypeStruct((3, n_z, SLOTS), jnp.float32),
        in_specs=[vmem, vmem],
        out_specs=vmem,
        name="pair_forces",
    )(tiles, order)


def solution(mesh):
    groups = tuple(mesh.shape[a] for a in ("gx", "gy", "gz"))
    n_z = groups[2]

    def on_device(positions, velocities, bead_keys, counts):
        tiles, order = exchange(
            groups,
            positions.reshape(3, n_z, SLOTS),
            velocities.reshape(3, n_z, SLOTS),
            bead_keys.reshape(n_z, SLOTS),
            counts.reshape(n_z),
        )
        kick = forces(n_z, tiles.reshape(-1, SLOTS), order)
        return kick.reshape(3, 1, n_z, 1, SLOTS)

    in_specs = (
        P(None, "gx", ("gy", "gz"), None, None),
        P(None, "gx", ("gy", "gz"), None, None),
        P("gx", ("gy", "gz"), None, None),
        P("gx", ("gy", "gz"), None),
    )
    out_specs = P(None, "gx", "gy", "gz", None)
    return jax.shard_map(
        on_device, mesh=mesh, in_specs=in_specs, out_specs=out_specs, check_vma=False
    )
```

```python
import functools

import jax
import jax.numpy as jnp
from jax import lax
from jax.experimental import pallas as pl
from jax.experimental.pallas import tpu as pltpu
from jax.sharding import PartitionSpec as P

MESH = pl.DeviceIdType.MESH
SIDE = 3.0
SLOTS = 128
FAR = 4096.0
HALF = 64
TURNS = 21

soft_radius = 0.05
friction = 4.5
noise_amplitude = 15.0
like_repulsion = 25.0
unlike_extra = 15.0
kick_scale = 0.02
root_twelve = 3.4641016151377544


def take(values, index):
    return jnp.take_along_axis(values, index, axis=1, mode="promise_in_bounds")


def cell_of(part):
    return jnp.where(part >= 2.0, 2, jnp.where(part >= 1.0, 1, 0))


def pair_force(own, own_key, other, other_key):
    sep = [own[c] - other[c] for c in range(3)]
    squared = sep[0] * sep[0] + sep[1] * sep[1] + sep[2] * sep[2]
    root = lax.rsqrt(jnp.maximum(squared, 1e-30))
    distance = squared * root
    inverse = jnp.minimum(root, 1.0 / soft_radius)
    weight = jnp.maximum(1.0 - distance, 0.0) * inverse
    along = sep[0] * (own[3] - other[3])
    along = along + sep[1] * (own[4] - other[4])
    along = along + sep[2] * (own[5] - other[5])
    mixed = own_key ^ other_key
    hashed = mixed * 1103515245 + (own_key + other_key) * 12345
    hashed = hashed ^ lax.shift_right_logical(hashed, 15)
    hashed = hashed * 747796405
    hashed = hashed ^ lax.shift_right_logical(hashed, 13)
    fraction = lax.shift_right_logical(hashed << 1, 8).astype(jnp.float32)
    scale = noise_amplitude * root_twelve / 16777216.0
    base = like_repulsion - 0.5 * noise_amplitude * root_twelve
    level = jnp.where((mixed & 1) == 0, base, base + unlike_extra)
    strength = weight * (fraction * scale + level - friction * (weight * along))
    return [strength * sep[c] for c in range(3)]


def exchange_kernel(
    groups, pos_hbm, vel_hbm, key_hbm, count_hbm, tiles_ref, order_ref,
    pos_ref, vel_ref, key_ref, count_ref, stage, ranks, mirrored, mirrored_ranks, edged,
    load_sem, send_sem, recv_sem, rank_send, rank_recv,
):
    n_x, n_y, n_z = groups
    n_half = n_z // 2
    gx, gy, gz = lax.axis_index("gx"), lax.axis_index("gy"), lax.axis_index("gz")
    half, along = gz // n_half, lax.rem(gz, n_half)
    mirror = lax.rem(gz + n_half, n_z)
    first, last = gz == 0, gz == n_z - 1
    start, end = along == 0, along == n_half - 1
    above, below = lax.rem(gy + 1, n_y), lax.rem(gy + n_y - 1, n_y)
    columns = [lax.rem(gx + n_x + dx, n_x) for dx in (-1, 0, 1)]
    peers = [(k, dx) for k in (2, 1, 3, 0) for dx in (-1, 0, 1) if (k, dx) != (0, 0)]

    def slot_at(k):
        return lax.rem(along + k, n_half)

    def device(x, y, z):
        return {"gx": x, "gy": y, "gz": z}

    barrier = pltpu.get_barrier_semaphore()

    def ready(target):
        pl.semaphore_signal(barrier, inc=1, device_id=target, device_id_type=MESH)

    ready(device(gx, gy, mirror))
    for k, dx in peers:
        ready(device(columns[dx + 1], gy, half * n_half + slot_at(k)))

    @pl.when(start)
    def _():
        ready(device(gx, above, jnp.int32(0)))

    @pl.when(end)
    def _():
        ready(device(gx, below, jnp.int32(n_z - 1)))

    loads = [
        pltpu.make_async_copy(source, target, load_sem.at[i])
        for i, (source, target) in enumerate(
            [(pos_hbm, pos_ref), (count_hbm, count_ref), (key_hbm, key_ref), (vel_hbm, vel_ref)]
        )
    ]
    for load in loads:
        load.start()
    for load in loads:
        load.wait()

    lane = lax.broadcasted_iota(jnp.int32, (n_z, SLOTS), 1)
    row = lax.broadcasted_iota(jnp.int32, (n_z, SLOTS), 0)
    occupancy = jnp.zeros((n_z, SLOTS), jnp.int32)
    for z in range(n_z):
        occupancy = jnp.where(row == z, count_ref[z], occupancy)
    px, py, pz = pos_ref[0], pos_ref[1], pos_ref[2]
    cell = cell_of(px) * 9 + cell_of(py) * 3 + cell_of(pz)
    cell = jnp.where(lane < occupancy, cell, 27)
    order = cell * SLOTS + lane
    rank = jnp.zeros((n_z, SLOTS), jnp.int32)
    for m in range(SLOTS):
        rank = rank + jnp.where(order[:, m : m + 1] < order, 1, 0)
    source = jnp.zeros((n_z, SLOTS), jnp.int32)
    for m in range(SLOTS):
        source = jnp.where(rank[:, m : m + 1] == lane, m, source)
    real = lane < occupancy
    key = key_ref[...]
    fields = [
        jnp.where(real, take(px, source), FAR),
        take(py, source),
        take(pz, source),
        take(vel_ref[0], source),
        take(vel_ref[1], source),
        take(vel_ref[2], source),
        take(lax.shift_right_logical(key, 15).astype(jnp.float32), source),
        take((key & 32767).astype(jnp.float32), source),
    ]
    for f, field in enumerate(fields):
        stage[pl.ds(8 + f, n_z, stride=8), :] = field
        stage[pl.ds(f, 1), :] = field[n_z - 1 : n_z]
        stage[pl.ds(8 * (n_z + 1) + f, 1), :] = field[0:1]

    sorted_key = take(key, source)

    def turned(shift):
        back = SLOTS - shift
        other = [pltpu.roll(field, back, 1) for field in fields[:6]]
        return pair_force(fields[:6], sorted_key, other, pltpu.roll(sorted_key, back, 1))

    def some_turns(step, summed):
        for u in range(TURNS):
            shift = step * TURNS + (u + 1)
            push = turned(shift)
            summed = tuple(
                summed[c] + (push[c] - pltpu.roll(push[c], shift, 1)) for c in range(3)
            )
        return summed

    zero = jnp.zeros((n_z, SLOTS), jnp.float32)
    summed = lax.fori_loop(0, (SLOTS // 2 - 1) // TURNS, some_turns, (zero, zero, zero))
    last_push = turned(SLOTS // 2)
    for c in range(3):
        ranks[:, c, :] = summed[c] + last_push[c]
    ranks[:, 3, :] = jnp.where(real, rank, rank + SLOTS).astype(jnp.float32)

    edge = jnp.logical_or(first, last)
    n_peers = len(peers)
    pl.semaphore_wait(barrier, jnp.where(edge, n_peers + 3, n_peers + 1))

    def copy(source, target, send, recv, to):
        return pltpu.make_async_remote_copy(
            src_ref=source, dst_ref=target, send_sem=send, recv_sem=recv,
            device_id=to, device_id_type=MESH,
        )

    def slab(h):
        return stage.at[pl.ds(pl.multiple_of(8 * n_half * h, 8), 8 * (n_half + 2)), :]

    across = copy(slab(1 - half), mirrored, send_sem.at[0], recv_sem.at[0], device(gx, gy, mirror))
    across.start()
    rank_across = copy(
        ranks.at[pl.ds(n_half * (1 - half), n_half)], mirrored_ranks,
        rank_send.at[0], rank_recv.at[0], device(gx, gy, mirror),
    )
    rank_across.start()

    def to_edge(h, y, position):
        return copy(
            slab(h), edged, send_sem.at[1 + h], recv_sem.at[1], device(gx, y, n_half * h + position)
        )

    @pl.when(first)
    def _():
        for h in (0, 1):
            to_edge(h, below, 0).start()

    @pl.when(last)
    def _():
        for h in (0, 1):
            to_edge(h, above, n_half - 1).start()

    def spread(buffer, offset, row_at, sem):
        def block(position):
            at = pl.multiple_of(8 * (offset + position), 8)
            return buffer.at[pl.ds(at, 24), :]

        for k, dx in peers:
            copy(
                block(slot_at(k)), tiles_ref.at[(1 - dx) * (n_z + 2) + row_at],
                send_sem.at[sem], recv_sem.at[2],
                device(columns[dx + 1], gy, half * n_half + slot_at(k)),
            ).start()
        pltpu.make_async_copy(
            block(along), tiles_ref.at[n_z + 2 + row_at], recv_sem.at[2]
        ).start()

    def spread_ranks(buffer, offset, row_at, sem):
        for k in (2, 1, 3):
            copy(
                buffer.at[offset + slot_at(k)], order_ref.at[row_at],
                rank_send.at[sem], rank_recv.at[1],
                device(gx, gy, half * n_half + slot_at(k)),
            ).start()
        pltpu.make_async_copy(
            buffer.at[offset + along], order_ref.at[row_at], rank_recv.at[1]
        ).start()

    spread(stage, half * n_half, gz + 1, 3)
    spread_ranks(ranks, half * n_half, gz, 1)
    across.wait_recv()
    spread(mirrored, 0, mirror + 1, 4)
    rank_across.wait_recv()
    spread_ranks(mirrored_ranks, 0, mirror, 2)
    relay = jnp.logical_or(start, end)

    @pl.when(relay)
    def _():
        copy(
            edged, edged, send_sem.at[1], recv_sem.at[1], device(gx, gy, mirror)
        ).wait_recv()
        spread(edged, 0, jnp.where(start, n_z + 1, 0), 5)

    def bulk(count, sem):
        part = tiles_ref.at[pl.ds(0, count)]
        return copy(part, part, send_sem.at[sem], recv_sem.at[2], device(gx, gy, mirror))

    def bulk_rank(count, sem):
        part = order_ref.at[pl.ds(0, count)]
        return copy(part, part, rank_send.at[sem], rank_recv.at[1], device(gx, gy, mirror))

    bulk(3 * (n_z + 2), 3).wait_recv()
    bulk_rank(n_z, 1).wait_recv()
    across.wait_send()
    rank_across.wait_send()
    for sem in (3, 4):
        bulk(n_peers, sem).wait_send()
    for sem in (1, 2):
        bulk_rank(n_half - 1, sem).wait_send()

    @pl.when(relay)
    def _():
        bulk(n_peers, 5).wait_send()

    @pl.when(edge)
    def _():
        for h in (0, 1):
            to_edge(h, gy, 0).wait_send()


def exchange(groups, positions, velocities, keys, counts):
    n_z = groups[2]
    anywhere = pl.BlockSpec(memory_space=pl.ANY)
    slab = pltpu.VMEM((8 * (n_z // 2 + 2), SLOTS), jnp.float32)
    return pl.pallas_call(
        functools.partial(exchange_kernel, groups),
        out_shape=[
            jax.ShapeDtypeStruct((3 * (n_z + 2), 24, SLOTS), jnp.float32),
            jax.ShapeDtypeStruct((n_z, 4, SLOTS), jnp.float32),
        ],
        in_specs=[anywhere] * 4,
        out_specs=[anywhere] * 2,
        scratch_shapes=[
            pltpu.VMEM((3, n_z, SLOTS), jnp.float32),
            pltpu.VMEM((3, n_z, SLOTS), jnp.float32),
            pltpu.VMEM((n_z, SLOTS), jnp.int32),
            pltpu.SMEM((n_z,), jnp.int32),
            pltpu.VMEM((8 * (n_z + 2), SLOTS), jnp.float32),
            pltpu.VMEM((n_z, 4, SLOTS), jnp.float32),
            slab,
            pltpu.VMEM((n_z // 2, 4, SLOTS), jnp.float32),
            slab,
            pltpu.SemaphoreType.DMA((4,)),
            pltpu.SemaphoreType.DMA((6,)),
            pltpu.SemaphoreType.DMA((3,)),
            pltpu.SemaphoreType.DMA((3,)),
            pltpu.SemaphoreType.DMA((2,)),
        ],
        compiler_params=pltpu.CompilerParams(collective_id=0, has_side_effects=True),
        name="sort_exchange",
    )(positions, velocities, keys, counts)


def runs_of(offset):
    spans = [{-1: (2, 3), 0: (0, 3), 1: (0, 1)}[o] for o in offset]
    runs = []
    for a in range(*spans[0]):
        for b in range(*spans[1]):
            low, high = a * 9 + b * 3 + spans[2][0], a * 9 + b * 3 + spans[2][1]
            if runs and runs[-1][1] == low:
                runs[-1] = (runs[-1][0], high)
            else:
                runs.append((low, high))
    return runs


def force_kernel(rows, tiles_ref, order_ref, out_ref):
    lane = lax.broadcasted_iota(jnp.int32, (rows, SLOTS), 1)
    left_half = lane < HALF
    position = lane & (HALF - 1)

    def load(offset, f):
        ox, oy, oz = offset
        start = (((1 + ox) * (rows + 2) + 1 + oy) * 3 + 1 + oz) * 8 + f
        return tiles_ref[pl.ds(start, rows, stride=24), :]

    def join(high, low):
        return high.astype(jnp.int32) * 32768 + low.astype(jnp.int32)

    home = (0, 0, 0)
    own = [load(home, f) for f in range(6)]
    own_key = join(load(home, 6), load(home, 7))

    def pair(other, other_key, summed):
        push = pair_force(own, own_key, other, other_key)
        return tuple(summed[c] + push[c] for c in range(3))

    zero = jnp.zeros((rows, SLOTS), jnp.float32)
    summed = tuple(order_ref[:, c, :] for c in range(3))

    def count_cells(cells, low, high):
        inside = jnp.logical_and(cells >= low, cells < high)
        return jnp.sum(jnp.where(inside, 1.0, 0.0), axis=1, keepdims=True).astype(jnp.int32)

    def cells_of(x, y, z):
        cells = cell_of(x) * 9 + cell_of(y) * 3 + cell_of(z)
        return jnp.where(x > 0.5 * FAR, 27, cells)

    def group(axis, summed):
        sides = []
        longest = None
        for side in (-1, 1):
            tiles = []
            ranges = [(0,)] * axis + [(side,)] + [(-1, 0, 1)] * (2 - axis)
            total = jnp.zeros((rows, 1), jnp.int32)
            for ox in ranges[0]:
                for oy in ranges[1]:
                    for oz in ranges[2]:
                        offset = (ox, oy, oz)
                        cells = cells_of(*(load(offset, f) for f in range(3)))
                        table = []
                        for low, high in runs_of(offset):
                            begin = count_cells(cells, 0, low) if low else jnp.zeros_like(total)
                            length = count_cells(cells, low, high)
                            table.append((total, begin - total))
                            total = total + length
                        tiles.append((offset, table))
            sides.append((tiles, total))
            peak = jnp.max(total)
            longest = peak if longest is None else jnp.maximum(longest, peak)
        side_at = jnp.where(own[axis] < 1.5, 0, HALF)

        def one_pass(p, summed):
            at = position + p * HALF
            packed = [jnp.full((rows, SLOTS), FAR, jnp.float32)] + [zero] * 7
            for half, (tiles, total) in enumerate(sides):
                mine = left_half if half == 0 else jnp.logical_not(left_half)
                alive = jnp.logical_and(mine, at < total)
                for offset, table in tiles:
                    index = at
                    for base, shift in table:
                        index = jnp.where(at >= base, at + shift, index)
                    index = index & (SLOTS - 1)
                    taken = jnp.logical_and(alive, at >= table[0][0])
                    for f in range(8):
                        value = load(offset, f)
                        if f < 3 and offset[f]:
                            value = value + SIDE * offset[f]
                        packed[f] = jnp.where(taken, take(value, index), packed[f])
            packed_key = join(packed[6], packed[7])

            def some_steps(s, summed):
                for u in range(16):
                    index = side_at + (s * 16 + u)
                    other = [take(packed[f], index) for f in range(6)]
                    summed = pair(other, take(packed_key, index), summed)
                return summed

            steps = jnp.minimum(longest - p * HALF, HALF)
            return lax.fori_loop(0, (steps + 16 - 1) // 16, some_steps, summed)

        return lax.fori_loop(0, (longest + HALF - 1) // HALF, one_pass, summed)

    for axis in range(3):
        summed = group(axis, summed)

    order = order_ref[:, 3, :].astype(jnp.int32)
    scale = jnp.where(order < SLOTS, kick_scale, 0.0)
    order = order & (SLOTS - 1)
    for c in range(3):
        out_ref[c] = scale * take(summed[c], order)


def forces(n_z, tiles, order):
    vmem = pl.BlockSpec(memory_space=pltpu.VMEM)
    return pl.pallas_call(
        functools.partial(force_kernel, n_z),
        out_shape=jax.ShapeDtypeStruct((3, n_z, SLOTS), jnp.float32),
        in_specs=[vmem, vmem],
        out_specs=vmem,
        name="pair_forces",
    )(tiles, order)


def solution(mesh):
    groups = tuple(mesh.shape[a] for a in ("gx", "gy", "gz"))
    n_z = groups[2]

    def on_device(positions, velocities, bead_keys, counts):
        tiles, order = exchange(
            groups,
            positions.reshape(3, n_z, SLOTS),
            velocities.reshape(3, n_z, SLOTS),
            bead_keys.reshape(n_z, SLOTS),
            counts.reshape(n_z),
        )
        kick = forces(n_z, tiles.reshape(-1, SLOTS), order)
        return kick.reshape(3, 1, n_z, 1, SLOTS)

    in_specs = (
        P(None, "gx", ("gy", "gz"), None, None),
        P(None, "gx", ("gy", "gz"), None, None),
        P("gx", ("gy", "gz"), None, None),
        P("gx", ("gy", "gz"), None),
    )
    out_specs = P(None, "gx", "gy", "gz", None)
    return jax.shard_map(
        on_device, mesh=mesh, in_specs=in_specs, out_specs=out_specs, check_vma=False
    )
```

```python
import functools

import jax
import jax.numpy as jnp
from jax import lax
from jax.experimental import pallas as pl
from jax.experimental.pallas import tpu as pltpu
from jax.sharding import PartitionSpec as P

MESH = pl.DeviceIdType.MESH
SIDE = 3.0
SLOTS = 128
FAR = 4096.0
HALF = 64
TURNS = 21

soft_radius = 0.05
friction = 4.5
noise_amplitude = 15.0
like_repulsion = 25.0
unlike_extra = 15.0
kick_scale = 0.02
root_twelve = 3.4641016151377544


def take(values, index):
    return jnp.take_along_axis(values, index, axis=1, mode="promise_in_bounds")


def cell_of(part):
    return jnp.where(part >= 2.0, 2, jnp.where(part >= 1.0, 1, 0))


def pair_force(own, own_key, other, other_key):
    sep = [own[c] - other[c] for c in range(3)]
    squared = sep[0] * sep[0] + sep[1] * sep[1] + sep[2] * sep[2]
    root = lax.rsqrt(jnp.maximum(squared, 1e-30))
    distance = squared * root
    inverse = jnp.minimum(root, 1.0 / soft_radius)
    weight = jnp.maximum(1.0 - distance, 0.0) * inverse
    along = sep[0] * (own[3] - other[3])
    along = along + sep[1] * (own[4] - other[4])
    along = along + sep[2] * (own[5] - other[5])
    mixed = own_key ^ other_key
    hashed = mixed * 1103515245 + (own_key + other_key) * 12345
    hashed = hashed ^ lax.shift_right_logical(hashed, 15)
    hashed = hashed * 747796405
    hashed = hashed ^ lax.shift_right_logical(hashed, 13)
    fraction = lax.shift_right_logical(hashed << 1, 8).astype(jnp.float32)
    scale = noise_amplitude * root_twelve / 16777216.0
    base = like_repulsion - 0.5 * noise_amplitude * root_twelve
    level = jnp.where((mixed & 1) == 0, base, base + unlike_extra)
    strength = weight * (fraction * scale + level - friction * (weight * along))
    return [strength * sep[c] for c in range(3)]


def exchange_kernel(
    groups, pos_hbm, vel_hbm, key_hbm, count_hbm, tiles_ref, order_ref,
    pos_ref, vel_ref, key_ref, count_ref, stage, ranks, mirrored, mirrored_ranks, edged,
    load_sem, send_sem, recv_sem, rank_send, rank_recv,
):
    n_x, n_y, n_z = groups
    n_half = n_z // 2
    gx, gy, gz = lax.axis_index("gx"), lax.axis_index("gy"), lax.axis_index("gz")
    half, along = gz // n_half, lax.rem(gz, n_half)
    mirror = lax.rem(gz + n_half, n_z)
    first, last = gz == 0, gz == n_z - 1
    start, end = along == 0, along == n_half - 1
    above, below = lax.rem(gy + 1, n_y), lax.rem(gy + n_y - 1, n_y)
    columns = [lax.rem(gx + n_x + dx, n_x) for dx in (-1, 0, 1)]
    peers = [(k, dx) for k in (2, 1, 3, 0) for dx in (-1, 0, 1) if (k, dx) != (0, 0)]

    def slot_at(k):
        return lax.rem(along + k, n_half)

    def device(x, y, z):
        return {"gx": x, "gy": y, "gz": z}

    barrier = pltpu.get_barrier_semaphore()

    def ready(target):
        pl.semaphore_signal(barrier, inc=1, device_id=target, device_id_type=MESH)

    ready(device(gx, gy, mirror))
    for k, dx in peers:
        ready(device(columns[dx + 1], gy, half * n_half + slot_at(k)))

    @pl.when(start)
    def _():
        ready(device(gx, above, jnp.int32(0)))

    @pl.when(end)
    def _():
        ready(device(gx, below, jnp.int32(n_z - 1)))

    loads = [
        pltpu.make_async_copy(source, target, load_sem.at[i])
        for i, (source, target) in enumerate(
            [(pos_hbm, pos_ref), (count_hbm, count_ref), (key_hbm, key_ref), (vel_hbm, vel_ref)]
        )
    ]
    for load in loads:
        load.start()
    for load in loads:
        load.wait()

    lane = lax.broadcasted_iota(jnp.int32, (n_z, SLOTS), 1)
    row = lax.broadcasted_iota(jnp.int32, (n_z, SLOTS), 0)
    occupancy = jnp.zeros((n_z, SLOTS), jnp.int32)
    for z in range(n_z):
        occupancy = jnp.where(row == z, count_ref[z], occupancy)
    px, py, pz = pos_ref[0], pos_ref[1], pos_ref[2]
    cell = cell_of(px) * 9 + cell_of(py) * 3 + cell_of(pz)
    cell = jnp.where(lane < occupancy, cell, 27)
    order = cell * SLOTS + lane
    rank = jnp.zeros((n_z, SLOTS), jnp.int32)
    for m in range(SLOTS):
        rank = rank + jnp.where(order[:, m : m + 1] < order, 1, 0)
    source = jnp.zeros((n_z, SLOTS), jnp.int32)
    for m in range(SLOTS):
        source = jnp.where(rank[:, m : m + 1] == lane, m, source)
    real = lane < occupancy
    key = key_ref[...]
    fields = [
        jnp.where(real, take(px, source), FAR),
        take(py, source),
        take(pz, source),
        take(vel_ref[0], source),
        take(vel_ref[1], source),
        take(vel_ref[2], source),
        take(lax.shift_right_logical(key, 15).astype(jnp.float32), source),
        take((key & 32767).astype(jnp.float32), source),
    ]
    for f, field in enumerate(fields):
        stage[pl.ds(8 + f, n_z, stride=8), :] = field
        stage[pl.ds(f, 1), :] = field[n_z - 1 : n_z]
        stage[pl.ds(8 * (n_z + 1) + f, 1), :] = field[0:1]

    sorted_key = take(key, source)

    def turned(shift):
        back = SLOTS - shift
        other = [pltpu.roll(field, back, 1) for field in fields[:6]]
        return pair_force(fields[:6], sorted_key, other, pltpu.roll(sorted_key, back, 1))

    def some_turns(step, summed):
        for u in range(TURNS):
            shift = step * TURNS + (u + 1)
            push = turned(shift)
            summed = tuple(
                summed[c] + (push[c] - pltpu.roll(push[c], shift, 1)) for c in range(3)
            )
        return summed

    zero = jnp.zeros((n_z, SLOTS), jnp.float32)
    summed = lax.fori_loop(0, (SLOTS // 2 - 1) // TURNS, some_turns, (zero, zero, zero))
    last_push = turned(SLOTS // 2)
    for c in range(3):
        ranks[:, c, :] = summed[c] + last_push[c]
    ranks[:, 3, :] = jnp.where(real, rank, rank + SLOTS).astype(jnp.float32)

    edge = jnp.logical_or(first, last)
    n_peers = len(peers)
    pl.semaphore_wait(barrier, jnp.where(edge, n_peers + 3, n_peers + 1))

    def copy(source, target, send, recv, to):
        return pltpu.make_async_remote_copy(
            src_ref=source, dst_ref=target, send_sem=send, recv_sem=recv,
            device_id=to, device_id_type=MESH,
        )

    def slab(h):
        return stage.at[pl.ds(pl.multiple_of(8 * n_half * h, 8), 8 * (n_half + 2)), :]

    across = copy(slab(1 - half), mirrored, send_sem.at[0], recv_sem.at[0], device(gx, gy, mirror))
    across.start()
    rank_across = copy(
        ranks.at[pl.ds(n_half * (1 - half), n_half)], mirrored_ranks,
        rank_send.at[0], rank_recv.at[0], device(gx, gy, mirror),
    )
    rank_across.start()

    def to_edge(h, y, position):
        return copy(
            slab(h), edged, send_sem.at[1 + h], recv_sem.at[1], device(gx, y, n_half * h + position)
        )

    @pl.when(first)
    def _():
        for h in (0, 1):
            to_edge(h, below, 0).start()

    @pl.when(last)
    def _():
        for h in (0, 1):
            to_edge(h, above, n_half - 1).start()

    def landing(slot):
        return tiles_ref.at[pl.ds(pl.multiple_of(24 * slot, 8), 24), :]

    def spread(buffer, offset, row_at, sem):
        def block(position):
            at = pl.multiple_of(8 * (offset + position), 8)
            return buffer.at[pl.ds(at, 24), :]

        for k, dx in peers:
            copy(
                block(slot_at(k)), landing((1 - dx) * (n_z + 2) + row_at),
                send_sem.at[sem], recv_sem.at[2],
                device(columns[dx + 1], gy, half * n_half + slot_at(k)),
            ).start()
        pltpu.make_async_copy(
            block(along), landing(n_z + 2 + row_at), recv_sem.at[2]
        ).start()

    def spread_ranks(buffer, offset, row_at, sem):
        for k in (2, 1, 3):
            copy(
                buffer.at[offset + slot_at(k)], order_ref.at[row_at],
                rank_send.at[sem], rank_recv.at[1],
                device(gx, gy, half * n_half + slot_at(k)),
            ).start()
        pltpu.make_async_copy(
            buffer.at[offset + along], order_ref.at[row_at], rank_recv.at[1]
        ).start()

    spread(stage, half * n_half, gz + 1, 3)
    spread_ranks(ranks, half * n_half, gz, 1)
    across.wait_recv()
    spread(mirrored, 0, mirror + 1, 4)
    rank_across.wait_recv()
    spread_ranks(mirrored_ranks, 0, mirror, 2)
    relay = jnp.logical_or(start, end)

    @pl.when(relay)
    def _():
        copy(
            edged, edged, send_sem.at[1], recv_sem.at[1], device(gx, gy, mirror)
        ).wait_recv()
        spread(edged, 0, jnp.where(start, n_z + 1, 0), 5)

    def bulk(count, sem):
        part = tiles_ref.at[pl.ds(0, 24 * count)]
        return copy(part, part, send_sem.at[sem], recv_sem.at[2], device(gx, gy, mirror))

    def bulk_rank(count, sem):
        part = order_ref.at[pl.ds(0, count)]
        return copy(part, part, rank_send.at[sem], rank_recv.at[1], device(gx, gy, mirror))

    bulk(3 * (n_z + 2), 3).wait_recv()
    bulk_rank(n_z, 1).wait_recv()
    across.wait_send()
    rank_across.wait_send()
    for sem in (3, 4):
        bulk(n_peers, sem).wait_send()
    for sem in (1, 2):
        bulk_rank(n_half - 1, sem).wait_send()

    @pl.when(relay)
    def _():
        bulk(n_peers, 5).wait_send()

    @pl.when(edge)
    def _():
        for h in (0, 1):
            to_edge(h, gy, 0).wait_send()


def exchange(groups, positions, velocities, keys, counts):
    n_z = groups[2]
    anywhere = pl.BlockSpec(memory_space=pl.ANY)
    slab = pltpu.VMEM((8 * (n_z // 2 + 2), SLOTS), jnp.float32)
    return pl.pallas_call(
        functools.partial(exchange_kernel, groups),
        out_shape=[
            pltpu.VMEM((72 * (n_z + 2), SLOTS), jnp.float32),
            pltpu.VMEM((n_z, 4, SLOTS), jnp.float32),
        ],
        in_specs=[anywhere] * 4,
        out_specs=[pl.BlockSpec(memory_space=pltpu.VMEM)] * 2,
        scratch_shapes=[
            pltpu.VMEM((3, n_z, SLOTS), jnp.float32),
            pltpu.VMEM((3, n_z, SLOTS), jnp.float32),
            pltpu.VMEM((n_z, SLOTS), jnp.int32),
            pltpu.SMEM((n_z,), jnp.int32),
            pltpu.VMEM((8 * (n_z + 2), SLOTS), jnp.float32),
            pltpu.VMEM((n_z, 4, SLOTS), jnp.float32),
            slab,
            pltpu.VMEM((n_z // 2, 4, SLOTS), jnp.float32),
            slab,
            pltpu.SemaphoreType.DMA((4,)),
            pltpu.SemaphoreType.DMA((6,)),
            pltpu.SemaphoreType.DMA((3,)),
            pltpu.SemaphoreType.DMA((3,)),
            pltpu.SemaphoreType.DMA((2,)),
        ],
        compiler_params=pltpu.CompilerParams(collective_id=0, has_side_effects=True),
        name="sort_exchange",
    )(positions, velocities, keys, counts)


def runs_of(offset):
    spans = [{-1: (2, 3), 0: (0, 3), 1: (0, 1)}[o] for o in offset]
    runs = []
    for a in range(*spans[0]):
        for b in range(*spans[1]):
            low, high = a * 9 + b * 3 + spans[2][0], a * 9 + b * 3 + spans[2][1]
            if runs and runs[-1][1] == low:
                runs[-1] = (runs[-1][0], high)
            else:
                runs.append((low, high))
    return runs


def force_kernel(rows, tiles_ref, order_ref, out_ref):
    lane = lax.broadcasted_iota(jnp.int32, (rows, SLOTS), 1)
    left_half = lane < HALF
    position = lane & (HALF - 1)

    def load(offset, f):
        ox, oy, oz = offset
        start = (((1 + ox) * (rows + 2) + 1 + oy) * 3 + 1 + oz) * 8 + f
        return tiles_ref[pl.ds(start, rows, stride=24), :]

    def join(high, low):
        return high.astype(jnp.int32) * 32768 + low.astype(jnp.int32)

    home = (0, 0, 0)
    own = [load(home, f) for f in range(6)]
    own_key = join(load(home, 6), load(home, 7))

    def pair(other, other_key, summed):
        push = pair_force(own, own_key, other, other_key)
        return tuple(summed[c] + push[c] for c in range(3))

    zero = jnp.zeros((rows, SLOTS), jnp.float32)
    summed = tuple(order_ref[:, c, :] for c in range(3))

    def count_cells(cells, low, high):
        inside = jnp.logical_and(cells >= low, cells < high)
        return jnp.sum(jnp.where(inside, 1.0, 0.0), axis=1, keepdims=True).astype(jnp.int32)

    def cells_of(x, y, z):
        cells = cell_of(x) * 9 + cell_of(y) * 3 + cell_of(z)
        return jnp.where(x > 0.5 * FAR, 27, cells)

    def group(axis, summed):
        sides = []
        longest = None
        for side in (-1, 1):
            tiles = []
            ranges = [(0,)] * axis + [(side,)] + [(-1, 0, 1)] * (2 - axis)
            total = jnp.zeros((rows, 1), jnp.int32)
            for ox in ranges[0]:
                for oy in ranges[1]:
                    for oz in ranges[2]:
                        offset = (ox, oy, oz)
                        cells = cells_of(*(load(offset, f) for f in range(3)))
                        table = []
                        for low, high in runs_of(offset):
                            begin = count_cells(cells, 0, low) if low else jnp.zeros_like(total)
                            length = count_cells(cells, low, high)
                            table.append((total, begin - total))
                            total = total + length
                        tiles.append((offset, table))
            sides.append((tiles, total))
            peak = jnp.max(total)
            longest = peak if longest is None else jnp.maximum(longest, peak)
        side_at = jnp.where(own[axis] < 1.5, 0, HALF)

        def one_pass(p, summed):
            at = position + p * HALF
            packed = [jnp.full((rows, SLOTS), FAR, jnp.float32)] + [zero] * 7
            for half, (tiles, total) in enumerate(sides):
                mine = left_half if half == 0 else jnp.logical_not(left_half)
                alive = jnp.logical_and(mine, at < total)
                for offset, table in tiles:
                    index = at
                    for base, shift in table:
                        index = jnp.where(at >= base, at + shift, index)
                    index = index & (SLOTS - 1)
                    taken = jnp.logical_and(alive, at >= table[0][0])
                    for f in range(8):
                        value = load(offset, f)
                        if f < 3 and offset[f]:
                            value = value + SIDE * offset[f]
                        packed[f] = jnp.where(taken, take(value, index), packed[f])
            packed_key = join(packed[6], packed[7])

            def some_steps(s, summed):
                for u in range(16):
                    index = side_at + (s * 16 + u)
                    other = [take(packed[f], index) for f in range(6)]
                    summed = pair(other, take(packed_key, index), summed)
                return summed

            steps = jnp.minimum(longest - p * HALF, HALF)
            return lax.fori_loop(0, (steps + 16 - 1) // 16, some_steps, summed)

        return lax.fori_loop(0, (longest + HALF - 1) // HALF, one_pass, summed)

    for axis in range(3):
        summed = group(axis, summed)

    order = order_ref[:, 3, :].astype(jnp.int32)
    scale = jnp.where(order < SLOTS, kick_scale, 0.0)
    order = order & (SLOTS - 1)
    for c in range(3):
        out_ref[c] = scale * take(summed[c], order)


def forces(n_z, tiles, order):
    vmem = pl.BlockSpec(memory_space=pltpu.VMEM)
    return pl.pallas_call(
        functools.partial(force_kernel, n_z),
        out_shape=jax.ShapeDtypeStruct((3, n_z, SLOTS), jnp.float32),
        in_specs=[vmem, vmem],
        out_specs=vmem,
        name="pair_forces",
    )(*(pltpu.with_memory_space_constraint(x, pltpu.VMEM) for x in (tiles, order)))


def solution(mesh):
    groups = tuple(mesh.shape[a] for a in ("gx", "gy", "gz"))
    n_z = groups[2]

    def on_device(positions, velocities, bead_keys, counts):
        tiles, order = exchange(
            groups,
            positions.reshape(3, n_z, SLOTS),
            velocities.reshape(3, n_z, SLOTS),
            bead_keys.reshape(n_z, SLOTS),
            counts.reshape(n_z),
        )
        kick = forces(n_z, tiles, order)
        return kick.reshape(3, 1, n_z, 1, SLOTS)

    in_specs = (
        P(None, "gx", ("gy", "gz"), None, None),
        P(None, "gx", ("gy", "gz"), None, None),
        P("gx", ("gy", "gz"), None, None),
        P("gx", ("gy", "gz"), None),
    )
    out_specs = P(None, "gx", "gy", "gz", None)
    return jax.shard_map(
        on_device, mesh=mesh, in_specs=in_specs, out_specs=out_specs, check_vma=False
    )
```

```python
import functools

import jax
import jax.numpy as jnp
from jax import lax
from jax.experimental import pallas as pl
from jax.experimental.pallas import tpu as pltpu
from jax.sharding import PartitionSpec as P

MESH = pl.DeviceIdType.MESH
SIDE = 3.0
SLOTS = 128
FAR = 4096.0
HALF = 64
TURNS = 21

soft_radius = 0.05
friction = 4.5
noise_amplitude = 15.0
like_repulsion = 25.0
unlike_extra = 15.0
kick_scale = 0.02
root_twelve = 3.4641016151377544


def take(values, index):
    return jnp.take_along_axis(values, index, axis=1, mode="promise_in_bounds")


def cell_of(part):
    return jnp.where(part >= 2.0, 2, jnp.where(part >= 1.0, 1, 0))


def pair_force(own, own_key, other, other_key):
    sep = [own[c] - other[c] for c in range(3)]
    squared = sep[0] * sep[0] + sep[1] * sep[1] + sep[2] * sep[2]
    root = lax.rsqrt(jnp.maximum(squared, 1e-30))
    distance = squared * root
    inverse = jnp.minimum(root, 1.0 / soft_radius)
    weight = jnp.maximum(1.0 - distance, 0.0) * inverse
    along = sep[0] * (own[3] - other[3])
    along = along + sep[1] * (own[4] - other[4])
    along = along + sep[2] * (own[5] - other[5])
    mixed = own_key ^ other_key
    hashed = mixed * 1103515245 + (own_key + other_key) * 12345
    hashed = hashed ^ lax.shift_right_logical(hashed, 15)
    hashed = hashed * 747796405
    hashed = hashed ^ lax.shift_right_logical(hashed, 13)
    fraction = lax.shift_right_logical(hashed << 1, 8).astype(jnp.float32)
    scale = noise_amplitude * root_twelve / 16777216.0
    base = like_repulsion - 0.5 * noise_amplitude * root_twelve
    level = jnp.where((mixed & 1) == 0, base, base + unlike_extra)
    strength = weight * (fraction * scale + level - friction * (weight * along))
    return [strength * sep[c] for c in range(3)]


def exchange_kernel(
    groups, pos_hbm, vel_hbm, key_hbm, count_hbm, tiles_ref, order_ref,
    pos_ref, vel_ref, key_ref, count_ref, stage, ranks, mirrored, edged,
    load_sem, send_sem, recv_sem, rank_send, rank_recv,
):
    n_x, n_y, n_z = groups
    n_half = n_z // 2
    gx, gy, gz = lax.axis_index("gx"), lax.axis_index("gy"), lax.axis_index("gz")
    half, along = gz // n_half, lax.rem(gz, n_half)
    mirror = lax.rem(gz + n_half, n_z)
    first, last = gz == 0, gz == n_z - 1
    start, end = along == 0, along == n_half - 1
    above, below = lax.rem(gy + 1, n_y), lax.rem(gy + n_y - 1, n_y)
    columns = [lax.rem(gx + n_x + dx, n_x) for dx in (-1, 0, 1)]
    peers = [(k, dx) for k in (2, 1, 3, 0) for dx in (-1, 0, 1) if (k, dx) != (0, 0)]

    def slot_at(k):
        return lax.rem(along + k, n_half)

    def device(x, y, z):
        return {"gx": x, "gy": y, "gz": z}

    barrier = pltpu.get_barrier_semaphore()

    def ready(target):
        pl.semaphore_signal(barrier, inc=1, device_id=target, device_id_type=MESH)

    opposite = [lax.rem(mirror // n_half * n_half + slot_at(k), n_z) for k in (2, 1, 3, 0)]
    for z in opposite:
        ready(device(gx, gy, z))
    for k, dx in peers:
        ready(device(columns[dx + 1], gy, half * n_half + slot_at(k)))

    @pl.when(start)
    def _():
        ready(device(gx, above, jnp.int32(0)))

    @pl.when(end)
    def _():
        ready(device(gx, below, jnp.int32(n_z - 1)))

    loads = [
        pltpu.make_async_copy(source, target, load_sem.at[i])
        for i, (source, target) in enumerate(
            [(pos_hbm, pos_ref), (count_hbm, count_ref), (key_hbm, key_ref), (vel_hbm, vel_ref)]
        )
    ]
    for load in loads:
        load.start()
    for load in loads:
        load.wait()

    lane = lax.broadcasted_iota(jnp.int32, (n_z, SLOTS), 1)
    row = lax.broadcasted_iota(jnp.int32, (n_z, SLOTS), 0)
    occupancy = jnp.zeros((n_z, SLOTS), jnp.int32)
    for z in range(n_z):
        occupancy = jnp.where(row == z, count_ref[z], occupancy)
    px, py, pz = pos_ref[0], pos_ref[1], pos_ref[2]
    cell = cell_of(px) * 9 + cell_of(py) * 3 + cell_of(pz)
    cell = jnp.where(lane < occupancy, cell, 27)
    order = cell * SLOTS + lane
    rank = jnp.zeros((n_z, SLOTS), jnp.int32)
    for m in range(SLOTS):
        rank = rank + jnp.where(order[:, m : m + 1] < order, 1, 0)
    source = jnp.zeros((n_z, SLOTS), jnp.int32)
    for m in range(SLOTS):
        source = jnp.where(rank[:, m : m + 1] == lane, m, source)
    real = lane < occupancy
    key = key_ref[...]
    fields = [
        jnp.where(real, take(px, source), FAR),
        take(py, source),
        take(pz, source),
        take(vel_ref[0], source),
        take(vel_ref[1], source),
        take(vel_ref[2], source),
        take(lax.shift_right_logical(key, 15).astype(jnp.float32), source),
        take((key & 32767).astype(jnp.float32), source),
    ]
    for f, field in enumerate(fields):
        stage[pl.ds(8 + f, n_z, stride=8), :] = field
        stage[pl.ds(f, 1), :] = field[n_z - 1 : n_z]
        stage[pl.ds(8 * (n_z + 1) + f, 1), :] = field[0:1]

    edge = jnp.logical_or(first, last)
    n_peers = len(peers)
    pl.semaphore_wait(barrier, jnp.where(edge, n_peers + 6, n_peers + 4))

    def copy(source, target, send, recv, to):
        return pltpu.make_async_remote_copy(
            src_ref=source, dst_ref=target, send_sem=send, recv_sem=recv,
            device_id=to, device_id_type=MESH,
        )

    def slab(h):
        return stage.at[pl.ds(pl.multiple_of(8 * n_half * h, 8), 8 * (n_half + 2)), :]

    across = copy(slab(1 - half), mirrored, send_sem.at[0], recv_sem.at[0], device(gx, gy, mirror))
    across.start()
    def to_edge(h, y, position):
        return copy(
            slab(h), edged, send_sem.at[1 + h], recv_sem.at[1], device(gx, y, n_half * h + position)
        )

    @pl.when(first)
    def _():
        for h in (0, 1):
            to_edge(h, below, 0).start()

    @pl.when(last)
    def _():
        for h in (0, 1):
            to_edge(h, above, n_half - 1).start()

    def landing(slot):
        return tiles_ref.at[pl.ds(pl.multiple_of(24 * slot, 8), 24), :]

    def spread(buffer, offset, row_at, sem):
        def block(position):
            at = pl.multiple_of(8 * (offset + position), 8)
            return buffer.at[pl.ds(at, 24), :]

        for k, dx in peers:
            copy(
                block(slot_at(k)), landing((1 - dx) * (n_z + 2) + row_at),
                send_sem.at[sem], recv_sem.at[2],
                device(columns[dx + 1], gy, half * n_half + slot_at(k)),
            ).start()
        pltpu.make_async_copy(
            block(along), landing(n_z + 2 + row_at), recv_sem.at[2]
        ).start()

    spread(stage, half * n_half, gz + 1, 3)
    sorted_key = take(key, source)

    def turned(shift):
        back = SLOTS - shift
        other = [pltpu.roll(field, back, 1) for field in fields[:6]]
        return pair_force(fields[:6], sorted_key, other, pltpu.roll(sorted_key, back, 1))

    def some_turns(step, summed):
        for u in range(TURNS):
            shift = step * TURNS + (u + 1)
            push = turned(shift)
            summed = tuple(
                summed[c] + (push[c] - pltpu.roll(push[c], shift, 1)) for c in range(3)
            )
        return summed

    zero = jnp.zeros((n_z, SLOTS), jnp.float32)
    summed = lax.fori_loop(0, (SLOTS // 2 - 1) // TURNS, some_turns, (zero, zero, zero))
    last_push = turned(SLOTS // 2)
    for c in range(3):
        ranks[:, c, :] = summed[c] + last_push[c]
    ranks[:, 3, :] = jnp.where(real, rank, rank + SLOTS).astype(jnp.float32)

    for z in opposite + [half * n_half + slot_at(k) for k in (2, 1, 3)]:
        copy(
            ranks.at[z], order_ref.at[gz], rank_send.at[0], rank_recv.at[0], device(gx, gy, z)
        ).start()
    pltpu.make_async_copy(ranks.at[gz], order_ref.at[gz], rank_recv.at[0]).start()

    across.wait_recv()
    spread(mirrored, 0, mirror + 1, 4)
    relay = jnp.logical_or(start, end)

    @pl.when(relay)
    def _():
        copy(
            edged, edged, send_sem.at[1], recv_sem.at[1], device(gx, gy, mirror)
        ).wait_recv()
        spread(edged, 0, jnp.where(start, n_z + 1, 0), 5)

    def bulk(count, sem):
        part = tiles_ref.at[pl.ds(0, 24 * count)]
        return copy(part, part, send_sem.at[sem], recv_sem.at[2], device(gx, gy, mirror))

    def bulk_rank(count):
        part = order_ref.at[pl.ds(0, count)]
        return copy(part, part, rank_send.at[0], rank_recv.at[0], device(gx, gy, mirror))

    bulk(3 * (n_z + 2), 3).wait_recv()
    bulk_rank(n_z).wait_recv()
    across.wait_send()
    bulk_rank(n_z - 1).wait_send()
    for sem in (3, 4):
        bulk(n_peers, sem).wait_send()

    @pl.when(relay)
    def _():
        bulk(n_peers, 5).wait_send()

    @pl.when(edge)
    def _():
        for h in (0, 1):
            to_edge(h, gy, 0).wait_send()


def exchange(groups, positions, velocities, keys, counts):
    n_z = groups[2]
    anywhere = pl.BlockSpec(memory_space=pl.ANY)
    slab = pltpu.VMEM((8 * (n_z // 2 + 2), SLOTS), jnp.float32)
    return pl.pallas_call(
        functools.partial(exchange_kernel, groups),
        out_shape=[
            pltpu.VMEM((72 * (n_z + 2), SLOTS), jnp.float32),
            pltpu.VMEM((n_z, 4, SLOTS), jnp.float32),
        ],
        in_specs=[anywhere] * 4,
        out_specs=[pl.BlockSpec(memory_space=pltpu.VMEM)] * 2,
        scratch_shapes=[
            pltpu.VMEM((3, n_z, SLOTS), jnp.float32),
            pltpu.VMEM((3, n_z, SLOTS), jnp.float32),
            pltpu.VMEM((n_z, SLOTS), jnp.int32),
            pltpu.SMEM((n_z,), jnp.int32),
            pltpu.VMEM((8 * (n_z + 2), SLOTS), jnp.float32),
            pltpu.VMEM((n_z, 4, SLOTS), jnp.float32),
            slab,
            slab,
            pltpu.SemaphoreType.DMA((4,)),
            pltpu.SemaphoreType.DMA((6,)),
            pltpu.SemaphoreType.DMA((3,)),
            pltpu.SemaphoreType.DMA((1,)),
            pltpu.SemaphoreType.DMA((1,)),
        ],
        compiler_params=pltpu.CompilerParams(collective_id=0, has_side_effects=True),
        name="sort_exchange",
    )(positions, velocities, keys, counts)


def runs_of(offset):
    spans = [{-1: (2, 3), 0: (0, 3), 1: (0, 1)}[o] for o in offset]
    runs = []
    for a in range(*spans[0]):
        for b in range(*spans[1]):
            low, high = a * 9 + b * 3 + spans[2][0], a * 9 + b * 3 + spans[2][1]
            if runs and runs[-1][1] == low:
                runs[-1] = (runs[-1][0], high)
            else:
                runs.append((low, high))
    return runs


def force_kernel(rows, tiles_ref, order_ref, out_ref):
    lane = lax.broadcasted_iota(jnp.int32, (rows, SLOTS), 1)
    left_half = lane < HALF
    position = lane & (HALF - 1)

    def load(offset, f):
        ox, oy, oz = offset
        start = (((1 + ox) * (rows + 2) + 1 + oy) * 3 + 1 + oz) * 8 + f
        return tiles_ref[pl.ds(start, rows, stride=24), :]

    def join(high, low):
        return high.astype(jnp.int32) * 32768 + low.astype(jnp.int32)

    home = (0, 0, 0)
    own = [load(home, f) for f in range(6)]
    own_key = join(load(home, 6), load(home, 7))

    def pair(other, other_key, summed):
        push = pair_force(own, own_key, other, other_key)
        return tuple(summed[c] + push[c] for c in range(3))

    zero = jnp.zeros((rows, SLOTS), jnp.float32)
    summed = tuple(order_ref[:, c, :] for c in range(3))

    def count_cells(cells, low, high):
        inside = jnp.logical_and(cells >= low, cells < high)
        return jnp.sum(jnp.where(inside, 1.0, 0.0), axis=1, keepdims=True).astype(jnp.int32)

    def cells_of(x, y, z):
        cells = cell_of(x) * 9 + cell_of(y) * 3 + cell_of(z)
        return jnp.where(x > 0.5 * FAR, 27, cells)

    def group(axis, summed):
        sides = []
        longest = None
        for side in (-1, 1):
            tiles = []
            ranges = [(0,)] * axis + [(side,)] + [(-1, 0, 1)] * (2 - axis)
            total = jnp.zeros((rows, 1), jnp.int32)
            for ox in ranges[0]:
                for oy in ranges[1]:
                    for oz in ranges[2]:
                        offset = (ox, oy, oz)
                        cells = cells_of(*(load(offset, f) for f in range(3)))
                        table = []
                        for low, high in runs_of(offset):
                            begin = count_cells(cells, 0, low) if low else jnp.zeros_like(total)
                            length = count_cells(cells, low, high)
                            table.append((total, begin - total))
                            total = total + length
                        tiles.append((offset, table))
            sides.append((tiles, total))
            peak = jnp.max(total)
            longest = peak if longest is None else jnp.maximum(longest, peak)
        side_at = jnp.where(own[axis] < 1.5, 0, HALF)

        def one_pass(p, summed):
            at = position + p * HALF
            packed = [jnp.full((rows, SLOTS), FAR, jnp.float32)] + [zero] * 7
            for half, (tiles, total) in enumerate(sides):
                mine = left_half if half == 0 else jnp.logical_not(left_half)
                alive = jnp.logical_and(mine, at < total)
                for offset, table in tiles:
                    index = at
                    for base, shift in table:
                        index = jnp.where(at >= base, at + shift, index)
                    index = index & (SLOTS - 1)
                    taken = jnp.logical_and(alive, at >= table[0][0])
                    for f in range(8):
                        value = load(offset, f)
                        if f < 3 and offset[f]:
                            value = value + SIDE * offset[f]
                        packed[f] = jnp.where(taken, take(value, index), packed[f])
            packed_key = join(packed[6], packed[7])

            def some_steps(s, summed):
                for u in range(16):
                    index = side_at + (s * 16 + u)
                    other = [take(packed[f], index) for f in range(6)]
                    summed = pair(other, take(packed_key, index), summed)
                return summed

            steps = jnp.minimum(longest - p * HALF, HALF)
            return lax.fori_loop(0, (steps + 16 - 1) // 16, some_steps, summed)

        return lax.fori_loop(0, (longest + HALF - 1) // HALF, one_pass, summed)

    for axis in range(3):
        summed = group(axis, summed)

    order = order_ref[:, 3, :].astype(jnp.int32)
    scale = jnp.where(order < SLOTS, kick_scale, 0.0)
    order = order & (SLOTS - 1)
    for c in range(3):
        out_ref[c] = scale * take(summed[c], order)


def forces(n_z, tiles, order):
    vmem = pl.BlockSpec(memory_space=pltpu.VMEM)
    return pl.pallas_call(
        functools.partial(force_kernel, n_z),
        out_shape=jax.ShapeDtypeStruct((3, n_z, SLOTS), jnp.float32),
        in_specs=[vmem, vmem],
        out_specs=vmem,
        name="pair_forces",
    )(*(pltpu.with_memory_space_constraint(x, pltpu.VMEM) for x in (tiles, order)))


def solution(mesh):
    groups = tuple(mesh.shape[a] for a in ("gx", "gy", "gz"))
    n_z = groups[2]

    def on_device(positions, velocities, bead_keys, counts):
        tiles, order = exchange(
            groups,
            positions.reshape(3, n_z, SLOTS),
            velocities.reshape(3, n_z, SLOTS),
            bead_keys.reshape(n_z, SLOTS),
            counts.reshape(n_z),
        )
        kick = forces(n_z, tiles, order)
        return kick.reshape(3, 1, n_z, 1, SLOTS)

    in_specs = (
        P(None, "gx", ("gy", "gz"), None, None),
        P(None, "gx", ("gy", "gz"), None, None),
        P("gx", ("gy", "gz"), None, None),
        P("gx", ("gy", "gz"), None),
    )
    out_specs = P(None, "gx", "gy", "gz", None)
    return jax.shard_map(
        on_device, mesh=mesh, in_specs=in_specs, out_specs=out_specs, check_vma=False
    )
```

```python
import functools

import jax
import jax.numpy as jnp
from jax import lax
from jax.experimental import pallas as pl
from jax.experimental.pallas import tpu as pltpu
from jax.sharding import PartitionSpec as P

MESH = pl.DeviceIdType.MESH
SIDE = 3.0
SLOTS = 128
FAR = 4096.0
HALF = 64
TURNS = 21
TURNS_Z = 16
UNROLL = 16

soft_radius = 0.05
friction = 4.5
noise_amplitude = 15.0
like_repulsion = 25.0
unlike_extra = 15.0
kick_scale = 0.02
root_twelve = 3.4641016151377544


def take(values, index):
    return jnp.take_along_axis(values, index, axis=1, mode="promise_in_bounds")


def cell_of(part):
    return jnp.where(part >= 2.0, 2, jnp.where(part >= 1.0, 1, 0))


def pair_force(own, own_key, other, other_key):
    sep = [own[c] - other[c] for c in range(3)]
    squared = sep[0] * sep[0] + sep[1] * sep[1] + sep[2] * sep[2]
    root = lax.rsqrt(jnp.maximum(squared, 1e-30))
    distance = squared * root
    inverse = jnp.minimum(root, 1.0 / soft_radius)
    weight = jnp.maximum(1.0 - distance, 0.0) * inverse
    along = sep[0] * (own[3] - other[3])
    along = along + sep[1] * (own[4] - other[4])
    along = along + sep[2] * (own[5] - other[5])
    mixed = own_key ^ other_key
    hashed = mixed * 1103515245 + (own_key + other_key) * 12345
    hashed = hashed ^ lax.shift_right_logical(hashed, 15)
    hashed = hashed * 747796405
    hashed = hashed ^ lax.shift_right_logical(hashed, 13)
    fraction = lax.shift_right_logical(hashed << 1, 8).astype(jnp.float32)
    scale = noise_amplitude * root_twelve / 16777216.0
    base = like_repulsion - 0.5 * noise_amplitude * root_twelve
    level = jnp.where((mixed & 1) == 0, base, base + unlike_extra)
    strength = weight * (fraction * scale + level - friction * (weight * along))
    return [strength * sep[c] for c in range(3)]


def exchange_kernel(
    groups, pos_hbm, vel_hbm, key_hbm, count_hbm, tiles_ref, order_ref,
    pos_ref, vel_ref, key_ref, count_ref, stage, ranks, mirrored, edged,
    load_sem, send_sem, recv_sem, rank_send, rank_recv,
):
    n_x, n_y, n_z = groups
    n_half = n_z // 2
    gx, gy, gz = lax.axis_index("gx"), lax.axis_index("gy"), lax.axis_index("gz")
    half, along = gz // n_half, lax.rem(gz, n_half)
    mirror = lax.rem(gz + n_half, n_z)
    first, last = gz == 0, gz == n_z - 1
    start, end = along == 0, along == n_half - 1
    above, below = lax.rem(gy + 1, n_y), lax.rem(gy + n_y - 1, n_y)
    columns = [lax.rem(gx + n_x + dx, n_x) for dx in (-1, 0, 1)]
    peers = [(k, dx) for k in (2, 1, 3, 0) for dx in (-1, 0, 1) if (k, dx) != (0, 0)]

    def slot_at(k):
        return lax.rem(along + k, n_half)

    def device(x, y, z):
        return {"gx": x, "gy": y, "gz": z}

    barrier = pltpu.get_barrier_semaphore()

    def ready(target):
        pl.semaphore_signal(barrier, inc=1, device_id=target, device_id_type=MESH)

    opposite = [lax.rem(mirror // n_half * n_half + slot_at(k), n_z) for k in (2, 1, 3, 0)]
    for z in opposite:
        ready(device(gx, gy, z))
    for k, dx in peers:
        ready(device(columns[dx + 1], gy, half * n_half + slot_at(k)))

    @pl.when(start)
    def _():
        ready(device(gx, above, jnp.int32(0)))

    @pl.when(end)
    def _():
        ready(device(gx, below, jnp.int32(n_z - 1)))

    loads = [
        pltpu.make_async_copy(source, target, load_sem.at[i])
        for i, (source, target) in enumerate(
            [(pos_hbm, pos_ref), (count_hbm, count_ref), (key_hbm, key_ref), (vel_hbm, vel_ref)]
        )
    ]
    for load in loads:
        load.start()
    for load in loads:
        load.wait()

    lane = lax.broadcasted_iota(jnp.int32, (n_z, SLOTS), 1)
    row = lax.broadcasted_iota(jnp.int32, (n_z, SLOTS), 0)
    occupancy = jnp.zeros((n_z, SLOTS), jnp.int32)
    for z in range(n_z):
        occupancy = jnp.where(row == z, count_ref[z], occupancy)
    px, py, pz = pos_ref[0], pos_ref[1], pos_ref[2]
    cell = cell_of(px) * 9 + cell_of(py) * 3 + cell_of(pz)
    cell = jnp.where(lane < occupancy, cell, 27)
    order = cell * SLOTS + lane
    rank = jnp.zeros((n_z, SLOTS), jnp.int32)
    for m in range(SLOTS):
        rank = rank + jnp.where(order[:, m : m + 1] < order, 1, 0)
    source = jnp.zeros((n_z, SLOTS), jnp.int32)
    for m in range(SLOTS):
        source = jnp.where(rank[:, m : m + 1] == lane, m, source)
    real = lane < occupancy
    key = key_ref[...]
    fields = [
        jnp.where(real, take(px, source), FAR),
        take(py, source),
        take(pz, source),
        take(vel_ref[0], source),
        take(vel_ref[1], source),
        take(vel_ref[2], source),
        take(lax.shift_right_logical(key, 15).astype(jnp.float32), source),
        take((key & 32767).astype(jnp.float32), source),
    ]
    for f, field in enumerate(fields):
        stage[pl.ds(8 + f, n_z, stride=8), :] = field
        stage[pl.ds(f, 1), :] = field[n_z - 1 : n_z]
        stage[pl.ds(8 * (n_z + 1) + f, 1), :] = field[0:1]

    edge = jnp.logical_or(first, last)
    n_peers = len(peers)
    pl.semaphore_wait(barrier, jnp.where(edge, n_peers + 6, n_peers + 4))

    def copy(source, target, send, recv, to):
        return pltpu.make_async_remote_copy(
            src_ref=source, dst_ref=target, send_sem=send, recv_sem=recv,
            device_id=to, device_id_type=MESH,
        )

    def slab(h):
        return stage.at[pl.ds(pl.multiple_of(8 * n_half * h, 8), 8 * (n_half + 2)), :]

    across = copy(slab(1 - half), mirrored, send_sem.at[0], recv_sem.at[0], device(gx, gy, mirror))
    across.start()
    def to_edge(h, y, position):
        return copy(
            slab(h), edged, send_sem.at[1 + h], recv_sem.at[1], device(gx, y, n_half * h + position)
        )

    @pl.when(first)
    def _():
        for h in (0, 1):
            to_edge(h, below, 0).start()

    @pl.when(last)
    def _():
        for h in (0, 1):
            to_edge(h, above, n_half - 1).start()

    def landing(slot):
        return tiles_ref.at[pl.ds(pl.multiple_of(24 * slot, 8), 24), :]

    def spread(buffer, offset, row_at, sem):
        def block(position):
            at = pl.multiple_of(8 * (offset + position), 8)
            return buffer.at[pl.ds(at, 24), :]

        for k, dx in peers:
            copy(
                block(slot_at(k)), landing((1 - dx) * (n_z + 2) + row_at),
                send_sem.at[sem], recv_sem.at[2],
                device(columns[dx + 1], gy, half * n_half + slot_at(k)),
            ).start()
        pltpu.make_async_copy(
            block(along), landing(n_z + 2 + row_at), recv_sem.at[2]
        ).start()

    spread(stage, half * n_half, gz + 1, 3)
    sorted_key = take(key, source)

    def turned(shift):
        back = SLOTS - shift
        other = [pltpu.roll(field, back, 1) for field in fields[:6]]
        return pair_force(fields[:6], sorted_key, other, pltpu.roll(sorted_key, back, 1))

    def some_turns(step, summed):
        for u in range(TURNS):
            shift = step * TURNS + (u + 1)
            push = turned(shift)
            summed = tuple(
                summed[c] + (push[c] - pltpu.roll(push[c], shift, 1)) for c in range(3)
            )
        return summed

    zero = jnp.zeros((n_z, SLOTS), jnp.float32)
    summed = lax.fori_loop(0, (SLOTS // 2 - 1) // TURNS, some_turns, (zero, zero, zero))
    last_push = turned(SLOTS // 2)
    summed = tuple(summed[c] + last_push[c] for c in range(3))

    left = lane < HALF
    inside = fields[0] < 0.5 * FAR
    top = jnp.logical_and(inside, fields[2] >= 2.0)
    bottom = jnp.logical_and(inside, fields[2] < 1.0)
    member = jnp.where(top, 1, jnp.where(bottom, 2 * SLOTS, 0))
    before = jnp.zeros((n_z, SLOTS), jnp.int32)
    for m in range(SLOTS):
        before = before + jnp.where(lane > m, member[:, m : m + 1], 0)
    low, high = before & (2 * SLOTS - 1), lax.shift_right_logical(before, 8)
    seat = jnp.where(jnp.logical_and(bottom, high < HALF), high + HALF, SLOTS)
    seat = jnp.where(jnp.logical_and(top, low < HALF), low, seat)
    origin = jnp.full((n_z, SLOTS), -1, jnp.int32)
    for m in range(SLOTS):
        origin = jnp.where(seat[:, m : m + 1] == lane, m, origin)
    taken = origin >= 0
    origin = jnp.maximum(origin, 0)

    def from_sides(values):
        return jnp.where(left, pltpu.roll(values, 1, 0), pltpu.roll(values, n_z - 1, 0))

    listed = [take(field, origin) for field in fields[:6]]
    listed[0] = jnp.where(taken, listed[0], FAR)
    listed = [from_sides(values) for values in listed]
    listed[2] = listed[2] + jnp.where(left, -SIDE, SIDE)
    listed_key = from_sides(take(sorted_key, origin))
    side_at = jnp.where(fields[2] < 1.5, 0, HALF)

    def some_sides(step, summed):
        for u in range(TURNS_Z):
            index = side_at + (step * TURNS_Z + u)
            push = pair_force(
                fields[:6], sorted_key, [take(v, index) for v in listed], take(listed_key, index)
            )
            summed = tuple(summed[c] + push[c] for c in range(3))
        return summed

    summed = lax.fori_loop(0, HALF // TURNS_Z, some_sides, summed)
    for c in range(3):
        ranks[:, c, :] = summed[c]
    ranks[:, 3, :] = jnp.where(real, rank, rank + SLOTS).astype(jnp.float32)

    for z in opposite + [half * n_half + slot_at(k) for k in (2, 1, 3)]:
        copy(
            ranks.at[z], order_ref.at[gz], rank_send.at[0], rank_recv.at[0], device(gx, gy, z)
        ).start()
    pltpu.make_async_copy(ranks.at[gz], order_ref.at[gz], rank_recv.at[0]).start()

    across.wait_recv()
    spread(mirrored, 0, mirror + 1, 4)
    relay = jnp.logical_or(start, end)

    @pl.when(relay)
    def _():
        copy(
            edged, edged, send_sem.at[1], recv_sem.at[1], device(gx, gy, mirror)
        ).wait_recv()
        spread(edged, 0, jnp.where(start, n_z + 1, 0), 5)

    def bulk(count, sem):
        part = tiles_ref.at[pl.ds(0, 24 * count)]
        return copy(part, part, send_sem.at[sem], recv_sem.at[2], device(gx, gy, mirror))

    def bulk_rank(count):
        part = order_ref.at[pl.ds(0, count)]
        return copy(part, part, rank_send.at[0], rank_recv.at[0], device(gx, gy, mirror))

    bulk(3 * (n_z + 2), 3).wait_recv()
    bulk_rank(n_z).wait_recv()
    across.wait_send()
    bulk_rank(n_z - 1).wait_send()
    for sem in (3, 4):
        bulk(n_peers, sem).wait_send()

    @pl.when(relay)
    def _():
        bulk(n_peers, 5).wait_send()

    @pl.when(edge)
    def _():
        for h in (0, 1):
            to_edge(h, gy, 0).wait_send()


def exchange(groups, positions, velocities, keys, counts):
    n_z = groups[2]
    anywhere = pl.BlockSpec(memory_space=pl.ANY)
    slab = pltpu.VMEM((8 * (n_z // 2 + 2), SLOTS), jnp.float32)
    return pl.pallas_call(
        functools.partial(exchange_kernel, groups),
        out_shape=[
            pltpu.VMEM((72 * (n_z + 2), SLOTS), jnp.float32),
            pltpu.VMEM((n_z, 4, SLOTS), jnp.float32),
        ],
        in_specs=[anywhere] * 4,
        out_specs=[pl.BlockSpec(memory_space=pltpu.VMEM)] * 2,
        scratch_shapes=[
            pltpu.VMEM((3, n_z, SLOTS), jnp.float32),
            pltpu.VMEM((3, n_z, SLOTS), jnp.float32),
            pltpu.VMEM((n_z, SLOTS), jnp.int32),
            pltpu.SMEM((n_z,), jnp.int32),
            pltpu.VMEM((8 * (n_z + 2), SLOTS), jnp.float32),
            pltpu.VMEM((n_z, 4, SLOTS), jnp.float32),
            slab,
            slab,
            pltpu.SemaphoreType.DMA((4,)),
            pltpu.SemaphoreType.DMA((6,)),
            pltpu.SemaphoreType.DMA((3,)),
            pltpu.SemaphoreType.DMA((1,)),
            pltpu.SemaphoreType.DMA((1,)),
        ],
        compiler_params=pltpu.CompilerParams(collective_id=0, has_side_effects=True),
        name="sort_exchange",
    )(positions, velocities, keys, counts)


def runs_of(offset):
    spans = [{-1: (2, 3), 0: (0, 3), 1: (0, 1)}[o] for o in offset]
    runs = []
    for a in range(*spans[0]):
        for b in range(*spans[1]):
            low, high = a * 9 + b * 3 + spans[2][0], a * 9 + b * 3 + spans[2][1]
            if runs and runs[-1][1] == low:
                runs[-1] = (runs[-1][0], high)
            else:
                runs.append((low, high))
    return runs


def force_kernel(rows, tiles_ref, order_ref, out_ref):
    lane = lax.broadcasted_iota(jnp.int32, (rows, SLOTS), 1)
    left_half = lane < HALF

    def load(offset, f):
        ox, oy, oz = offset
        start = (((1 + ox) * (rows + 2) + 1 + oy) * 3 + 1 + oz) * 8 + f
        return tiles_ref[pl.ds(start, rows, stride=24), :]

    def join(high, low):
        return high.astype(jnp.int32) * 32768 + low.astype(jnp.int32)

    home = (0, 0, 0)
    own = [load(home, f) for f in range(6)]
    own_key = join(load(home, 6), load(home, 7))

    def pair(other, other_key, summed):
        push = pair_force(own, own_key, other, other_key)
        return tuple(summed[c] + push[c] for c in range(3))

    zero = jnp.zeros((rows, SLOTS), jnp.float32)
    summed = tuple(order_ref[:, c, :] for c in range(3))

    def count_cells(cells, low, high):
        inside = jnp.logical_and(cells >= low, cells < high)
        return jnp.sum(jnp.where(inside, 1.0, 0.0), axis=1, keepdims=True).astype(jnp.int32)

    def cells_of(x, y, z):
        cells = cell_of(x) * 9 + cell_of(y) * 3 + cell_of(z)
        return jnp.where(x > 0.5 * FAR, 27, cells)

    def tiles_beside(axis, side):
        ranges = [(0,)] * axis + [(side,)] + [(-1, 0, 1)] * (2 - axis)
        return [(ox, oy, oz) for ox in ranges[0] for oy in ranges[1] for oz in ranges[2]]

    def tables(axis, side):
        tiles = []
        total = jnp.zeros((rows, 1), jnp.int32)
        for offset in tiles_beside(axis, side):
            cells = cells_of(*(load(offset, f) for f in range(3)))
            table = []
            for low, high in runs_of(offset):
                begin = count_cells(cells, 0, low) if low else jnp.zeros_like(total)
                length = count_cells(cells, low, high)
                table.append((total, begin - total))
                total = total + length
            tiles.append((offset, table))
        return tiles, total

    def listed(tiles, total, at):
        alive = at < total
        packed = [jnp.full((rows, SLOTS), FAR, jnp.float32)] + [zero] * 5 + [jnp.zeros_like(lane)]
        for offset, table in tiles:
            index = at
            for base, shift in table:
                index = jnp.where(at >= base, at + shift, index)
            index = index & (SLOTS - 1)
            taken = jnp.logical_and(alive, at >= table[0][0])
            for f in range(7):
                if f < 6:
                    value = load(offset, f)
                else:
                    value = join(load(offset, 6), load(offset, 7))
                if f < 3 and offset[f]:
                    value = value + SIDE * offset[f]
                packed[f] = jnp.where(taken, take(value, index), packed[f])
        return packed

    def sweep(axis, lists, steps, summed):
        side_at = jnp.where(own[axis] < 1.5, 0, HALF)

        def some_steps(s, summed):
            for u in range(UNROLL):
                index = side_at + (s * UNROLL + u)
                other = [take(values, index) for values in lists[:6]]
                summed = pair(other, take(lists[6], index), summed)
            return summed

        steps = jnp.minimum(steps, HALF)
        return lax.fori_loop(0, (steps + UNROLL - 1) // UNROLL, some_steps, summed)

    def group(axis, summed):
        sides = [tables(axis, side) for side in (-1, 1)]
        longest = jnp.maximum(jnp.max(sides[0][1]), jnp.max(sides[1][1]))

        def one_pass(p, summed):
            at = lane + p * SLOTS
            lower, upper = (listed(tiles, total, at) for tiles, total in sides)
            left = longest - p * SLOTS
            lists = [
                jnp.where(left_half, a, pltpu.roll(b, HALF, 1)) for a, b in zip(lower, upper)
            ]
            summed = sweep(axis, lists, left, summed)
            lists = [
                jnp.where(left_half, pltpu.roll(a, HALF, 1), b) for a, b in zip(lower, upper)
            ]
            return sweep(axis, lists, left - HALF, summed)

        return lax.fori_loop(0, (longest + SLOTS - 1) // SLOTS, one_pass, summed)

    def rest_along_z(summed):
        lengths = [
            count_layer(load((0, 0, side), 0), load((0, 0, side), 2), side) for side in (-1, 1)
        ]
        longest = jnp.maximum(jnp.max(lengths[0]), jnp.max(lengths[1]))

        def second_half(_, summed):
            lower, upper = (listed(*tables(2, side), lane) for side in (-1, 1))
            lists = [
                jnp.where(left_half, pltpu.roll(a, HALF, 1), b) for a, b in zip(lower, upper)
            ]
            return sweep(2, lists, longest - HALF, summed)

        return lax.fori_loop(0, jnp.where(longest > HALF, 1, 0), second_half, summed)

    def count_layer(x, z, side):
        inside = jnp.logical_and(x < 0.5 * FAR, z >= 2.0 if side < 0 else z < 1.0)
        return jnp.sum(jnp.where(inside, 1.0, 0.0), axis=1, keepdims=True).astype(jnp.int32)

    for axis in range(2):
        summed = group(axis, summed)
    summed = rest_along_z(summed)

    order = order_ref[:, 3, :].astype(jnp.int32)
    scale = jnp.where(order < SLOTS, kick_scale, 0.0)
    order = order & (SLOTS - 1)
    for c in range(3):
        out_ref[c] = scale * take(summed[c], order)


def forces(n_z, tiles, order):
    vmem = pl.BlockSpec(memory_space=pltpu.VMEM)
    return pl.pallas_call(
        functools.partial(force_kernel, n_z),
        out_shape=jax.ShapeDtypeStruct((3, n_z, SLOTS), jnp.float32),
        in_specs=[vmem, vmem],
        out_specs=vmem,
        name="pair_forces",
    )(*(pltpu.with_memory_space_constraint(x, pltpu.VMEM) for x in (tiles, order)))


def solution(mesh):
    groups = tuple(mesh.shape[a] for a in ("gx", "gy", "gz"))
    n_z = groups[2]

    def on_device(positions, velocities, bead_keys, counts):
        tiles, order = exchange(
            groups,
            positions.reshape(3, n_z, SLOTS),
            velocities.reshape(3, n_z, SLOTS),
            bead_keys.reshape(n_z, SLOTS),
            counts.reshape(n_z),
        )
        kick = forces(n_z, tiles, order)
        return kick.reshape(3, 1, n_z, 1, SLOTS)

    in_specs = (
        P(None, "gx", ("gy", "gz"), None, None),
        P(None, "gx", ("gy", "gz"), None, None),
        P("gx", ("gy", "gz"), None, None),
        P("gx", ("gy", "gz"), None),
    )
    out_specs = P(None, "gx", "gy", "gz", None)
    return jax.shard_map(
        on_device, mesh=mesh, in_specs=in_specs, out_specs=out_specs, check_vma=False
    )
```

```python
import functools

import jax
import jax.numpy as jnp
from jax import lax
from jax.experimental import pallas as pl
from jax.experimental.pallas import tpu as pltpu
from jax.sharding import PartitionSpec as P

MESH = pl.DeviceIdType.MESH
SIDE = 3.0
SLOTS = 128
FAR = 4096.0
HALF = 64
TURNS = 21
TURNS_Z = 16
UNROLL = 16
UNROLL_BOTH = 32
UNIT = 5461.0
CENTRE = 32768.0

soft_radius = 0.05
friction = 4.5
noise_amplitude = 15.0
like_repulsion = 25.0
unlike_extra = 15.0
kick_scale = 0.02
root_twelve = 3.4641016151377544


def take(values, index):
    return jnp.take_along_axis(values, index, axis=1, mode="promise_in_bounds")


def cell_of(part):
    return jnp.where(part >= 2.0, 2, jnp.where(part >= 1.0, 1, 0))


def halves(first, second):
    high = (first * UNIT + (CENTRE + 0.5)).astype(jnp.int32)
    low = (second * UNIT + (CENTRE + 0.5)).astype(jnp.int32)
    return high * 65536 + low


def as_own(x, y, z, vx, vy, vz, key):
    return x, y, z, vx * UNIT + CENTRE, vy * UNIT + CENTRE, vz * UNIT, key


def as_other(x, y, z, vx, vy, vz, key):
    return x, y, z, halves(vx, vy), vz * UNIT, key


def pair_force(own, other):
    own_key, other_key = own[6], other[5]
    sep = [own[c] - other[c] for c in range(3)]
    squared = sep[0] * sep[0] + sep[1] * sep[1] + sep[2] * sep[2]
    root = lax.rsqrt(jnp.maximum(squared, 1e-30))
    distance = squared * root
    inverse = jnp.minimum(root, 1.0 / soft_radius)
    weight = jnp.maximum(1.0 - distance, 0.0) * inverse
    other_vx = lax.shift_right_logical(other[3], 16).astype(jnp.float32)
    other_vy = (other[3] & 65535).astype(jnp.float32)
    along = sep[0] * (own[3] - other_vx)
    along = along + sep[1] * (own[4] - other_vy)
    along = along + sep[2] * (own[5] - other[4])
    mixed = own_key ^ other_key
    hashed = mixed * 1103515245 + (own_key + other_key) * 12345
    hashed = hashed ^ lax.shift_right_logical(hashed, 15)
    hashed = hashed * 747796405
    hashed = hashed ^ lax.shift_right_logical(hashed, 13)
    fraction = lax.shift_right_logical(hashed << 1, 8).astype(jnp.float32)
    scale = noise_amplitude * root_twelve / 16777216.0
    base = like_repulsion - 0.5 * noise_amplitude * root_twelve
    level = jnp.where((mixed & 1) == 0, base, base + unlike_extra)
    strength = weight * (fraction * scale + level - (friction / UNIT) * (weight * along))
    return [strength * sep[c] for c in range(3)]


def exchange_kernel(
    groups, pos_hbm, vel_hbm, key_hbm, count_hbm, tiles_ref, order_ref,
    pos_ref, vel_ref, key_ref, count_ref, stage, ranks, mirrored, edged,
    load_sem, send_sem, recv_sem, rank_send, rank_recv,
):
    n_x, n_y, n_z = groups
    n_half = n_z // 2
    gx, gy, gz = lax.axis_index("gx"), lax.axis_index("gy"), lax.axis_index("gz")
    half, along = gz // n_half, lax.rem(gz, n_half)
    mirror = lax.rem(gz + n_half, n_z)
    first, last = gz == 0, gz == n_z - 1
    start, end = along == 0, along == n_half - 1
    above, below = lax.rem(gy + 1, n_y), lax.rem(gy + n_y - 1, n_y)
    columns = [lax.rem(gx + n_x + dx, n_x) for dx in (-1, 0, 1)]
    peers = [(k, dx) for k in (2, 1, 3, 0) for dx in (-1, 0, 1) if (k, dx) != (0, 0)]

    def slot_at(k):
        return lax.rem(along + k, n_half)

    def device(x, y, z):
        return {"gx": x, "gy": y, "gz": z}

    barrier = pltpu.get_barrier_semaphore()

    def ready(target):
        pl.semaphore_signal(barrier, inc=1, device_id=target, device_id_type=MESH)

    opposite = [lax.rem(mirror // n_half * n_half + slot_at(k), n_z) for k in (2, 1, 3, 0)]
    for z in opposite:
        ready(device(gx, gy, z))
    for k, dx in peers:
        ready(device(columns[dx + 1], gy, half * n_half + slot_at(k)))

    @pl.when(start)
    def _():
        ready(device(gx, above, jnp.int32(0)))

    @pl.when(end)
    def _():
        ready(device(gx, below, jnp.int32(n_z - 1)))

    loads = [
        pltpu.make_async_copy(source, target, load_sem.at[i])
        for i, (source, target) in enumerate(
            [(pos_hbm, pos_ref), (count_hbm, count_ref), (key_hbm, key_ref), (vel_hbm, vel_ref)]
        )
    ]
    for load in loads:
        load.start()
    for load in loads:
        load.wait()

    lane = lax.broadcasted_iota(jnp.int32, (n_z, SLOTS), 1)
    row = lax.broadcasted_iota(jnp.int32, (n_z, SLOTS), 0)
    occupancy = jnp.zeros((n_z, SLOTS), jnp.int32)
    for z in range(n_z):
        occupancy = jnp.where(row == z, count_ref[z], occupancy)
    px, py, pz = pos_ref[0], pos_ref[1], pos_ref[2]
    cell = cell_of(px) * 9 + cell_of(py) * 3 + cell_of(pz)
    cell = jnp.where(lane < occupancy, cell, 27)
    order = cell * SLOTS + lane
    rank = jnp.zeros((n_z, SLOTS), jnp.int32)
    for m in range(SLOTS):
        rank = rank + jnp.where(order[:, m : m + 1] < order, 1, 0)
    source = jnp.zeros((n_z, SLOTS), jnp.int32)
    for m in range(SLOTS):
        source = jnp.where(rank[:, m : m + 1] == lane, m, source)
    real = lane < occupancy
    key = key_ref[...]
    fields = [
        jnp.where(real, take(px, source), FAR),
        take(py, source),
        take(pz, source),
        take(vel_ref[0], source),
        take(vel_ref[1], source),
        take(vel_ref[2], source),
        take(lax.shift_right_logical(key, 15).astype(jnp.float32), source),
        take((key & 32767).astype(jnp.float32), source),
    ]
    for f, field in enumerate(fields):
        stage[pl.ds(8 + f, n_z, stride=8), :] = field
        stage[pl.ds(f, 1), :] = field[n_z - 1 : n_z]
        stage[pl.ds(8 * (n_z + 1) + f, 1), :] = field[0:1]

    edge = jnp.logical_or(first, last)
    n_peers = len(peers)
    pl.semaphore_wait(barrier, jnp.where(edge, n_peers + 6, n_peers + 4))

    def copy(source, target, send, recv, to):
        return pltpu.make_async_remote_copy(
            src_ref=source, dst_ref=target, send_sem=send, recv_sem=recv,
            device_id=to, device_id_type=MESH,
        )

    def slab(h):
        return stage.at[pl.ds(pl.multiple_of(8 * n_half * h, 8), 8 * (n_half + 2)), :]

    across = copy(slab(1 - half), mirrored, send_sem.at[0], recv_sem.at[0], device(gx, gy, mirror))
    across.start()
    def to_edge(h, y, position):
        return copy(
            slab(h), edged, send_sem.at[1 + h], recv_sem.at[1], device(gx, y, n_half * h + position)
        )

    @pl.when(first)
    def _():
        for h in (0, 1):
            to_edge(h, below, 0).start()

    @pl.when(last)
    def _():
        for h in (0, 1):
            to_edge(h, above, n_half - 1).start()

    def landing(slot):
        return tiles_ref.at[pl.ds(pl.multiple_of(24 * slot, 8), 24), :]

    def spread(buffer, offset, row_at, sem):
        def block(position):
            at = pl.multiple_of(8 * (offset + position), 8)
            return buffer.at[pl.ds(at, 24), :]

        for k, dx in peers:
            copy(
                block(slot_at(k)), landing((1 - dx) * (n_z + 2) + row_at),
                send_sem.at[sem], recv_sem.at[2],
                device(columns[dx + 1], gy, half * n_half + slot_at(k)),
            ).start()
        pltpu.make_async_copy(
            block(along), landing(n_z + 2 + row_at), recv_sem.at[2]
        ).start()

    spread(stage, half * n_half, gz + 1, 3)
    sorted_key = take(key, source)

    own = as_own(*fields[:6], sorted_key)
    words = as_other(*fields[:6], sorted_key)

    def turned(shift):
        return pair_force(own, [pltpu.roll(word, SLOTS - shift, 1) for word in words])

    def some_turns(step, summed):
        for u in range(TURNS):
            shift = step * TURNS + (u + 1)
            push = turned(shift)
            summed = tuple(
                summed[c] + (push[c] - pltpu.roll(push[c], shift, 1)) for c in range(3)
            )
        return summed

    zero = jnp.zeros((n_z, SLOTS), jnp.float32)
    summed = lax.fori_loop(0, (SLOTS // 2 - 1) // TURNS, some_turns, (zero, zero, zero))
    last_push = turned(SLOTS // 2)
    summed = tuple(summed[c] + last_push[c] for c in range(3))

    left = lane < HALF
    inside = fields[0] < 0.5 * FAR
    top = jnp.logical_and(inside, fields[2] >= 2.0)
    bottom = jnp.logical_and(inside, fields[2] < 1.0)
    member = jnp.where(top, 1, jnp.where(bottom, 2 * SLOTS, 0))
    before = jnp.zeros((n_z, SLOTS), jnp.int32)
    for m in range(SLOTS):
        before = before + jnp.where(lane > m, member[:, m : m + 1], 0)
    low, high = before & (2 * SLOTS - 1), lax.shift_right_logical(before, 8)
    seat = jnp.where(jnp.logical_and(bottom, high < HALF), high + HALF, SLOTS)
    seat = jnp.where(jnp.logical_and(top, low < HALF), low, seat)
    origin = jnp.full((n_z, SLOTS), -1, jnp.int32)
    for m in range(SLOTS):
        origin = jnp.where(seat[:, m : m + 1] == lane, m, origin)
    taken = origin >= 0
    origin = jnp.maximum(origin, 0)

    def from_sides(values):
        return jnp.where(left, pltpu.roll(values, 1, 0), pltpu.roll(values, n_z - 1, 0))

    listed = [take(word, origin) for word in words]
    listed[0] = jnp.where(taken, listed[0], FAR)
    listed = [from_sides(values) for values in listed]
    listed[2] = listed[2] + jnp.where(left, -SIDE, SIDE)
    side_at = jnp.where(fields[2] < 1.5, 0, HALF)

    def some_sides(step, summed):
        for u in range(TURNS_Z):
            index = side_at + (step * TURNS_Z + u)
            push = pair_force(own, [take(values, index) for values in listed])
            summed = tuple(summed[c] + push[c] for c in range(3))
        return summed

    summed = lax.fori_loop(0, HALF // TURNS_Z, some_sides, summed)
    for c in range(3):
        ranks[:, c, :] = summed[c]
    ranks[:, 3, :] = jnp.where(real, rank, rank + SLOTS).astype(jnp.float32)

    for z in opposite + [half * n_half + slot_at(k) for k in (2, 1, 3)]:
        copy(
            ranks.at[z], order_ref.at[gz], rank_send.at[0], rank_recv.at[0], device(gx, gy, z)
        ).start()
    pltpu.make_async_copy(ranks.at[gz], order_ref.at[gz], rank_recv.at[0]).start()

    across.wait_recv()
    spread(mirrored, 0, mirror + 1, 4)
    relay = jnp.logical_or(start, end)

    @pl.when(relay)
    def _():
        copy(
            edged, edged, send_sem.at[1], recv_sem.at[1], device(gx, gy, mirror)
        ).wait_recv()
        spread(edged, 0, jnp.where(start, n_z + 1, 0), 5)

    def bulk(count, sem):
        part = tiles_ref.at[pl.ds(0, 24 * count)]
        return copy(part, part, send_sem.at[sem], recv_sem.at[2], device(gx, gy, mirror))

    def bulk_rank(count):
        part = order_ref.at[pl.ds(0, count)]
        return copy(part, part, rank_send.at[0], rank_recv.at[0], device(gx, gy, mirror))

    bulk(3 * (n_z + 2), 3).wait_recv()
    bulk_rank(n_z).wait_recv()
    across.wait_send()
    bulk_rank(n_z - 1).wait_send()
    for sem in (3, 4):
        bulk(n_peers, sem).wait_send()

    @pl.when(relay)
    def _():
        bulk(n_peers, 5).wait_send()

    @pl.when(edge)
    def _():
        for h in (0, 1):
            to_edge(h, gy, 0).wait_send()


def exchange(groups, positions, velocities, keys, counts):
    n_z = groups[2]
    anywhere = pl.BlockSpec(memory_space=pl.ANY)
    slab = pltpu.VMEM((8 * (n_z // 2 + 2), SLOTS), jnp.float32)
    return pl.pallas_call(
        functools.partial(exchange_kernel, groups),
        out_shape=[
            pltpu.VMEM((72 * (n_z + 2), SLOTS), jnp.float32),
            pltpu.VMEM((n_z, 4, SLOTS), jnp.float32),
        ],
        in_specs=[anywhere] * 4,
        out_specs=[pl.BlockSpec(memory_space=pltpu.VMEM)] * 2,
        scratch_shapes=[
            pltpu.VMEM((3, n_z, SLOTS), jnp.float32),
            pltpu.VMEM((3, n_z, SLOTS), jnp.float32),
            pltpu.VMEM((n_z, SLOTS), jnp.int32),
            pltpu.SMEM((n_z,), jnp.int32),
            pltpu.VMEM((8 * (n_z + 2), SLOTS), jnp.float32),
            pltpu.VMEM((n_z, 4, SLOTS), jnp.float32),
            slab,
            slab,
            pltpu.SemaphoreType.DMA((4,)),
            pltpu.SemaphoreType.DMA((6,)),
            pltpu.SemaphoreType.DMA((3,)),
            pltpu.SemaphoreType.DMA((1,)),
            pltpu.SemaphoreType.DMA((1,)),
        ],
        compiler_params=pltpu.CompilerParams(collective_id=0, has_side_effects=True),
        name="sort_exchange",
    )(positions, velocities, keys, counts)


def runs_of(offset):
    spans = [{-1: (2, 3), 0: (0, 3), 1: (0, 1)}[o] for o in offset]
    runs = []
    for a in range(*spans[0]):
        for b in range(*spans[1]):
            low, high = a * 9 + b * 3 + spans[2][0], a * 9 + b * 3 + spans[2][1]
            if runs and runs[-1][1] == low:
                runs[-1] = (runs[-1][0], high)
            else:
                runs.append((low, high))
    return runs


def force_kernel(rows, tiles_ref, order_ref, out_ref):
    lane = lax.broadcasted_iota(jnp.int32, (rows, SLOTS), 1)
    left_half = lane < HALF

    def load(offset, f):
        ox, oy, oz = offset
        start = (((1 + ox) * (rows + 2) + 1 + oy) * 3 + 1 + oz) * 8 + f
        return tiles_ref[pl.ds(start, rows, stride=24), :]

    def join(high, low):
        return high.astype(jnp.int32) * 32768 + low.astype(jnp.int32)

    def beads(offset):
        return [load(offset, f) for f in range(6)] + [join(load(offset, 6), load(offset, 7))]

    own = as_own(*beads((0, 0, 0)))

    def pair(other, summed):
        push = pair_force(own, other)
        return tuple(summed[c] + push[c] for c in range(3))

    zero = jnp.zeros((rows, SLOTS), jnp.float32)
    summed = tuple(order_ref[:, c, :] for c in range(3))

    def count_cells(cells, low, high):
        inside = jnp.logical_and(cells >= low, cells < high)
        return jnp.sum(jnp.where(inside, 1.0, 0.0), axis=1, keepdims=True).astype(jnp.int32)

    def cells_of(x, y, z):
        cells = cell_of(x) * 9 + cell_of(y) * 3 + cell_of(z)
        return jnp.where(x > 0.5 * FAR, 27, cells)

    def tiles_beside(axis, side):
        ranges = [(0,)] * axis + [(side,)] + [(-1, 0, 1)] * (2 - axis)
        return [(ox, oy, oz) for ox in ranges[0] for oy in ranges[1] for oz in ranges[2]]

    def tables(axis, side):
        tiles = []
        total = jnp.zeros((rows, 1), jnp.int32)
        for offset in tiles_beside(axis, side):
            cells = cells_of(*(load(offset, f) for f in range(3)))
            table = []
            for low, high in runs_of(offset):
                begin = count_cells(cells, 0, low) if low else jnp.zeros_like(total)
                length = count_cells(cells, low, high)
                table.append((total, begin - total))
                total = total + length
            tiles.append((offset, table))
        return tiles, total

    def listed(tiles, total, at):
        alive = at < total
        blank = jnp.zeros_like(lane)
        packed = [jnp.full((rows, SLOTS), FAR, jnp.float32), zero, zero, blank, zero, blank]
        for offset, table in tiles:
            index = at
            for base, shift in table:
                index = jnp.where(at >= base, at + shift, index)
            index = index & (SLOTS - 1)
            taken = jnp.logical_and(alive, at >= table[0][0])
            for f, value in enumerate(as_other(*beads(offset))):
                if f < 3 and offset[f]:
                    value = value + SIDE * offset[f]
                packed[f] = jnp.where(taken, take(value, index), packed[f])
        return packed

    def sweep(jobs, first, last, unroll, summed):
        def some_steps(s, summed):
            for u in range(unroll):
                for axis, lists in jobs:
                    index = side_at[axis] + (s * unroll + u)
                    summed = pair([take(values, index) for values in lists], summed)
            return summed

        return lax.fori_loop(first // unroll, (last + unroll - 1) // unroll, some_steps, summed)

    side_at = [jnp.where(own[axis] < 1.5, 0, HALF) for axis in range(3)]

    def merged(lower, upper, half):
        return [
            jnp.where(left_half, a if half == 0 else pltpu.roll(a, HALF, 1),
                      pltpu.roll(b, HALF, 1) if half == 0 else b)
            for a, b in zip(lower, upper)
        ]

    def along_x_and_y(summed):
        sides = [[tables(axis, side) for side in (-1, 1)] for axis in (0, 1)]
        longest = [jnp.maximum(jnp.max(a[1]), jnp.max(b[1])) for a, b in sides]

        def one_pass(p, summed):
            at = lane + p * SLOTS
            packed = [[listed(tiles, total, at) for tiles, total in pairs] for pairs in sides]
            for half in (0, 1):
                jobs = [(axis, merged(*packed[axis], half)) for axis in (0, 1)]
                steps = [
                    jnp.clip(longest[axis] - p * SLOTS - half * HALF, 0, HALF) for axis in (0, 1)
                ]
                if half == 0:
                    both = jnp.maximum(steps[0], steps[1])
                    summed = sweep(jobs, 0, both, UNROLL_BOTH, summed)
                else:
                    both = (jnp.minimum(steps[0], steps[1]) + UNROLL - 1) // UNROLL * UNROLL
                    summed = sweep(jobs, 0, both, UNROLL, summed)
                    for axis in (0, 1):
                        summed = sweep(jobs[axis : axis + 1], both, steps[axis], UNROLL, summed)
            return summed

        passes = (jnp.maximum(longest[0], longest[1]) + SLOTS - 1) // SLOTS
        return lax.fori_loop(0, passes, one_pass, summed)

    def rest_along_z(summed):
        lengths = [
            count_layer(load((0, 0, side), 0), load((0, 0, side), 2), side) for side in (-1, 1)
        ]
        longest = jnp.maximum(jnp.max(lengths[0]), jnp.max(lengths[1]))

        def second_half(_, summed):
            lists = merged(*(listed(*tables(2, side), lane) for side in (-1, 1)), 1)
            return sweep([(2, lists)], 0, longest - HALF, UNROLL, summed)

        return lax.fori_loop(0, jnp.where(longest > HALF, 1, 0), second_half, summed)

    def count_layer(x, z, side):
        inside = jnp.logical_and(x < 0.5 * FAR, z >= 2.0 if side < 0 else z < 1.0)
        return jnp.sum(jnp.where(inside, 1.0, 0.0), axis=1, keepdims=True).astype(jnp.int32)

    summed = along_x_and_y(summed)
    summed = rest_along_z(summed)

    order = order_ref[:, 3, :].astype(jnp.int32)
    scale = jnp.where(order < SLOTS, kick_scale, 0.0)
    order = order & (SLOTS - 1)
    for c in range(3):
        out_ref[c] = scale * take(summed[c], order)


def forces(n_z, tiles, order):
    vmem = pl.BlockSpec(memory_space=pltpu.VMEM)
    return pl.pallas_call(
        functools.partial(force_kernel, n_z),
        out_shape=jax.ShapeDtypeStruct((3, n_z, SLOTS), jnp.float32),
        in_specs=[vmem, vmem],
        out_specs=vmem,
        name="pair_forces",
    )(*(pltpu.with_memory_space_constraint(x, pltpu.VMEM) for x in (tiles, order)))


def solution(mesh):
    groups = tuple(mesh.shape[a] for a in ("gx", "gy", "gz"))
    n_z = groups[2]

    def on_device(positions, velocities, bead_keys, counts):
        tiles, order = exchange(
            groups,
            positions.reshape(3, n_z, SLOTS),
            velocities.reshape(3, n_z, SLOTS),
            bead_keys.reshape(n_z, SLOTS),
            counts.reshape(n_z),
        )
        kick = forces(n_z, tiles, order)
        return kick.reshape(3, 1, n_z, 1, SLOTS)

    in_specs = (
        P(None, "gx", ("gy", "gz"), None, None),
        P(None, "gx", ("gy", "gz"), None, None),
        P("gx", ("gy", "gz"), None, None),
        P("gx", ("gy", "gz"), None),
    )
    out_specs = P(None, "gx", "gy", "gz", None)
    return jax.shard_map(
        on_device, mesh=mesh, in_specs=in_specs, out_specs=out_specs, check_vma=False
    )
```

```python
import functools

import jax
import jax.numpy as jnp
from jax import lax
from jax.experimental import pallas as pl
from jax.experimental.pallas import tpu as pltpu
from jax.sharding import PartitionSpec as P

MESH = pl.DeviceIdType.MESH
SIDE = 3.0
SLOTS = 128
FAR = 4096.0
HALF = 64
TURNS = 21
TURNS_Z = 64
UNROLL = 16
UNIT = 5461.0
CENTRE = 32768.0

soft_radius = 0.05
friction = 4.5
noise_amplitude = 15.0
like_repulsion = 25.0
unlike_extra = 15.0
kick_scale = 0.02
root_twelve = 3.4641016151377544


def take(values, index):
    return jnp.take_along_axis(values, index, axis=1, mode="promise_in_bounds")


def cell_of(part):
    return jnp.where(part >= 2.0, 2, jnp.where(part >= 1.0, 1, 0))


def halves(first, second):
    high = (first * UNIT + (CENTRE + 0.5)).astype(jnp.int32)
    low = (second * UNIT + (CENTRE + 0.5)).astype(jnp.int32)
    return high * 65536 + low


def as_own(x, y, z, vx, vy, vz, key):
    return x, y, z, vx * UNIT + CENTRE, vy * UNIT + CENTRE, vz * UNIT, key


def as_other(x, y, z, vx, vy, vz, key):
    return x, y, z, halves(vx, vy), vz * UNIT, key


def pair_force(own, other):
    own_key, other_key = own[6], other[5]
    sep = [own[c] - other[c] for c in range(3)]
    squared = sep[0] * sep[0] + sep[1] * sep[1] + sep[2] * sep[2]
    root = lax.rsqrt(jnp.maximum(squared, 1e-30))
    distance = squared * root
    inverse = jnp.minimum(root, 1.0 / soft_radius)
    weight = jnp.maximum(1.0 - distance, 0.0) * inverse
    other_vx = lax.shift_right_logical(other[3], 16).astype(jnp.float32)
    other_vy = (other[3] & 65535).astype(jnp.float32)
    along = sep[0] * (own[3] - other_vx)
    along = along + sep[1] * (own[4] - other_vy)
    along = along + sep[2] * (own[5] - other[4])
    mixed = own_key ^ other_key
    hashed = mixed * 1103515245 + (own_key + other_key) * 12345
    hashed = hashed ^ lax.shift_right_logical(hashed, 15)
    hashed = hashed * 747796405
    hashed = hashed ^ lax.shift_right_logical(hashed, 13)
    fraction = lax.shift_right_logical(hashed << 1, 8).astype(jnp.float32)
    scale = noise_amplitude * root_twelve / 16777216.0
    base = like_repulsion - 0.5 * noise_amplitude * root_twelve
    level = jnp.where((mixed & 1) == 0, base, base + unlike_extra)
    strength = weight * (fraction * scale + level - (friction / UNIT) * (weight * along))
    return [strength * sep[c] for c in range(3)]


def exchange_kernel(
    groups, pos_hbm, vel_hbm, key_hbm, count_hbm, tiles_ref, order_ref,
    pos_ref, vel_ref, key_ref, count_ref, stage, ranks, mirrored, edged,
    load_sem, send_sem, recv_sem, rank_send, rank_recv,
):
    n_x, n_y, n_z = groups
    n_half = n_z // 2
    gx, gy, gz = lax.axis_index("gx"), lax.axis_index("gy"), lax.axis_index("gz")
    half, along = gz // n_half, lax.rem(gz, n_half)
    mirror = lax.rem(gz + n_half, n_z)
    first, last = gz == 0, gz == n_z - 1
    start, end = along == 0, along == n_half - 1
    above, below = lax.rem(gy + 1, n_y), lax.rem(gy + n_y - 1, n_y)
    columns = [lax.rem(gx + n_x + dx, n_x) for dx in (-1, 0, 1)]
    peers = [(k, dx) for k in (2, 1, 3, 0) for dx in (-1, 0, 1) if (k, dx) != (0, 0)]

    def slot_at(k):
        return lax.rem(along + k, n_half)

    def device(x, y, z):
        return {"gx": x, "gy": y, "gz": z}

    barrier = pltpu.get_barrier_semaphore()

    def ready(target):
        pl.semaphore_signal(barrier, inc=1, device_id=target, device_id_type=MESH)

    opposite = [lax.rem(mirror // n_half * n_half + slot_at(k), n_z) for k in (2, 1, 3, 0)]
    for z in opposite:
        ready(device(gx, gy, z))
    for k, dx in peers:
        ready(device(columns[dx + 1], gy, half * n_half + slot_at(k)))

    @pl.when(start)
    def _():
        ready(device(gx, above, jnp.int32(0)))

    @pl.when(end)
    def _():
        ready(device(gx, below, jnp.int32(n_z - 1)))

    loads = [
        pltpu.make_async_copy(source, target, load_sem.at[i])
        for i, (source, target) in enumerate(
            [(pos_hbm, pos_ref), (count_hbm, count_ref), (key_hbm, key_ref), (vel_hbm, vel_ref)]
        )
    ]
    for load in loads:
        load.start()
    for load in loads:
        load.wait()

    lane = lax.broadcasted_iota(jnp.int32, (n_z, SLOTS), 1)
    row = lax.broadcasted_iota(jnp.int32, (n_z, SLOTS), 0)
    occupancy = jnp.zeros((n_z, SLOTS), jnp.int32)
    for z in range(n_z):
        occupancy = jnp.where(row == z, count_ref[z], occupancy)
    px, py, pz = pos_ref[0], pos_ref[1], pos_ref[2]
    cell = cell_of(px) * 9 + cell_of(py) * 3 + cell_of(pz)
    cell = jnp.where(lane < occupancy, cell, 27)
    order = cell * SLOTS + lane
    rank = jnp.zeros((n_z, SLOTS), jnp.int32)
    for m in range(SLOTS):
        rank = rank + jnp.where(order[:, m : m + 1] < order, 1, 0)
    source = jnp.zeros((n_z, SLOTS), jnp.int32)
    for m in range(SLOTS):
        source = jnp.where(rank[:, m : m + 1] == lane, m, source)
    real = lane < occupancy
    key = key_ref[...]
    fields = [
        jnp.where(real, take(px, source), FAR),
        take(py, source),
        take(pz, source),
        take(vel_ref[0], source),
        take(vel_ref[1], source),
        take(vel_ref[2], source),
        take(lax.shift_right_logical(key, 15).astype(jnp.float32), source),
        take((key & 32767).astype(jnp.float32), source),
    ]
    for f, field in enumerate(fields):
        stage[pl.ds(8 + f, n_z, stride=8), :] = field
        stage[pl.ds(f, 1), :] = field[n_z - 1 : n_z]
        stage[pl.ds(8 * (n_z + 1) + f, 1), :] = field[0:1]

    edge = jnp.logical_or(first, last)
    n_peers = len(peers)
    pl.semaphore_wait(barrier, jnp.where(edge, n_peers + 6, n_peers + 4))

    def copy(source, target, send, recv, to):
        return pltpu.make_async_remote_copy(
            src_ref=source, dst_ref=target, send_sem=send, recv_sem=recv,
            device_id=to, device_id_type=MESH,
        )

    def slab(h):
        return stage.at[pl.ds(pl.multiple_of(8 * n_half * h, 8), 8 * (n_half + 2)), :]

    across = copy(slab(1 - half), mirrored, send_sem.at[0], recv_sem.at[0], device(gx, gy, mirror))
    across.start()
    def to_edge(h, y, position):
        return copy(
            slab(h), edged, send_sem.at[1 + h], recv_sem.at[1], device(gx, y, n_half * h + position)
        )

    @pl.when(first)
    def _():
        for h in (0, 1):
            to_edge(h, below, 0).start()

    @pl.when(last)
    def _():
        for h in (0, 1):
            to_edge(h, above, n_half - 1).start()

    def landing(slot):
        return tiles_ref.at[pl.ds(pl.multiple_of(24 * slot, 8), 24), :]

    def spread(buffer, offset, row_at, sem):
        def block(position):
            at = pl.multiple_of(8 * (offset + position), 8)
            return buffer.at[pl.ds(at, 24), :]

        for k, dx in peers:
            copy(
                block(slot_at(k)), landing((1 - dx) * (n_z + 2) + row_at),
                send_sem.at[sem], recv_sem.at[2],
                device(columns[dx + 1], gy, half * n_half + slot_at(k)),
            ).start()
        pltpu.make_async_copy(
            block(along), landing(n_z + 2 + row_at), recv_sem.at[2]
        ).start()

    spread(stage, half * n_half, gz + 1, 3)
    sorted_key = take(key, source)

    own = as_own(*fields[:6], sorted_key)
    words = as_other(*fields[:6], sorted_key)

    def turned(shift):
        return pair_force(own, [pltpu.roll(word, SLOTS - shift, 1) for word in words])

    def some_turns(step, summed):
        for u in range(TURNS):
            shift = step * TURNS + (u + 1)
            push = turned(shift)
            summed = tuple(
                summed[c] + (push[c] - pltpu.roll(push[c], shift, 1)) for c in range(3)
            )
        return summed

    zero = jnp.zeros((n_z, SLOTS), jnp.float32)
    summed = lax.fori_loop(0, (SLOTS // 2 - 1) // TURNS, some_turns, (zero, zero, zero))
    last_push = turned(SLOTS // 2)
    summed = tuple(summed[c] + last_push[c] for c in range(3))

    left = lane < HALF
    inside = fields[0] < 0.5 * FAR
    top = jnp.logical_and(inside, fields[2] >= 2.0)
    bottom = jnp.logical_and(inside, fields[2] < 1.0)
    member = jnp.where(top, 1, jnp.where(bottom, 2 * SLOTS, 0))
    before = jnp.zeros((n_z, SLOTS), jnp.int32)
    for m in range(SLOTS):
        before = before + jnp.where(lane > m, member[:, m : m + 1], 0)
    low, high = before & (2 * SLOTS - 1), lax.shift_right_logical(before, 8)
    seat = jnp.where(jnp.logical_and(bottom, high < HALF), high + HALF, SLOTS)
    seat = jnp.where(jnp.logical_and(top, low < HALF), low, seat)
    origin = jnp.full((n_z, SLOTS), -1, jnp.int32)
    for m in range(SLOTS):
        origin = jnp.where(seat[:, m : m + 1] == lane, m, origin)
    taken = origin >= 0
    origin = jnp.maximum(origin, 0)

    def from_sides(values):
        return jnp.where(left, pltpu.roll(values, 1, 0), pltpu.roll(values, n_z - 1, 0))

    listed = [take(word, origin) for word in words]
    listed[0] = jnp.where(taken, listed[0], FAR)
    listed = [from_sides(values) for values in listed]
    listed[2] = listed[2] + jnp.where(left, -SIDE, SIDE)
    side_at = jnp.where(fields[2] < 1.5, 0, HALF)

    def some_sides(step, summed):
        for u in range(TURNS_Z):
            index = side_at + (step * TURNS_Z + u)
            push = pair_force(own, [take(values, index) for values in listed])
            summed = tuple(summed[c] + push[c] for c in range(3))
        return summed

    summed = some_sides(0, summed)
    for c in range(3):
        ranks[:, c, :] = summed[c]
    ranks[:, 3, :] = jnp.where(real, rank, rank + SLOTS).astype(jnp.float32)

    for z in opposite + [half * n_half + slot_at(k) for k in (2, 1, 3)]:
        copy(
            ranks.at[z], order_ref.at[gz], rank_send.at[0], rank_recv.at[0], device(gx, gy, z)
        ).start()
    pltpu.make_async_copy(ranks.at[gz], order_ref.at[gz], rank_recv.at[0]).start()

    across.wait_recv()
    spread(mirrored, 0, mirror + 1, 4)
    relay = jnp.logical_or(start, end)

    @pl.when(relay)
    def _():
        copy(
            edged, edged, send_sem.at[1], recv_sem.at[1], device(gx, gy, mirror)
        ).wait_recv()
        spread(edged, 0, jnp.where(start, n_z + 1, 0), 5)

    def bulk(count, sem):
        part = tiles_ref.at[pl.ds(0, 24 * count)]
        return copy(part, part, send_sem.at[sem], recv_sem.at[2], device(gx, gy, mirror))

    def bulk_rank(count):
        part = order_ref.at[pl.ds(0, count)]
        return copy(part, part, rank_send.at[0], rank_recv.at[0], device(gx, gy, mirror))

    bulk(3 * (n_z + 2), 3).wait_recv()
    bulk_rank(n_z).wait_recv()
    across.wait_send()
    bulk_rank(n_z - 1).wait_send()
    for sem in (3, 4):
        bulk(n_peers, sem).wait_send()

    @pl.when(relay)
    def _():
        bulk(n_peers, 5).wait_send()

    @pl.when(edge)
    def _():
        for h in (0, 1):
            to_edge(h, gy, 0).wait_send()


def exchange(groups, positions, velocities, keys, counts):
    n_z = groups[2]
    anywhere = pl.BlockSpec(memory_space=pl.ANY)
    slab = pltpu.VMEM((8 * (n_z // 2 + 2), SLOTS), jnp.float32)
    return pl.pallas_call(
        functools.partial(exchange_kernel, groups),
        out_shape=[
            pltpu.VMEM((72 * (n_z + 2), SLOTS), jnp.float32),
            pltpu.VMEM((n_z, 4, SLOTS), jnp.float32),
        ],
        in_specs=[anywhere] * 4,
        out_specs=[pl.BlockSpec(memory_space=pltpu.VMEM)] * 2,
        scratch_shapes=[
            pltpu.VMEM((3, n_z, SLOTS), jnp.float32),
            pltpu.VMEM((3, n_z, SLOTS), jnp.float32),
            pltpu.VMEM((n_z, SLOTS), jnp.int32),
            pltpu.SMEM((n_z,), jnp.int32),
            pltpu.VMEM((8 * (n_z + 2), SLOTS), jnp.float32),
            pltpu.VMEM((n_z, 4, SLOTS), jnp.float32),
            slab,
            slab,
            pltpu.SemaphoreType.DMA((4,)),
            pltpu.SemaphoreType.DMA((6,)),
            pltpu.SemaphoreType.DMA((3,)),
            pltpu.SemaphoreType.DMA((1,)),
            pltpu.SemaphoreType.DMA((1,)),
        ],
        compiler_params=pltpu.CompilerParams(collective_id=0, has_side_effects=True),
        name="sort_exchange",
    )(positions, velocities, keys, counts)


def runs_of(offset):
    spans = [{-1: (2, 3), 0: (0, 3), 1: (0, 1)}[o] for o in offset]
    runs = []
    for a in range(*spans[0]):
        for b in range(*spans[1]):
            low, high = a * 9 + b * 3 + spans[2][0], a * 9 + b * 3 + spans[2][1]
            if runs and runs[-1][1] == low:
                runs[-1] = (runs[-1][0], high)
            else:
                runs.append((low, high))
    return runs


def force_kernel(rows, tiles_ref, order_ref, out_ref):
    lane = lax.broadcasted_iota(jnp.int32, (rows, SLOTS), 1)
    left_half = lane < HALF

    def load(offset, f):
        ox, oy, oz = offset
        start = (((1 + ox) * (rows + 2) + 1 + oy) * 3 + 1 + oz) * 8 + f
        return tiles_ref[pl.ds(start, rows, stride=24), :]

    def join(high, low):
        return high.astype(jnp.int32) * 32768 + low.astype(jnp.int32)

    def beads(offset):
        return [load(offset, f) for f in range(6)] + [join(load(offset, 6), load(offset, 7))]

    own = as_own(*beads((0, 0, 0)))

    def pair(other, summed):
        push = pair_force(own, other)
        return tuple(summed[c] + push[c] for c in range(3))

    zero = jnp.zeros((rows, SLOTS), jnp.float32)
    summed = tuple(order_ref[:, c, :] for c in range(3))

    def count_cells(cells, low, high):
        inside = jnp.logical_and(cells >= low, cells < high)
        return jnp.sum(jnp.where(inside, 1.0, 0.0), axis=1, keepdims=True).astype(jnp.int32)

    def cells_of(x, y, z):
        cells = cell_of(x) * 9 + cell_of(y) * 3 + cell_of(z)
        return jnp.where(x > 0.5 * FAR, 27, cells)

    def tiles_beside(axis, side):
        ranges = [(0,)] * axis + [(side,)] + [(-1, 0, 1)] * (2 - axis)
        return [(ox, oy, oz) for ox in ranges[0] for oy in ranges[1] for oz in ranges[2]]

    def tables(axis, side):
        tiles = []
        total = jnp.zeros((rows, 1), jnp.int32)
        for offset in tiles_beside(axis, side):
            cells = cells_of(*(load(offset, f) for f in range(3)))
            table = []
            for low, high in runs_of(offset):
                begin = count_cells(cells, 0, low) if low else jnp.zeros_like(total)
                length = count_cells(cells, low, high)
                table.append((total, begin - total))
                total = total + length
            tiles.append((offset, table))
        return tiles, total

    def listed(tiles, total, at):
        alive = at < total
        blank = jnp.zeros_like(lane)
        packed = [jnp.full((rows, SLOTS), FAR, jnp.float32), zero, zero, blank, zero, blank]
        for offset, table in tiles:
            index = at
            for base, shift in table:
                index = jnp.where(at >= base, at + shift, index)
            index = index & (SLOTS - 1)
            taken = jnp.logical_and(alive, at >= table[0][0])
            for f, value in enumerate(as_other(*beads(offset))):
                if f < 3 and offset[f]:
                    value = value + SIDE * offset[f]
                packed[f] = jnp.where(taken, take(value, index), packed[f])
        return packed

    def sweep(jobs, first, last, unroll, summed):
        def some_steps(s, summed):
            for u in range(unroll):
                for axis, lists in jobs:
                    index = side_at[axis] + (s * unroll + u)
                    summed = pair([take(values, index) for values in lists], summed)
            return summed

        if unroll == HALF:
            return some_steps(0, summed)
        return lax.fori_loop(first // unroll, (last + unroll - 1) // unroll, some_steps, summed)

    side_at = [jnp.where(own[axis] < 1.5, 0, HALF) for axis in range(3)]

    def merged(lower, upper, half):
        return [
            jnp.where(left_half, a if half == 0 else pltpu.roll(a, HALF, 1),
                      pltpu.roll(b, HALF, 1) if half == 0 else b)
            for a, b in zip(lower, upper)
        ]

    def along_x_and_y(summed):
        sides = [[tables(axis, side) for side in (-1, 1)] for axis in (0, 1)]
        longest = [jnp.maximum(jnp.max(a[1]), jnp.max(b[1])) for a, b in sides]

        def one_pass(p, summed):
            at = lane + p * SLOTS
            packed = [[listed(tiles, total, at) for tiles, total in pairs] for pairs in sides]
            for half in (0, 1):
                jobs = [(axis, merged(*packed[axis], half)) for axis in (0, 1)]
                steps = [
                    jnp.clip(longest[axis] - p * SLOTS - half * HALF, 0, HALF) for axis in (0, 1)
                ]
                if half == 0:
                    summed = sweep(jobs, 0, HALF, HALF, summed)
                else:
                    both = (jnp.minimum(steps[0], steps[1]) + UNROLL - 1) // UNROLL * UNROLL
                    summed = sweep(jobs, 0, both, UNROLL, summed)
                    for axis in (0, 1):
                        summed = sweep(jobs[axis : axis + 1], both, steps[axis], UNROLL, summed)
            return summed

        passes = (jnp.maximum(longest[0], longest[1]) + SLOTS - 1) // SLOTS
        return lax.fori_loop(0, passes, one_pass, summed)

    def rest_along_z(summed):
        lengths = [
            count_layer(load((0, 0, side), 0), load((0, 0, side), 2), side) for side in (-1, 1)
        ]
        longest = jnp.maximum(jnp.max(lengths[0]), jnp.max(lengths[1]))

        def second_half(_, summed):
            lists = merged(*(listed(*tables(2, side), lane) for side in (-1, 1)), 1)
            return sweep([(2, lists)], 0, longest - HALF, UNROLL, summed)

        return lax.fori_loop(0, jnp.where(longest > HALF, 1, 0), second_half, summed)

    def count_layer(x, z, side):
        inside = jnp.logical_and(x < 0.5 * FAR, z >= 2.0 if side < 0 else z < 1.0)
        return jnp.sum(jnp.where(inside, 1.0, 0.0), axis=1, keepdims=True).astype(jnp.int32)

    summed = along_x_and_y(summed)
    summed = rest_along_z(summed)

    order = order_ref[:, 3, :].astype(jnp.int32)
    scale = jnp.where(order < SLOTS, kick_scale, 0.0)
    order = order & (SLOTS - 1)
    for c in range(3):
        out_ref[c] = scale * take(summed[c], order)


def forces(n_z, tiles, order):
    vmem = pl.BlockSpec(memory_space=pltpu.VMEM)
    return pl.pallas_call(
        functools.partial(force_kernel, n_z),
        out_shape=jax.ShapeDtypeStruct((3, n_z, SLOTS), jnp.float32),
        in_specs=[vmem, vmem],
        out_specs=vmem,
        name="pair_forces",
    )(*(pltpu.with_memory_space_constraint(x, pltpu.VMEM) for x in (tiles, order)))


def solution(mesh):
    groups = tuple(mesh.shape[a] for a in ("gx", "gy", "gz"))
    n_z = groups[2]

    def on_device(positions, velocities, bead_keys, counts):
        tiles, order = exchange(
            groups,
            positions.reshape(3, n_z, SLOTS),
            velocities.reshape(3, n_z, SLOTS),
            bead_keys.reshape(n_z, SLOTS),
            counts.reshape(n_z),
        )
        kick = forces(n_z, tiles, order)
        return kick.reshape(3, 1, n_z, 1, SLOTS)

    in_specs = (
        P(None, "gx", ("gy", "gz"), None, None),
        P(None, "gx", ("gy", "gz"), None, None),
        P("gx", ("gy", "gz"), None, None),
        P("gx", ("gy", "gz"), None),
    )
    out_specs = P(None, "gx", "gy", "gz", None)
    return jax.shard_map(
        on_device, mesh=mesh, in_specs=in_specs, out_specs=out_specs, check_vma=False
    )
```

```python
import functools

import jax
import jax.numpy as jnp
from jax import lax
from jax.experimental import pallas as pl
from jax.experimental.pallas import tpu as pltpu
from jax.sharding import PartitionSpec as P

MESH = pl.DeviceIdType.MESH
SIDE = 3.0
SLOTS = 128
FAR = 4096.0
HALF = 64
TURNS = 21
TURNS_Z = 64
UNROLL = 16
UNIT = 5461.0
CENTRE = 32768.0

soft_radius = 0.05
friction = 4.5
noise_amplitude = 15.0
like_repulsion = 25.0
unlike_extra = 15.0
kick_scale = 0.02
root_twelve = 3.4641016151377544


def take(values, index):
    return jnp.take_along_axis(values, index, axis=1, mode="promise_in_bounds")


def cell_of(part):
    return jnp.where(part >= 2.0, 2, jnp.where(part >= 1.0, 1, 0))


def halves(first, second):
    high = (first * UNIT + (CENTRE + 0.5)).astype(jnp.int32)
    low = (second * UNIT + (CENTRE + 0.5)).astype(jnp.int32)
    return high * 65536 + low


def as_own(x, y, z, vx, vy, vz, key):
    return x, y, z, vx * UNIT + CENTRE, vy * UNIT + CENTRE, vz * UNIT, key


def as_other(x, y, z, vx, vy, vz, key):
    return x, y, z, halves(vx, vy), vz * UNIT, key


def pair_force(own, other):
    own_key, other_key = own[6], other[5]
    sep = [own[c] - other[c] for c in range(3)]
    squared = sep[0] * sep[0] + sep[1] * sep[1] + sep[2] * sep[2]
    root = lax.rsqrt(jnp.maximum(squared, 1e-30))
    distance = squared * root
    inverse = jnp.minimum(root, 1.0 / soft_radius)
    weight = jnp.maximum(1.0 - distance, 0.0) * inverse
    other_vx = lax.shift_right_logical(other[3], 16).astype(jnp.float32)
    other_vy = (other[3] & 65535).astype(jnp.float32)
    along = sep[0] * (own[3] - other_vx)
    along = along + sep[1] * (own[4] - other_vy)
    along = along + sep[2] * (own[5] - other[4])
    mixed = own_key ^ other_key
    hashed = mixed * 1103515245 + (own_key + other_key) * 12345
    hashed = hashed ^ lax.shift_right_logical(hashed, 15)
    hashed = hashed * 747796405
    hashed = hashed ^ lax.shift_right_logical(hashed, 13)
    fraction = lax.shift_right_logical(hashed << 1, 8).astype(jnp.float32)
    scale = noise_amplitude * root_twelve / 16777216.0
    base = like_repulsion - 0.5 * noise_amplitude * root_twelve
    level = jnp.where((mixed & 1) == 0, base, base + unlike_extra)
    strength = weight * (fraction * scale + level - (friction / UNIT) * (weight * along))
    return [strength * sep[c] for c in range(3)]


def exchange_kernel(
    groups, pos_hbm, vel_hbm, key_hbm, count_hbm, tiles_ref, order_ref,
    pos_ref, vel_ref, key_ref, count_ref, stage, ranks, mirrored, edged,
    load_sem, send_sem, recv_sem, rank_send, rank_recv, plane_sem,
):
    n_x, n_y, n_z = groups
    n_half = n_z // 2
    gx, gy, gz = lax.axis_index("gx"), lax.axis_index("gy"), lax.axis_index("gz")
    half, along = gz // n_half, lax.rem(gz, n_half)
    mirror = lax.rem(gz + n_half, n_z)
    first, last = gz == 0, gz == n_z - 1
    start, end = along == 0, along == n_half - 1
    above, below = lax.rem(gy + 1, n_y), lax.rem(gy + n_y - 1, n_y)
    columns = [lax.rem(gx + n_x + dx, n_x) for dx in (-1, 0, 1)]
    peers = [(k, dx) for k in (2, 1, 3, 0) for dx in (-1, 0, 1) if (k, dx) != (0, 0)]

    def slot_at(k):
        return lax.rem(along + k, n_half)

    def device(x, y, z):
        return {"gx": x, "gy": y, "gz": z}

    barrier = pltpu.get_barrier_semaphore()

    def ready(target):
        pl.semaphore_signal(barrier, inc=1, device_id=target, device_id_type=MESH)

    other_half = 1 - half
    opposite = [n_half * other_half + slot_at(k) for k in (2, 1, 3, 0)]
    early, late = half == 0, half == 1

    @pl.when(early)
    def _():
        for k, dx in peers:
            ready(device(columns[dx + 1], gy, slot_at(k)))
        for z in opposite:
            ready(device(gx, gy, z))

        @pl.when(start)
        def _():
            ready(device(gx, above, jnp.int32(0)))

        @pl.when(end)
        def _():
            ready(device(gx, below, jnp.int32(n_z - 1)))

    @pl.when(late)
    def _():
        for k, dx in peers + [(0, 0)]:
            ready(device(columns[dx + 1], gy, slot_at(k)))

        @pl.when(start)
        def _():
            ready(device(gx, above, jnp.int32(0)))

        @pl.when(end)
        def _():
            ready(device(gx, below, jnp.int32(n_half - 1)))

    loads = [
        pltpu.make_async_copy(source, target, load_sem.at[i])
        for i, (source, target) in enumerate(
            [(pos_hbm, pos_ref), (count_hbm, count_ref), (key_hbm, key_ref), (vel_hbm, vel_ref)]
        )
    ]
    for load in loads:
        load.start()
    for load in loads:
        load.wait()

    lane = lax.broadcasted_iota(jnp.int32, (n_z, SLOTS), 1)
    row = lax.broadcasted_iota(jnp.int32, (n_z, SLOTS), 0)
    occupancy = jnp.zeros((n_z, SLOTS), jnp.int32)
    for z in range(n_z):
        occupancy = jnp.where(row == z, count_ref[z], occupancy)
    px, py, pz = pos_ref[0], pos_ref[1], pos_ref[2]
    cell = cell_of(px) * 9 + cell_of(py) * 3 + cell_of(pz)
    cell = jnp.where(lane < occupancy, cell, 27)
    order = cell * SLOTS + lane
    rank = jnp.zeros((n_z, SLOTS), jnp.int32)
    for m in range(SLOTS):
        rank = rank + jnp.where(order[:, m : m + 1] < order, 1, 0)
    source = jnp.zeros((n_z, SLOTS), jnp.int32)
    for m in range(SLOTS):
        source = jnp.where(rank[:, m : m + 1] == lane, m, source)
    real = lane < occupancy
    key = key_ref[...]
    fields = [
        jnp.where(real, take(px, source), FAR),
        take(py, source),
        take(pz, source),
        take(vel_ref[0], source),
        take(vel_ref[1], source),
        take(vel_ref[2], source),
        take(lax.shift_right_logical(key, 15).astype(jnp.float32), source),
        take((key & 32767).astype(jnp.float32), source),
    ]
    for f, field in enumerate(fields):
        stage[pl.ds(8 + f, n_z, stride=8), :] = field
        stage[pl.ds(f, 1), :] = field[n_z - 1 : n_z]
        stage[pl.ds(8 * (n_z + 1) + f, 1), :] = field[0:1]

    edge = jnp.logical_or(first, last)
    n_peers = len(peers)

    def copy(source, target, send, recv, to):
        return pltpu.make_async_remote_copy(
            src_ref=source, dst_ref=target, send_sem=send, recv_sem=recv,
            device_id=to, device_id_type=MESH,
        )

    def slab(h):
        return stage.at[pl.ds(pl.multiple_of(8 * n_half * h, 8), 8 * (n_half + 2)), :]

    across = copy(slab(1 - half), mirrored, send_sem.at[0], recv_sem.at[0], device(gx, gy, mirror))

    def send_sums(targets):
        for z in targets:
            copy(
                ranks.at[z], order_ref.at[gz], rank_send.at[0], rank_recv.at[0],
                device(gx, gy, z),
            ).start()

    def to_edge(h, y, position):
        return copy(
            slab(h), edged, send_sem.at[1 + h], recv_sem.at[1], device(gx, y, n_half * h + position)
        )

    @pl.when(late)
    def _():
        pl.semaphore_wait(barrier, jnp.where(last, n_half + 1, n_half))
        across.start()

        @pl.when(last)
        def _():
            to_edge(0, above, n_half - 1).start()

    sorted_key = take(key, source)

    own = as_own(*fields[:6], sorted_key)
    words = as_other(*fields[:6], sorted_key)

    def turned(shift):
        return pair_force(own, [pltpu.roll(word, SLOTS - shift, 1) for word in words])

    def some_turns(step, summed):
        for u in range(TURNS):
            shift = step * TURNS + (u + 1)
            push = turned(shift)
            summed = tuple(
                summed[c] + (push[c] - pltpu.roll(push[c], shift, 1)) for c in range(3)
            )
        return summed

    zero = jnp.zeros((n_z, SLOTS), jnp.float32)
    summed = lax.fori_loop(0, (SLOTS // 2 - 1) // TURNS, some_turns, (zero, zero, zero))
    last_push = turned(SLOTS // 2)
    summed = tuple(summed[c] + last_push[c] for c in range(3))

    left = lane < HALF
    inside = fields[0] < 0.5 * FAR
    top = jnp.logical_and(inside, fields[2] >= 2.0)
    bottom = jnp.logical_and(inside, fields[2] < 1.0)
    member = jnp.where(top, 1, jnp.where(bottom, 2 * SLOTS, 0))
    before = jnp.zeros((n_z, SLOTS), jnp.int32)
    for m in range(SLOTS):
        before = before + jnp.where(lane > m, member[:, m : m + 1], 0)
    low, high = before & (2 * SLOTS - 1), lax.shift_right_logical(before, 8)
    seat = jnp.where(jnp.logical_and(bottom, high < HALF), high + HALF, SLOTS)
    seat = jnp.where(jnp.logical_and(top, low < HALF), low, seat)
    origin = jnp.full((n_z, SLOTS), -1, jnp.int32)
    for m in range(SLOTS):
        origin = jnp.where(seat[:, m : m + 1] == lane, m, origin)
    taken = origin >= 0
    origin = jnp.maximum(origin, 0)

    def from_sides(values):
        return jnp.where(left, pltpu.roll(values, 1, 0), pltpu.roll(values, n_z - 1, 0))

    listed = [take(word, origin) for word in words]
    listed[0] = jnp.where(taken, listed[0], FAR)
    listed = [from_sides(values) for values in listed]
    listed[2] = listed[2] + jnp.where(left, -SIDE, SIDE)
    side_at = jnp.where(fields[2] < 1.5, 0, HALF)

    def some_sides(step, summed):
        for u in range(TURNS_Z):
            index = side_at + (step * TURNS_Z + u)
            push = pair_force(own, [take(values, index) for values in listed])
            summed = tuple(summed[c] + push[c] for c in range(3))
        return summed

    summed = some_sides(0, summed)
    for c in range(3):
        ranks[:, c, :] = summed[c]
    ranks[:, 3, :] = jnp.where(real, rank, rank + SLOTS).astype(jnp.float32)

    @pl.when(early)
    def _():
        from_edges = jnp.where(first, 2, jnp.where(end, 1, 0))
        pl.semaphore_wait(barrier, 2 * n_peers + 1 + from_edges)
        across.start()
        pl.semaphore_signal(
            plane_sem, inc=1, device_id=device(gx, gy, mirror), device_id_type=MESH
        )

        @pl.when(first)
        def _():
            for h in (0, 1):
                to_edge(h, below, 0).start()

    send_sums(opposite)

    @pl.when(late)
    def _():
        pl.semaphore_wait(plane_sem, 1)

        @pl.when(last)
        def _():
            to_edge(1, above, n_half - 1).start()

    def landing(slot):
        return tiles_ref.at[pl.ds(pl.multiple_of(24 * slot, 8), 24), :]

    def spread(buffer, offset, row_at, sem):
        def block(position):
            at = pl.multiple_of(8 * (offset + position), 8)
            return buffer.at[pl.ds(at, 24), :]

        for k, dx in peers:
            copy(
                block(slot_at(k)), landing((1 - dx) * (n_z + 2) + row_at),
                send_sem.at[sem], recv_sem.at[2],
                device(columns[dx + 1], gy, half * n_half + slot_at(k)),
            ).start()
        pltpu.make_async_copy(
            block(along), landing(n_z + 2 + row_at), recv_sem.at[2]
        ).start()

    spread(stage, half * n_half, gz + 1, 3)
    send_sums([half * n_half + slot_at(k) for k in (2, 1, 3)])
    pltpu.make_async_copy(ranks.at[gz], order_ref.at[gz], rank_recv.at[0]).start()

    across.wait_recv()
    spread(mirrored, 0, mirror + 1, 4)
    relay = jnp.logical_or(start, end)

    @pl.when(relay)
    def _():
        copy(
            edged, edged, send_sem.at[1], recv_sem.at[1], device(gx, gy, mirror)
        ).wait_recv()
        spread(edged, 0, jnp.where(start, n_z + 1, 0), 5)

    def bulk(count, sem):
        part = tiles_ref.at[pl.ds(0, 24 * count)]
        return copy(part, part, send_sem.at[sem], recv_sem.at[2], device(gx, gy, mirror))

    def bulk_rank(count):
        part = order_ref.at[pl.ds(0, count)]
        return copy(part, part, rank_send.at[0], rank_recv.at[0], device(gx, gy, mirror))

    bulk(3 * (n_z + 2), 3).wait_recv()
    bulk_rank(n_z).wait_recv()
    across.wait_send()
    bulk_rank(n_z - 1).wait_send()
    for sem in (3, 4):
        bulk(n_peers, sem).wait_send()

    @pl.when(relay)
    def _():
        bulk(n_peers, 5).wait_send()

    @pl.when(edge)
    def _():
        for h in (0, 1):
            to_edge(h, gy, 0).wait_send()


def exchange(groups, positions, velocities, keys, counts):
    n_z = groups[2]
    anywhere = pl.BlockSpec(memory_space=pl.ANY)
    slab = pltpu.VMEM((8 * (n_z // 2 + 2), SLOTS), jnp.float32)
    return pl.pallas_call(
        functools.partial(exchange_kernel, groups),
        out_shape=[
            pltpu.VMEM((72 * (n_z + 2), SLOTS), jnp.float32),
            pltpu.VMEM((n_z, 4, SLOTS), jnp.float32),
        ],
        in_specs=[anywhere] * 4,
        out_specs=[pl.BlockSpec(memory_space=pltpu.VMEM)] * 2,
        scratch_shapes=[
            pltpu.VMEM((3, n_z, SLOTS), jnp.float32),
            pltpu.VMEM((3, n_z, SLOTS), jnp.float32),
            pltpu.VMEM((n_z, SLOTS), jnp.int32),
            pltpu.SMEM((n_z,), jnp.int32),
            pltpu.VMEM((8 * (n_z + 2), SLOTS), jnp.float32),
            pltpu.VMEM((n_z, 4, SLOTS), jnp.float32),
            slab,
            slab,
            pltpu.SemaphoreType.DMA((4,)),
            pltpu.SemaphoreType.DMA((6,)),
            pltpu.SemaphoreType.DMA((3,)),
            pltpu.SemaphoreType.DMA((1,)),
            pltpu.SemaphoreType.DMA((1,)),
            pltpu.SemaphoreType.REGULAR,
        ],
        compiler_params=pltpu.CompilerParams(collective_id=0, has_side_effects=True),
        name="sort_exchange",
    )(positions, velocities, keys, counts)


def runs_of(offset):
    spans = [{-1: (2, 3), 0: (0, 3), 1: (0, 1)}[o] for o in offset]
    runs = []
    for a in range(*spans[0]):
        for b in range(*spans[1]):
            low, high = a * 9 + b * 3 + spans[2][0], a * 9 + b * 3 + spans[2][1]
            if runs and runs[-1][1] == low:
                runs[-1] = (runs[-1][0], high)
            else:
                runs.append((low, high))
    return runs


def force_kernel(rows, tiles_ref, order_ref, out_ref):
    lane = lax.broadcasted_iota(jnp.int32, (rows, SLOTS), 1)
    left_half = lane < HALF

    def load(offset, f):
        ox, oy, oz = offset
        start = (((1 + ox) * (rows + 2) + 1 + oy) * 3 + 1 + oz) * 8 + f
        return tiles_ref[pl.ds(start, rows, stride=24), :]

    def join(high, low):
        return high.astype(jnp.int32) * 32768 + low.astype(jnp.int32)

    def beads(offset):
        return [load(offset, f) for f in range(6)] + [join(load(offset, 6), load(offset, 7))]

    own = as_own(*beads((0, 0, 0)))

    def pair(other, summed):
        push = pair_force(own, other)
        return tuple(summed[c] + push[c] for c in range(3))

    zero = jnp.zeros((rows, SLOTS), jnp.float32)
    summed = tuple(order_ref[:, c, :] for c in range(3))

    def count_cells(cells, low, high):
        inside = jnp.logical_and(cells >= low, cells < high)
        return jnp.sum(jnp.where(inside, 1.0, 0.0), axis=1, keepdims=True).astype(jnp.int32)

    def cells_of(x, y, z):
        cells = cell_of(x) * 9 + cell_of(y) * 3 + cell_of(z)
        return jnp.where(x > 0.5 * FAR, 27, cells)

    def tiles_beside(axis, side):
        ranges = [(0,)] * axis + [(side,)] + [(-1, 0, 1)] * (2 - axis)
        return [(ox, oy, oz) for ox in ranges[0] for oy in ranges[1] for oz in ranges[2]]

    def tables(axis, side):
        tiles = []
        total = jnp.zeros((rows, 1), jnp.int32)
        for offset in tiles_beside(axis, side):
            cells = cells_of(*(load(offset, f) for f in range(3)))
            table = []
            for low, high in runs_of(offset):
                begin = count_cells(cells, 0, low) if low else jnp.zeros_like(total)
                length = count_cells(cells, low, high)
                table.append((total, begin - total))
                total = total + length
            tiles.append((offset, table))
        return tiles, total

    def listed(tiles, total, at):
        alive = at < total
        blank = jnp.zeros_like(lane)
        packed = [jnp.full((rows, SLOTS), FAR, jnp.float32), zero, zero, blank, zero, blank]
        for offset, table in tiles:
            index = at
            for base, shift in table:
                index = jnp.where(at >= base, at + shift, index)
            index = index & (SLOTS - 1)
            taken = jnp.logical_and(alive, at >= table[0][0])
            for f, value in enumerate(as_other(*beads(offset))):
                if f < 3 and offset[f]:
                    value = value + SIDE * offset[f]
                packed[f] = jnp.where(taken, take(value, index), packed[f])
        return packed

    def sweep(jobs, first, last, unroll, summed):
        def some_steps(s, summed):
            for u in range(unroll):
                for axis, lists in jobs:
                    index = side_at[axis] + (s * unroll + u)
                    summed = pair([take(values, index) for values in lists], summed)
            return summed

        if unroll == HALF:
            return some_steps(0, summed)
        return lax.fori_loop(first // unroll, (last + unroll - 1) // unroll, some_steps, summed)

    side_at = [jnp.where(own[axis] < 1.5, 0, HALF) for axis in range(3)]

    def merged(lower, upper, half):
        return [
            jnp.where(left_half, a if half == 0 else pltpu.roll(a, HALF, 1),
                      pltpu.roll(b, HALF, 1) if half == 0 else b)
            for a, b in zip(lower, upper)
        ]

    def along_x_and_y(summed):
        sides = [[tables(axis, side) for side in (-1, 1)] for axis in (0, 1)]
        longest = [jnp.maximum(jnp.max(a[1]), jnp.max(b[1])) for a, b in sides]

        def one_pass(p, summed):
            at = lane + p * SLOTS
            packed = [[listed(tiles, total, at) for tiles, total in pairs] for pairs in sides]
            for half in (0, 1):
                jobs = [(axis, merged(*packed[axis], half)) for axis in (0, 1)]
                steps = [
                    jnp.clip(longest[axis] - p * SLOTS - half * HALF, 0, HALF) for axis in (0, 1)
                ]
                if half == 0:
                    summed = sweep(jobs, 0, HALF, HALF, summed)
                else:
                    both = (jnp.minimum(steps[0], steps[1]) + UNROLL - 1) // UNROLL * UNROLL
                    summed = sweep(jobs, 0, both, UNROLL, summed)
                    for axis in (0, 1):
                        summed = sweep(jobs[axis : axis + 1], both, steps[axis], UNROLL, summed)
            return summed

        passes = (jnp.maximum(longest[0], longest[1]) + SLOTS - 1) // SLOTS
        return lax.fori_loop(0, passes, one_pass, summed)

    def rest_along_z(summed):
        lengths = [
            count_layer(load((0, 0, side), 0), load((0, 0, side), 2), side) for side in (-1, 1)
        ]
        longest = jnp.maximum(jnp.max(lengths[0]), jnp.max(lengths[1]))

        def second_half(_, summed):
            lists = merged(*(listed(*tables(2, side), lane) for side in (-1, 1)), 1)
            return sweep([(2, lists)], 0, longest - HALF, UNROLL, summed)

        return lax.fori_loop(0, jnp.where(longest > HALF, 1, 0), second_half, summed)

    def count_layer(x, z, side):
        inside = jnp.logical_and(x < 0.5 * FAR, z >= 2.0 if side < 0 else z < 1.0)
        return jnp.sum(jnp.where(inside, 1.0, 0.0), axis=1, keepdims=True).astype(jnp.int32)

    summed = along_x_and_y(summed)
    summed = rest_along_z(summed)

    order = order_ref[:, 3, :].astype(jnp.int32)
    scale = jnp.where(order < SLOTS, kick_scale, 0.0)
    order = order & (SLOTS - 1)
    for c in range(3):
        out_ref[c] = scale * take(summed[c], order)


def forces(n_z, tiles, order):
    vmem = pl.BlockSpec(memory_space=pltpu.VMEM)
    return pl.pallas_call(
        functools.partial(force_kernel, n_z),
        out_shape=jax.ShapeDtypeStruct((3, n_z, SLOTS), jnp.float32),
        in_specs=[vmem, vmem],
        out_specs=vmem,
        name="pair_forces",
    )(*(pltpu.with_memory_space_constraint(x, pltpu.VMEM) for x in (tiles, order)))


def solution(mesh):
    groups = tuple(mesh.shape[a] for a in ("gx", "gy", "gz"))
    n_z = groups[2]

    def on_device(positions, velocities, bead_keys, counts):
        tiles, order = exchange(
            groups,
            positions.reshape(3, n_z, SLOTS),
            velocities.reshape(3, n_z, SLOTS),
            bead_keys.reshape(n_z, SLOTS),
            counts.reshape(n_z),
        )
        kick = forces(n_z, tiles, order)
        return kick.reshape(3, 1, n_z, 1, SLOTS)

    in_specs = (
        P(None, "gx", ("gy", "gz"), None, None),
        P(None, "gx", ("gy", "gz"), None, None),
        P("gx", ("gy", "gz"), None, None),
        P("gx", ("gy", "gz"), None),
    )
    out_specs = P(None, "gx", "gy", "gz", None)
    return jax.shard_map(
        on_device, mesh=mesh, in_specs=in_specs, out_specs=out_specs, check_vma=False
    )
```

```python
import functools

import jax
import jax.numpy as jnp
from jax import lax
from jax.experimental import pallas as pl
from jax.experimental.pallas import tpu as pltpu
from jax.sharding import PartitionSpec as P

MESH = pl.DeviceIdType.MESH
SIDE = 3.0
SLOTS = 128
FAR = 4096.0
HALF = 64
TURNS = 21
TURNS_Z = 64
UNROLL = 16
UNIT = 5461.0
CENTRE = 32768.0

soft_radius = 0.05
friction = 4.5
noise_amplitude = 15.0
like_repulsion = 25.0
unlike_extra = 15.0
kick_scale = 0.02
root_twelve = 3.4641016151377544


def take(values, index):
    return jnp.take_along_axis(values, index, axis=1, mode="promise_in_bounds")


def cell_of(part):
    return jnp.where(part >= 2.0, 2, jnp.where(part >= 1.0, 1, 0))


def halves(first, second):
    high = (first * UNIT + (CENTRE + 0.5)).astype(jnp.int32)
    low = (second * UNIT + (CENTRE + 0.5)).astype(jnp.int32)
    return high * 65536 + low


def as_own(x, y, z, vx, vy, vz, key):
    return x, y, z, vx * UNIT + CENTRE, vy * UNIT + CENTRE, vz * UNIT, key


def as_other(x, y, z, vx, vy, vz, key):
    return x, y, z, halves(vx, vy), vz * UNIT, key


def pair_force(own, other):
    own_key, other_key = own[6], other[5]
    sep = [own[c] - other[c] for c in range(3)]
    squared = sep[0] * sep[0] + sep[1] * sep[1] + sep[2] * sep[2]
    root = lax.rsqrt(jnp.maximum(squared, 1e-30))
    distance = squared * root
    inverse = jnp.minimum(root, 1.0 / soft_radius)
    weight = jnp.maximum(1.0 - distance, 0.0) * inverse
    other_vx = lax.shift_right_logical(other[3], 16).astype(jnp.float32)
    other_vy = (other[3] & 65535).astype(jnp.float32)
    along = sep[0] * (own[3] - other_vx)
    along = along + sep[1] * (own[4] - other_vy)
    along = along + sep[2] * (own[5] - other[4])
    mixed = own_key ^ other_key
    hashed = mixed * 1103515245 + (own_key + other_key) * 12345
    hashed = hashed ^ lax.shift_right_logical(hashed, 15)
    hashed = hashed * 747796405
    hashed = hashed ^ lax.shift_right_logical(hashed, 13)
    fraction = lax.shift_right_logical(hashed << 1, 8).astype(jnp.float32)
    scale = noise_amplitude * root_twelve / 16777216.0
    base = like_repulsion - 0.5 * noise_amplitude * root_twelve
    level = jnp.where((mixed & 1) == 0, base, base + unlike_extra)
    strength = weight * (fraction * scale + level - (friction / UNIT) * (weight * along))
    return [strength * sep[c] for c in range(3)]


def exchange_kernel(
    groups, pos_hbm, vel_hbm, key_hbm, count_hbm, tiles_ref, order_ref,
    pos_ref, vel_ref, key_ref, count_ref, stage, ranks, mirrored, edged, passing,
    load_sem, send_sem, recv_sem, rank_send, rank_recv, plane_sem, mirror_sem,
):
    n_x, n_y, n_z = groups
    n_half = n_z // 2
    gx, gy, gz = lax.axis_index("gx"), lax.axis_index("gy"), lax.axis_index("gz")
    half, along = gz // n_half, lax.rem(gz, n_half)
    mirror = lax.rem(gz + n_half, n_z)
    first, last = gz == 0, gz == n_z - 1
    start, end = along == 0, along == n_half - 1
    above, below = lax.rem(gy + 1, n_y), lax.rem(gy + n_y - 1, n_y)
    columns = [lax.rem(gx + n_x + dx, n_x) for dx in (-1, 0, 1)]
    peers = [(k, dx) for k in (2, 1, 3, 0) for dx in (-1, 0, 1) if (k, dx) != (0, 0)]

    def slot_at(k):
        return lax.rem(along + k, n_half)

    def device(x, y, z):
        return {"gx": x, "gy": y, "gz": z}

    barrier = pltpu.get_barrier_semaphore()

    def ready(target):
        pl.semaphore_signal(barrier, inc=1, device_id=target, device_id_type=MESH)

    other_half = 1 - half
    opposite = [n_half * other_half + slot_at(k) for k in (2, 1, 3, 0)]
    early, late = half == 0, half == 1

    everyone = peers + [(0, 0)]
    is_top, is_bottom = gy == n_y - 1, gy == 0

    @pl.when(early)
    def _():
        for k, dx in peers:
            ready(device(columns[dx + 1], gy, slot_at(k)))
        for k, dx in everyone:
            ready(device(columns[dx + 1], gy, n_half + slot_at(k)))

        @pl.when(start)
        def _():
            ready(device(gx, above, jnp.int32(0)))
            ready(device(gx, below, jnp.int32(n_half)))

        @pl.when(end)
        def _():
            ready(device(gx, below, jnp.int32(n_z - 1)))

            @pl.when(jnp.logical_not(is_top))
            def _():
                ready(device(gx, above, jnp.int32(n_z - 1)))

    loads = [
        pltpu.make_async_copy(source, target, load_sem.at[i])
        for i, (source, target) in enumerate(
            [(pos_hbm, pos_ref), (count_hbm, count_ref), (key_hbm, key_ref), (vel_hbm, vel_ref)]
        )
    ]
    for load in loads:
        load.start()
    for load in loads:
        load.wait()

    lane = lax.broadcasted_iota(jnp.int32, (n_z, SLOTS), 1)
    row = lax.broadcasted_iota(jnp.int32, (n_z, SLOTS), 0)
    occupancy = jnp.zeros((n_z, SLOTS), jnp.int32)
    for z in range(n_z):
        occupancy = jnp.where(row == z, count_ref[z], occupancy)
    px, py, pz = pos_ref[0], pos_ref[1], pos_ref[2]
    cell = cell_of(px) * 9 + cell_of(py) * 3 + cell_of(pz)
    cell = jnp.where(lane < occupancy, cell, 27)
    order = cell * SLOTS + lane
    rank = jnp.zeros((n_z, SLOTS), jnp.int32)
    for m in range(SLOTS):
        rank = rank + jnp.where(order[:, m : m + 1] < order, 1, 0)
    source = jnp.zeros((n_z, SLOTS), jnp.int32)
    for m in range(SLOTS):
        source = jnp.where(rank[:, m : m + 1] == lane, m, source)
    real = lane < occupancy
    key = key_ref[...]
    fields = [
        jnp.where(real, take(px, source), FAR),
        take(py, source),
        take(pz, source),
        take(vel_ref[0], source),
        take(vel_ref[1], source),
        take(vel_ref[2], source),
        take(lax.shift_right_logical(key, 15).astype(jnp.float32), source),
        take((key & 32767).astype(jnp.float32), source),
    ]
    for f, field in enumerate(fields):
        stage[pl.ds(8 + f, n_z, stride=8), :] = field
        stage[pl.ds(f, 1), :] = field[n_z - 1 : n_z]
        stage[pl.ds(8 * (n_z + 1) + f, 1), :] = field[0:1]

    edge = jnp.logical_or(first, last)
    n_peers = len(peers)

    def copy(source, target, send, recv, to):
        return pltpu.make_async_remote_copy(
            src_ref=source, dst_ref=target, send_sem=send, recv_sem=recv,
            device_id=to, device_id_type=MESH,
        )

    def slab(h):
        return stage.at[pl.ds(pl.multiple_of(8 * n_half * h, 8), 8 * (n_half + 2)), :]

    def tell(target):
        pl.semaphore_signal(plane_sem, inc=1, device_id=target, device_id_type=MESH)

    across = copy(slab(1 - half), mirrored, send_sem.at[0], recv_sem.at[0], device(gx, gy, mirror))

    def send_sums(targets):
        for z in targets:
            copy(
                ranks.at[z], order_ref.at[gz], rank_send.at[0], rank_recv.at[0],
                device(gx, gy, z),
            ).start()

    def to_edge(h, y, position):
        return copy(
            slab(h), edged, send_sem.at[1 + h], recv_sem.at[1], device(gx, y, n_half * h + position)
        )

    @pl.when(late)
    def _():
        from_edges = jnp.where(last, jnp.where(is_bottom, 1, 2), jnp.where(start, 1, 0))
        pl.semaphore_wait(barrier, len(everyone) + from_edges)
        across.start()
        @pl.when(last)
        def _():
            to_edge(0, above, n_half - 1).start()

            @pl.when(is_top)
            def _():
                copy(
                    slab(1), passing, send_sem.at[2], recv_sem.at[3],
                    device(gx, above, n_half - 1),
                ).start()

            @pl.when(jnp.logical_not(is_bottom))
            def _():
                tell(device(gx, below, jnp.int32(n_half - 1)))

        pl.semaphore_signal(
            mirror_sem, inc=1, device_id=device(gx, gy, mirror), device_id_type=MESH
        )
        for k, dx in peers:
            tell(device(columns[dx + 1], gy, slot_at(k)))

        @pl.when(start)
        def _():
            tell(device(gx, above, jnp.int32(0)))

    sorted_key = take(key, source)

    own = as_own(*fields[:6], sorted_key)
    words = as_other(*fields[:6], sorted_key)

    def turned(shift):
        return pair_force(own, [pltpu.roll(word, SLOTS - shift, 1) for word in words])

    def some_turns(step, summed):
        for u in range(TURNS):
            shift = step * TURNS + (u + 1)
            push = turned(shift)
            summed = tuple(
                summed[c] + (push[c] - pltpu.roll(push[c], shift, 1)) for c in range(3)
            )
        return summed

    zero = jnp.zeros((n_z, SLOTS), jnp.float32)
    summed = lax.fori_loop(0, (SLOTS // 2 - 1) // TURNS, some_turns, (zero, zero, zero))
    last_push = turned(SLOTS // 2)
    summed = tuple(summed[c] + last_push[c] for c in range(3))

    left = lane < HALF
    inside = fields[0] < 0.5 * FAR
    top = jnp.logical_and(inside, fields[2] >= 2.0)
    bottom = jnp.logical_and(inside, fields[2] < 1.0)
    member = jnp.where(top, 1, jnp.where(bottom, 2 * SLOTS, 0))
    before = jnp.zeros((n_z, SLOTS), jnp.int32)
    for m in range(SLOTS):
        before = before + jnp.where(lane > m, member[:, m : m + 1], 0)
    low, high = before & (2 * SLOTS - 1), lax.shift_right_logical(before, 8)
    seat = jnp.where(jnp.logical_and(bottom, high < HALF), high + HALF, SLOTS)
    seat = jnp.where(jnp.logical_and(top, low < HALF), low, seat)
    origin = jnp.full((n_z, SLOTS), -1, jnp.int32)
    for m in range(SLOTS):
        origin = jnp.where(seat[:, m : m + 1] == lane, m, origin)
    taken = origin >= 0
    origin = jnp.maximum(origin, 0)

    def from_sides(values):
        return jnp.where(left, pltpu.roll(values, 1, 0), pltpu.roll(values, n_z - 1, 0))

    listed = [take(word, origin) for word in words]
    listed[0] = jnp.where(taken, listed[0], FAR)
    listed = [from_sides(values) for values in listed]
    listed[2] = listed[2] + jnp.where(left, -SIDE, SIDE)
    side_at = jnp.where(fields[2] < 1.5, 0, HALF)

    def some_sides(step, summed):
        for u in range(TURNS_Z):
            index = side_at + (step * TURNS_Z + u)
            push = pair_force(own, [take(values, index) for values in listed])
            summed = tuple(summed[c] + push[c] for c in range(3))
        return summed

    summed = some_sides(0, summed)
    for c in range(3):
        ranks[:, c, :] = summed[c]
    ranks[:, 3, :] = jnp.where(real, rank, rank + SLOTS).astype(jnp.float32)

    @pl.when(early)
    def _():
        pl.semaphore_wait(barrier, jnp.where(first, n_peers + 1, n_peers))

        @pl.when(first)
        def _():
            to_edge(0, below, 0).start()

    @pl.when(late)
    def _():
        send_sums(opposite)
        pl.semaphore_wait(plane_sem, 1)

        @pl.when(jnp.logical_and(last, jnp.logical_not(is_top)))
        def _():
            to_edge(1, above, n_half - 1).start()


    def landing(slot):
        return tiles_ref.at[pl.ds(pl.multiple_of(24 * slot, 8), 24), :]

    def spread(buffer, offset, row_at, sem):
        def block(position):
            at = pl.multiple_of(8 * (offset + position), 8)
            return buffer.at[pl.ds(at, 24), :]

        for k, dx in peers:
            copy(
                block(slot_at(k)), landing((1 - dx) * (n_z + 2) + row_at),
                send_sem.at[sem], recv_sem.at[2],
                device(columns[dx + 1], gy, half * n_half + slot_at(k)),
            ).start()
        pltpu.make_async_copy(
            block(along), landing(n_z + 2 + row_at), recv_sem.at[2]
        ).start()

    spread(stage, half * n_half, gz + 1, 3)
    send_sums([half * n_half + slot_at(k) for k in (2, 1, 3)])
    pltpu.make_async_copy(ranks.at[gz], order_ref.at[gz], rank_recv.at[0]).start()

    @pl.when(early)
    def _():
        pl.semaphore_wait(mirror_sem, 1)
        across.start()

    across.wait_recv()
    spread(mirrored, 0, mirror + 1, 4)

    relay = jnp.logical_or(start, end)

    @pl.when(relay)
    def _():
        copy(
            edged, edged, send_sem.at[1], recv_sem.at[1], device(gx, gy, mirror)
        ).wait_recv()
        spread(edged, 0, jnp.where(start, n_z + 1, 0), 5)

    @pl.when(jnp.logical_and(early, jnp.logical_and(end, is_bottom)))
    def _():
        copy(
            passing, passing, send_sem.at[1], recv_sem.at[3], device(gx, gy, mirror)
        ).wait_recv()
        copy(
            passing, edged, send_sem.at[6], recv_sem.at[1], device(gx, gy, mirror)
        ).start()

    @pl.when(early)
    def _():
        extra = jnp.logical_or(start, jnp.logical_and(end, jnp.logical_not(is_top)))
        pl.semaphore_wait(plane_sem, jnp.where(extra, n_peers + 1, n_peers))
        tell(device(gx, gy, mirror))

        @pl.when(first)
        def _():
            to_edge(1, below, 0).start()

        send_sums(opposite)

    def bulk(count, sem):
        part = tiles_ref.at[pl.ds(0, 24 * count)]
        return copy(part, part, send_sem.at[sem], recv_sem.at[2], device(gx, gy, mirror))

    def bulk_rank(count):
        part = order_ref.at[pl.ds(0, count)]
        return copy(part, part, rank_send.at[0], rank_recv.at[0], device(gx, gy, mirror))

    bulk(3 * (n_z + 2), 3).wait_recv()
    bulk_rank(n_z).wait_recv()
    across.wait_send()
    bulk_rank(n_z - 1).wait_send()
    for sem in (3, 4):
        bulk(n_peers, sem).wait_send()

    @pl.when(relay)
    def _():
        bulk(n_peers, 5).wait_send()

    @pl.when(edge)
    def _():
        for h in (0, 1):
            to_edge(h, gy, 0).wait_send()

    @pl.when(jnp.logical_and(early, jnp.logical_and(end, is_bottom)))
    def _():
        copy(
            passing, edged, send_sem.at[6], recv_sem.at[1], device(gx, gy, mirror)
        ).wait_send()


def exchange(groups, positions, velocities, keys, counts):
    n_z = groups[2]
    anywhere = pl.BlockSpec(memory_space=pl.ANY)
    slab = pltpu.VMEM((8 * (n_z // 2 + 2), SLOTS), jnp.float32)
    return pl.pallas_call(
        functools.partial(exchange_kernel, groups),
        out_shape=[
            pltpu.VMEM((72 * (n_z + 2), SLOTS), jnp.float32),
            pltpu.VMEM((n_z, 4, SLOTS), jnp.float32),
        ],
        in_specs=[anywhere] * 4,
        out_specs=[pl.BlockSpec(memory_space=pltpu.VMEM)] * 2,
        scratch_shapes=[
            pltpu.VMEM((3, n_z, SLOTS), jnp.float32),
            pltpu.VMEM((3, n_z, SLOTS), jnp.float32),
            pltpu.VMEM((n_z, SLOTS), jnp.int32),
            pltpu.SMEM((n_z,), jnp.int32),
            pltpu.VMEM((8 * (n_z + 2), SLOTS), jnp.float32),
            pltpu.VMEM((n_z, 4, SLOTS), jnp.float32),
            slab,
            slab,
            slab,
            pltpu.SemaphoreType.DMA((4,)),
            pltpu.SemaphoreType.DMA((7,)),
            pltpu.SemaphoreType.DMA((4,)),
            pltpu.SemaphoreType.DMA((1,)),
            pltpu.SemaphoreType.DMA((1,)),
            pltpu.SemaphoreType.REGULAR,
            pltpu.SemaphoreType.REGULAR,
        ],
        compiler_params=pltpu.CompilerParams(collective_id=0, has_side_effects=True),
        name="sort_exchange",
    )(positions, velocities, keys, counts)


def runs_of(offset):
    spans = [{-1: (2, 3), 0: (0, 3), 1: (0, 1)}[o] for o in offset]
    runs = []
    for a in range(*spans[0]):
        for b in range(*spans[1]):
            low, high = a * 9 + b * 3 + spans[2][0], a * 9 + b * 3 + spans[2][1]
            if runs and runs[-1][1] == low:
                runs[-1] = (runs[-1][0], high)
            else:
                runs.append((low, high))
    return runs


def force_kernel(rows, tiles_ref, order_ref, out_ref):
    lane = lax.broadcasted_iota(jnp.int32, (rows, SLOTS), 1)
    left_half = lane < HALF

    def load(offset, f):
        ox, oy, oz = offset
        start = (((1 + ox) * (rows + 2) + 1 + oy) * 3 + 1 + oz) * 8 + f
        return tiles_ref[pl.ds(start, rows, stride=24), :]

    def join(high, low):
        return high.astype(jnp.int32) * 32768 + low.astype(jnp.int32)

    def beads(offset):
        return [load(offset, f) for f in range(6)] + [join(load(offset, 6), load(offset, 7))]

    own = as_own(*beads((0, 0, 0)))

    def pair(other, summed):
        push = pair_force(own, other)
        return tuple(summed[c] + push[c] for c in range(3))

    zero = jnp.zeros((rows, SLOTS), jnp.float32)
    summed = tuple(order_ref[:, c, :] for c in range(3))

    def count_cells(cells, low, high):
        inside = jnp.logical_and(cells >= low, cells < high)
        return jnp.sum(jnp.where(inside, 1.0, 0.0), axis=1, keepdims=True).astype(jnp.int32)

    def cells_of(x, y, z):
        cells = cell_of(x) * 9 + cell_of(y) * 3 + cell_of(z)
        return jnp.where(x > 0.5 * FAR, 27, cells)

    def tiles_beside(axis, side):
        ranges = [(0,)] * axis + [(side,)] + [(-1, 0, 1)] * (2 - axis)
        return [(ox, oy, oz) for ox in ranges[0] for oy in ranges[1] for oz in ranges[2]]

    def tables(axis, side):
        tiles = []
        total = jnp.zeros((rows, 1), jnp.int32)
        for offset in tiles_beside(axis, side):
            cells = cells_of(*(load(offset, f) for f in range(3)))
            table = []
            for low, high in runs_of(offset):
                begin = count_cells(cells, 0, low) if low else jnp.zeros_like(total)
                length = count_cells(cells, low, high)
                table.append((total, begin - total))
                total = total + length
            tiles.append((offset, table))
        return tiles, total

    def listed(tiles, total, at):
        alive = at < total
        blank = jnp.zeros_like(lane)
        packed = [jnp.full((rows, SLOTS), FAR, jnp.float32), zero, zero, blank, zero, blank]
        for offset, table in tiles:
            index = at
            for base, shift in table:
                index = jnp.where(at >= base, at + shift, index)
            index = index & (SLOTS - 1)
            taken = jnp.logical_and(alive, at >= table[0][0])
            for f, value in enumerate(as_other(*beads(offset))):
                if f < 3 and offset[f]:
                    value = value + SIDE * offset[f]
                packed[f] = jnp.where(taken, take(value, index), packed[f])
        return packed

    def sweep(jobs, first, last, unroll, summed):
        def some_steps(s, summed):
            for u in range(unroll):
                for axis, lists in jobs:
                    index = side_at[axis] + (s * unroll + u)
                    summed = pair([take(values, index) for values in lists], summed)
            return summed

        if unroll == HALF:
            return some_steps(0, summed)
        return lax.fori_loop(first // unroll, (last + unroll - 1) // unroll, some_steps, summed)

    side_at = [jnp.where(own[axis] < 1.5, 0, HALF) for axis in range(3)]

    def merged(lower, upper, half):
        return [
            jnp.where(left_half, a if half == 0 else pltpu.roll(a, HALF, 1),
                      pltpu.roll(b, HALF, 1) if half == 0 else b)
            for a, b in zip(lower, upper)
        ]

    def along_x_and_y(summed):
        sides = [[tables(axis, side) for side in (-1, 1)] for axis in (0, 1)]
        longest = [jnp.maximum(jnp.max(a[1]), jnp.max(b[1])) for a, b in sides]

        def one_pass(p, summed):
            at = lane + p * SLOTS
            packed = [[listed(tiles, total, at) for tiles, total in pairs] for pairs in sides]
            for half in (0, 1):
                jobs = [(axis, merged(*packed[axis], half)) for axis in (0, 1)]
                steps = [
                    jnp.clip(longest[axis] - p * SLOTS - half * HALF, 0, HALF) for axis in (0, 1)
                ]
                if half == 0:
                    summed = sweep(jobs, 0, HALF, HALF, summed)
                else:
                    both = (jnp.minimum(steps[0], steps[1]) + UNROLL - 1) // UNROLL * UNROLL
                    summed = sweep(jobs, 0, both, UNROLL, summed)
                    for axis in (0, 1):
                        summed = sweep(jobs[axis : axis + 1], both, steps[axis], UNROLL, summed)
            return summed

        passes = (jnp.maximum(longest[0], longest[1]) + SLOTS - 1) // SLOTS
        return lax.fori_loop(0, passes, one_pass, summed)

    def rest_along_z(summed):
        lengths = [
            count_layer(load((0, 0, side), 0), load((0, 0, side), 2), side) for side in (-1, 1)
        ]
        longest = jnp.maximum(jnp.max(lengths[0]), jnp.max(lengths[1]))

        def second_half(_, summed):
            lists = merged(*(listed(*tables(2, side), lane) for side in (-1, 1)), 1)
            return sweep([(2, lists)], 0, longest - HALF, UNROLL, summed)

        return lax.fori_loop(0, jnp.where(longest > HALF, 1, 0), second_half, summed)

    def count_layer(x, z, side):
        inside = jnp.logical_and(x < 0.5 * FAR, z >= 2.0 if side < 0 else z < 1.0)
        return jnp.sum(jnp.where(inside, 1.0, 0.0), axis=1, keepdims=True).astype(jnp.int32)

    summed = along_x_and_y(summed)
    summed = rest_along_z(summed)

    order = order_ref[:, 3, :].astype(jnp.int32)
    scale = jnp.where(order < SLOTS, kick_scale, 0.0)
    order = order & (SLOTS - 1)
    for c in range(3):
        out_ref[c] = scale * take(summed[c], order)


def forces(n_z, tiles, order):
    vmem = pl.BlockSpec(memory_space=pltpu.VMEM)
    return pl.pallas_call(
        functools.partial(force_kernel, n_z),
        out_shape=jax.ShapeDtypeStruct((3, n_z, SLOTS), jnp.float32),
        in_specs=[vmem, vmem],
        out_specs=vmem,
        name="pair_forces",
    )(*(pltpu.with_memory_space_constraint(x, pltpu.VMEM) for x in (tiles, order)))


def solution(mesh):
    groups = tuple(mesh.shape[a] for a in ("gx", "gy", "gz"))
    n_z = groups[2]

    def on_device(positions, velocities, bead_keys, counts):
        tiles, order = exchange(
            groups,
            positions.reshape(3, n_z, SLOTS),
            velocities.reshape(3, n_z, SLOTS),
            bead_keys.reshape(n_z, SLOTS),
            counts.reshape(n_z),
        )
        kick = forces(n_z, tiles, order)
        return kick.reshape(3, 1, n_z, 1, SLOTS)

    in_specs = (
        P(None, "gx", ("gy", "gz"), None, None),
        P(None, "gx", ("gy", "gz"), None, None),
        P("gx", ("gy", "gz"), None, None),
        P("gx", ("gy", "gz"), None),
    )
    out_specs = P(None, "gx", "gy", "gz", None)
    return jax.shard_map(
        on_device, mesh=mesh, in_specs=in_specs, out_specs=out_specs, check_vma=False
    )
```

```python
import functools

import jax
import jax.numpy as jnp
from jax import lax
from jax.experimental import pallas as pl
from jax.experimental.pallas import tpu as pltpu
from jax.sharding import PartitionSpec as P

MESH = pl.DeviceIdType.MESH
SIDE = 3.0
SLOTS = 128
FAR = 4096.0
HALF = 64
TURNS = 21
TURNS_Z = 64
UNROLL = 16
UNIT = 5461.0
CENTRE = 32768.0

soft_radius = 0.05
friction = 4.5
noise_amplitude = 15.0
like_repulsion = 25.0
unlike_extra = 15.0
kick_scale = 0.02
root_twelve = 3.4641016151377544


def take(values, index):
    return jnp.take_along_axis(values, index, axis=1, mode="promise_in_bounds")


def cell_of(part):
    return jnp.where(part >= 2.0, 2, jnp.where(part >= 1.0, 1, 0))


def halves(first, second):
    high = (first * UNIT + (CENTRE + 0.5)).astype(jnp.int32)
    low = (second * UNIT + (CENTRE + 0.5)).astype(jnp.int32)
    return high * 65536 + low


def as_own(x, y, z, vx, vy, vz, key):
    return x, y, z, vx * UNIT + CENTRE, vy * UNIT + CENTRE, vz * UNIT, key


def as_other(x, y, z, vx, vy, vz, key):
    return x, y, z, halves(vx, vy), vz * UNIT, key


def pair_force(own, other):
    own_key, other_key = own[6], other[5]
    sep = [own[c] - other[c] for c in range(3)]
    squared = sep[0] * sep[0] + sep[1] * sep[1] + sep[2] * sep[2]
    root = lax.rsqrt(jnp.maximum(squared, 1e-30))
    distance = squared * root
    inverse = jnp.minimum(root, 1.0 / soft_radius)
    weight = jnp.maximum(1.0 - distance, 0.0) * inverse
    other_vx = lax.shift_right_logical(other[3], 16).astype(jnp.float32)
    other_vy = (other[3] & 65535).astype(jnp.float32)
    along = sep[0] * (own[3] - other_vx)
    along = along + sep[1] * (own[4] - other_vy)
    along = along + sep[2] * (own[5] - other[4])
    mixed = own_key ^ other_key
    hashed = mixed * 1103515245 + (own_key + other_key) * 12345
    hashed = hashed ^ lax.shift_right_logical(hashed, 15)
    hashed = hashed * 747796405
    hashed = hashed ^ lax.shift_right_logical(hashed, 13)
    fraction = lax.shift_right_logical(hashed << 1, 8).astype(jnp.float32)
    scale = noise_amplitude * root_twelve / 16777216.0
    base = like_repulsion - 0.5 * noise_amplitude * root_twelve
    level = jnp.where((mixed & 1) == 0, base, base + unlike_extra)
    strength = weight * (fraction * scale + level - (friction / UNIT) * (weight * along))
    return [strength * sep[c] for c in range(3)]


def exchange_kernel(
    groups, pos_hbm, vel_hbm, key_hbm, count_hbm, tiles_ref, order_ref,
    pos_ref, vel_ref, key_ref, count_ref, stage, ranks, mirrored, edged, passing,
    load_sem, send_sem, recv_sem, rank_send, rank_recv, plane_sem, mirror_sem,
):
    n_x, n_y, n_z = groups
    n_half = n_z // 2
    gx, gy, gz = lax.axis_index("gx"), lax.axis_index("gy"), lax.axis_index("gz")
    half, along = gz // n_half, lax.rem(gz, n_half)
    mirror = lax.rem(gz + n_half, n_z)
    first, last = gz == 0, gz == n_z - 1
    start, end = along == 0, along == n_half - 1
    above, below = lax.rem(gy + 1, n_y), lax.rem(gy + n_y - 1, n_y)
    columns = [lax.rem(gx + n_x + dx, n_x) for dx in (-1, 0, 1)]
    peers = [(k, dx) for k in (2, 1, 3, 0) for dx in (-1, 0, 1) if (k, dx) != (0, 0)]

    def slot_at(k):
        return lax.rem(along + k, n_half)

    def device(x, y, z):
        return {"gx": x, "gy": y, "gz": z}

    loads = [
        pltpu.make_async_copy(source, target, load_sem.at[i])
        for i, (source, target) in enumerate(
            [(pos_hbm, pos_ref), (count_hbm, count_ref), (key_hbm, key_ref), (vel_hbm, vel_ref)]
        )
    ]
    for load in loads:
        load.start()

    barrier = pltpu.get_barrier_semaphore()

    def ready(target):
        pl.semaphore_signal(barrier, inc=1, device_id=target, device_id_type=MESH)

    other_half = 1 - half
    opposite = [n_half * other_half + slot_at(k) for k in (2, 1, 3, 0)]
    early, late = half == 0, half == 1

    everyone = peers + [(0, 0)]
    is_top, is_bottom = gy == n_y - 1, gy == 0

    @pl.when(early)
    def _():
        for k, dx in peers:
            ready(device(columns[dx + 1], gy, slot_at(k)))
        for k, dx in everyone:
            ready(device(columns[dx + 1], gy, n_half + slot_at(k)))

        @pl.when(start)
        def _():
            ready(device(gx, above, jnp.int32(0)))
            ready(device(gx, below, jnp.int32(n_half)))

        @pl.when(end)
        def _():
            ready(device(gx, below, jnp.int32(n_z - 1)))

            @pl.when(jnp.logical_not(is_top))
            def _():
                ready(device(gx, above, jnp.int32(n_z - 1)))

    for load in loads[:2]:
        load.wait()

    lane = lax.broadcasted_iota(jnp.int32, (n_z, SLOTS), 1)
    row = lax.broadcasted_iota(jnp.int32, (n_z, SLOTS), 0)
    occupancy = jnp.zeros((n_z, SLOTS), jnp.int32)
    for z in range(n_z):
        occupancy = jnp.where(row == z, count_ref[z], occupancy)
    px, py, pz = pos_ref[0], pos_ref[1], pos_ref[2]
    cell = cell_of(px) * 9 + cell_of(py) * 3 + cell_of(pz)
    cell = jnp.where(lane < occupancy, cell, 27)
    order = cell * SLOTS + lane
    rank = jnp.zeros((n_z, SLOTS), jnp.int32)
    for m in range(SLOTS):
        rank = rank + jnp.where(order[:, m : m + 1] < order, 1, 0)
    source = jnp.zeros((n_z, SLOTS), jnp.int32)
    for m in range(SLOTS):
        source = jnp.where(rank[:, m : m + 1] == lane, m, source)
    real = lane < occupancy
    for load in loads[2:]:
        load.wait()
    key = key_ref[...]
    fields = [
        jnp.where(real, take(px, source), FAR),
        take(py, source),
        take(pz, source),
        take(vel_ref[0], source),
        take(vel_ref[1], source),
        take(vel_ref[2], source),
        take(lax.shift_right_logical(key, 15).astype(jnp.float32), source),
        take((key & 32767).astype(jnp.float32), source),
    ]
    for f, field in enumerate(fields):
        stage[pl.ds(8 + f, n_z, stride=8), :] = field
        stage[pl.ds(f, 1), :] = field[n_z - 1 : n_z]
        stage[pl.ds(8 * (n_z + 1) + f, 1), :] = field[0:1]

    edge = jnp.logical_or(first, last)
    n_peers = len(peers)

    def copy(source, target, send, recv, to):
        return pltpu.make_async_remote_copy(
            src_ref=source, dst_ref=target, send_sem=send, recv_sem=recv,
            device_id=to, device_id_type=MESH,
        )

    def slab(h):
        return stage.at[pl.ds(pl.multiple_of(8 * n_half * h, 8), 8 * (n_half + 2)), :]

    def tell(target):
        pl.semaphore_signal(plane_sem, inc=1, device_id=target, device_id_type=MESH)

    across = copy(slab(1 - half), mirrored, send_sem.at[0], recv_sem.at[0], device(gx, gy, mirror))

    def send_sums(targets):
        for z in targets:
            copy(
                ranks.at[z], order_ref.at[gz], rank_send.at[0], rank_recv.at[0],
                device(gx, gy, z),
            ).start()

    def to_edge(h, y, position):
        return copy(
            slab(h), edged, send_sem.at[1 + h], recv_sem.at[1], device(gx, y, n_half * h + position)
        )

    @pl.when(late)
    def _():
        from_edges = jnp.where(last, jnp.where(is_bottom, 1, 2), jnp.where(start, 1, 0))
        pl.semaphore_wait(barrier, len(everyone) + from_edges)
        across.start()
        @pl.when(last)
        def _():
            to_edge(0, above, n_half - 1).start()

            @pl.when(is_top)
            def _():
                copy(
                    slab(1), passing, send_sem.at[2], recv_sem.at[3],
                    device(gx, above, n_half - 1),
                ).start()

            @pl.when(jnp.logical_not(is_bottom))
            def _():
                tell(device(gx, below, jnp.int32(n_half - 1)))

        pl.semaphore_signal(
            mirror_sem, inc=1, device_id=device(gx, gy, mirror), device_id_type=MESH
        )
        for k, dx in peers:
            tell(device(columns[dx + 1], gy, slot_at(k)))

        @pl.when(start)
        def _():
            tell(device(gx, above, jnp.int32(0)))

    sorted_key = take(key, source)

    own = as_own(*fields[:6], sorted_key)
    words = as_other(*fields[:6], sorted_key)

    def turned(shift):
        return pair_force(own, [pltpu.roll(word, SLOTS - shift, 1) for word in words])

    def some_turns(step, summed):
        for u in range(TURNS):
            shift = step * TURNS + (u + 1)
            push = turned(shift)
            summed = tuple(
                summed[c] + (push[c] - pltpu.roll(push[c], shift, 1)) for c in range(3)
            )
        return summed

    zero = jnp.zeros((n_z, SLOTS), jnp.float32)
    summed = lax.fori_loop(0, (SLOTS // 2 - 1) // TURNS, some_turns, (zero, zero, zero))
    last_push = turned(SLOTS // 2)
    summed = tuple(summed[c] + last_push[c] for c in range(3))

    left = lane < HALF
    inside = fields[0] < 0.5 * FAR
    top = jnp.logical_and(inside, fields[2] >= 2.0)
    bottom = jnp.logical_and(inside, fields[2] < 1.0)
    member = jnp.where(top, 1, jnp.where(bottom, 2 * SLOTS, 0))
    before = jnp.zeros((n_z, SLOTS), jnp.int32)
    for m in range(SLOTS):
        before = before + jnp.where(lane > m, member[:, m : m + 1], 0)
    low, high = before & (2 * SLOTS - 1), lax.shift_right_logical(before, 8)
    seat = jnp.where(jnp.logical_and(bottom, high < HALF), high + HALF, SLOTS)
    seat = jnp.where(jnp.logical_and(top, low < HALF), low, seat)
    origin = jnp.full((n_z, SLOTS), -1, jnp.int32)
    for m in range(SLOTS):
        origin = jnp.where(seat[:, m : m + 1] == lane, m, origin)
    taken = origin >= 0
    origin = jnp.maximum(origin, 0)

    def from_sides(values):
        return jnp.where(left, pltpu.roll(values, 1, 0), pltpu.roll(values, n_z - 1, 0))

    listed = [take(word, origin) for word in words]
    listed[0] = jnp.where(taken, listed[0], FAR)
    listed = [from_sides(values) for values in listed]
    listed[2] = listed[2] + jnp.where(left, -SIDE, SIDE)
    side_at = jnp.where(fields[2] < 1.5, 0, HALF)

    def some_sides(step, summed):
        for u in range(TURNS_Z):
            index = side_at + (step * TURNS_Z + u)
            push = pair_force(own, [take(values, index) for values in listed])
            summed = tuple(summed[c] + push[c] for c in range(3))
        return summed

    summed = some_sides(0, summed)
    for c in range(3):
        ranks[:, c, :] = summed[c]
    ranks[:, 3, :] = jnp.where(real, rank, rank + SLOTS).astype(jnp.float32)

    @pl.when(early)
    def _():
        pl.semaphore_wait(barrier, jnp.where(first, n_peers + 1, n_peers))

        @pl.when(first)
        def _():
            to_edge(0, below, 0).start()

    @pl.when(late)
    def _():
        send_sums(opposite)
        pl.semaphore_wait(plane_sem, 1)

        @pl.when(jnp.logical_and(last, jnp.logical_not(is_top)))
        def _():
            to_edge(1, above, n_half - 1).start()


    def landing(slot):
        return tiles_ref.at[pl.ds(pl.multiple_of(24 * slot, 8), 24), :]

    def spread(buffer, offset, row_at, sem):
        def block(position):
            at = pl.multiple_of(8 * (offset + position), 8)
            return buffer.at[pl.ds(at, 24), :]

        for k, dx in peers:
            copy(
                block(slot_at(k)), landing((1 - dx) * (n_z + 2) + row_at),
                send_sem.at[sem], recv_sem.at[2],
                device(columns[dx + 1], gy, half * n_half + slot_at(k)),
            ).start()
        pltpu.make_async_copy(
            block(along), landing(n_z + 2 + row_at), recv_sem.at[2]
        ).start()

    spread(stage, half * n_half, gz + 1, 3)
    send_sums([half * n_half + slot_at(k) for k in (2, 1, 3)])
    pltpu.make_async_copy(ranks.at[gz], order_ref.at[gz], rank_recv.at[0]).start()

    @pl.when(early)
    def _():
        pl.semaphore_wait(mirror_sem, 1)
        across.start()

    across.wait_recv()
    spread(mirrored, 0, mirror + 1, 4)

    relay = jnp.logical_or(start, end)

    @pl.when(relay)
    def _():
        copy(
            edged, edged, send_sem.at[1], recv_sem.at[1], device(gx, gy, mirror)
        ).wait_recv()
        spread(edged, 0, jnp.where(start, n_z + 1, 0), 5)

    @pl.when(jnp.logical_and(early, jnp.logical_and(end, is_bottom)))
    def _():
        copy(
            passing, passing, send_sem.at[1], recv_sem.at[3], device(gx, gy, mirror)
        ).wait_recv()
        copy(
            passing, edged, send_sem.at[6], recv_sem.at[1], device(gx, gy, mirror)
        ).start()

    @pl.when(early)
    def _():
        extra = jnp.logical_or(start, jnp.logical_and(end, jnp.logical_not(is_top)))
        pl.semaphore_wait(plane_sem, jnp.where(extra, n_peers + 1, n_peers))
        tell(device(gx, gy, mirror))

        @pl.when(first)
        def _():
            to_edge(1, below, 0).start()

        send_sums(opposite)

    def bulk(count, sem):
        part = tiles_ref.at[pl.ds(0, 24 * count)]
        return copy(part, part, send_sem.at[sem], recv_sem.at[2], device(gx, gy, mirror))

    def bulk_rank(count):
        part = order_ref.at[pl.ds(0, count)]
        return copy(part, part, rank_send.at[0], rank_recv.at[0], device(gx, gy, mirror))

    bulk(3 * (n_z + 2), 3).wait_recv()
    bulk_rank(n_z).wait_recv()
    across.wait_send()
    bulk_rank(n_z - 1).wait_send()
    for sem in (3, 4):
        bulk(n_peers, sem).wait_send()

    @pl.when(relay)
    def _():
        bulk(n_peers, 5).wait_send()

    @pl.when(edge)
    def _():
        for h in (0, 1):
            to_edge(h, gy, 0).wait_send()

    @pl.when(jnp.logical_and(early, jnp.logical_and(end, is_bottom)))
    def _():
        copy(
            passing, edged, send_sem.at[6], recv_sem.at[1], device(gx, gy, mirror)
        ).wait_send()


def exchange(groups, positions, velocities, keys, counts):
    n_z = groups[2]
    anywhere = pl.BlockSpec(memory_space=pl.ANY)
    slab = pltpu.VMEM((8 * (n_z // 2 + 2), SLOTS), jnp.float32)
    return pl.pallas_call(
        functools.partial(exchange_kernel, groups),
        out_shape=[
            pltpu.VMEM((72 * (n_z + 2), SLOTS), jnp.float32),
            pltpu.VMEM((n_z, 4, SLOTS), jnp.float32),
        ],
        in_specs=[anywhere] * 4,
        out_specs=[pl.BlockSpec(memory_space=pltpu.VMEM)] * 2,
        scratch_shapes=[
            pltpu.VMEM((3, n_z, SLOTS), jnp.float32),
            pltpu.VMEM((3, n_z, SLOTS), jnp.float32),
            pltpu.VMEM((n_z, SLOTS), jnp.int32),
            pltpu.SMEM((n_z,), jnp.int32),
            pltpu.VMEM((8 * (n_z + 2), SLOTS), jnp.float32),
            pltpu.VMEM((n_z, 4, SLOTS), jnp.float32),
            slab,
            slab,
            slab,
            pltpu.SemaphoreType.DMA((4,)),
            pltpu.SemaphoreType.DMA((7,)),
            pltpu.SemaphoreType.DMA((4,)),
            pltpu.SemaphoreType.DMA((1,)),
            pltpu.SemaphoreType.DMA((1,)),
            pltpu.SemaphoreType.REGULAR,
            pltpu.SemaphoreType.REGULAR,
        ],
        compiler_params=pltpu.CompilerParams(collective_id=0, has_side_effects=True),
        name="sort_exchange",
    )(positions, velocities, keys, counts)


def runs_of(offset):
    spans = [{-1: (2, 3), 0: (0, 3), 1: (0, 1)}[o] for o in offset]
    runs = []
    for a in range(*spans[0]):
        for b in range(*spans[1]):
            low, high = a * 9 + b * 3 + spans[2][0], a * 9 + b * 3 + spans[2][1]
            if runs and runs[-1][1] == low:
                runs[-1] = (runs[-1][0], high)
            else:
                runs.append((low, high))
    return runs


def force_kernel(rows, tiles_ref, order_ref, out_ref):
    lane = lax.broadcasted_iota(jnp.int32, (rows, SLOTS), 1)
    left_half = lane < HALF

    def load(offset, f):
        ox, oy, oz = offset
        start = (((1 + ox) * (rows + 2) + 1 + oy) * 3 + 1 + oz) * 8 + f
        return tiles_ref[pl.ds(start, rows, stride=24), :]

    def join(high, low):
        return high.astype(jnp.int32) * 32768 + low.astype(jnp.int32)

    def beads(offset):
        return [load(offset, f) for f in range(6)] + [join(load(offset, 6), load(offset, 7))]

    own = as_own(*beads((0, 0, 0)))

    def pair(other, summed):
        push = pair_force(own, other)
        return tuple(summed[c] + push[c] for c in range(3))

    zero = jnp.zeros((rows, SLOTS), jnp.float32)
    summed = tuple(order_ref[:, c, :] for c in range(3))

    def count_cells(cells, low, high):
        inside = jnp.logical_and(cells >= low, cells < high)
        return jnp.sum(jnp.where(inside, 1.0, 0.0), axis=1, keepdims=True).astype(jnp.int32)

    def cells_of(x, y, z):
        cells = cell_of(x) * 9 + cell_of(y) * 3 + cell_of(z)
        return jnp.where(x > 0.5 * FAR, 27, cells)

    def tiles_beside(axis, side):
        ranges = [(0,)] * axis + [(side,)] + [(-1, 0, 1)] * (2 - axis)
        return [(ox, oy, oz) for ox in ranges[0] for oy in ranges[1] for oz in ranges[2]]

    def tables(axis, side):
        tiles = []
        total = jnp.zeros((rows, 1), jnp.int32)
        for offset in tiles_beside(axis, side):
            cells = cells_of(*(load(offset, f) for f in range(3)))
            table = []
            for low, high in runs_of(offset):
                begin = count_cells(cells, 0, low) if low else jnp.zeros_like(total)
                length = count_cells(cells, low, high)
                table.append((total, begin - total))
                total = total + length
            tiles.append((offset, table))
        return tiles, total

    def listed(tiles, total, at):
        alive = at < total
        blank = jnp.zeros_like(lane)
        packed = [jnp.full((rows, SLOTS), FAR, jnp.float32), zero, zero, blank, zero, blank]
        for offset, table in tiles:
            index = at
            for base, shift in table:
                index = jnp.where(at >= base, at + shift, index)
            index = index & (SLOTS - 1)
            taken = jnp.logical_and(alive, at >= table[0][0])
            for f, value in enumerate(as_other(*beads(offset))):
                if f < 3 and offset[f]:
                    value = value + SIDE * offset[f]
                packed[f] = jnp.where(taken, take(value, index), packed[f])
        return packed

    def sweep(jobs, first, last, unroll, summed):
        def some_steps(s, summed):
            for u in range(unroll):
                for axis, lists in jobs:
                    index = side_at[axis] + (s * unroll + u)
                    summed = pair([take(values, index) for values in lists], summed)
            return summed

        if unroll == HALF:
            return some_steps(0, summed)
        return lax.fori_loop(first // unroll, (last + unroll - 1) // unroll, some_steps, summed)

    side_at = [jnp.where(own[axis] < 1.5, 0, HALF) for axis in range(3)]

    def merged(lower, upper, half):
        return [
            jnp.where(left_half, a if half == 0 else pltpu.roll(a, HALF, 1),
                      pltpu.roll(b, HALF, 1) if half == 0 else b)
            for a, b in zip(lower, upper)
        ]

    def along_x_and_y(summed):
        sides = [[tables(axis, side) for side in (-1, 1)] for axis in (0, 1)]
        longest = [jnp.maximum(jnp.max(a[1]), jnp.max(b[1])) for a, b in sides]

        def one_pass(p, summed):
            at = lane + p * SLOTS
            packed = [[listed(tiles, total, at) for tiles, total in pairs] for pairs in sides]
            for half in (0, 1):
                jobs = [(axis, merged(*packed[axis], half)) for axis in (0, 1)]
                steps = [
                    jnp.clip(longest[axis] - p * SLOTS - half * HALF, 0, HALF) for axis in (0, 1)
                ]
                if half == 0:
                    summed = sweep(jobs, 0, HALF, HALF, summed)
                else:
                    both = (jnp.minimum(steps[0], steps[1]) + UNROLL - 1) // UNROLL * UNROLL
                    summed = sweep(jobs, 0, both, UNROLL, summed)
                    for axis in (0, 1):
                        summed = sweep(jobs[axis : axis + 1], both, steps[axis], UNROLL, summed)
            return summed

        passes = (jnp.maximum(longest[0], longest[1]) + SLOTS - 1) // SLOTS
        return lax.fori_loop(0, passes, one_pass, summed)

    def rest_along_z(summed):
        lengths = [
            count_layer(load((0, 0, side), 0), load((0, 0, side), 2), side) for side in (-1, 1)
        ]
        longest = jnp.maximum(jnp.max(lengths[0]), jnp.max(lengths[1]))

        def second_half(_, summed):
            lists = merged(*(listed(*tables(2, side), lane) for side in (-1, 1)), 1)
            return sweep([(2, lists)], 0, longest - HALF, UNROLL, summed)

        return lax.fori_loop(0, jnp.where(longest > HALF, 1, 0), second_half, summed)

    def count_layer(x, z, side):
        inside = jnp.logical_and(x < 0.5 * FAR, z >= 2.0 if side < 0 else z < 1.0)
        return jnp.sum(jnp.where(inside, 1.0, 0.0), axis=1, keepdims=True).astype(jnp.int32)

    summed = along_x_and_y(summed)
    summed = rest_along_z(summed)

    order = order_ref[:, 3, :].astype(jnp.int32)
    scale = jnp.where(order < SLOTS, kick_scale, 0.0)
    order = order & (SLOTS - 1)
    for c in range(3):
        out_ref[c] = scale * take(summed[c], order)


def forces(n_z, tiles, order):
    vmem = pl.BlockSpec(memory_space=pltpu.VMEM)
    return pl.pallas_call(
        functools.partial(force_kernel, n_z),
        out_shape=jax.ShapeDtypeStruct((3, n_z, SLOTS), jnp.float32),
        in_specs=[vmem, vmem],
        out_specs=vmem,
        name="pair_forces",
    )(*(pltpu.with_memory_space_constraint(x, pltpu.VMEM) for x in (tiles, order)))


def solution(mesh):
    groups = tuple(mesh.shape[a] for a in ("gx", "gy", "gz"))
    n_z = groups[2]

    def on_device(positions, velocities, bead_keys, counts):
        tiles, order = exchange(
            groups,
            positions.reshape(3, n_z, SLOTS),
            velocities.reshape(3, n_z, SLOTS),
            bead_keys.reshape(n_z, SLOTS),
            counts.reshape(n_z),
        )
        kick = forces(n_z, tiles, order)
        return kick.reshape(3, 1, n_z, 1, SLOTS)

    in_specs = (
        P(None, "gx", ("gy", "gz"), None, None),
        P(None, "gx", ("gy", "gz"), None, None),
        P("gx", ("gy", "gz"), None, None),
        P("gx", ("gy", "gz"), None),
    )
    out_specs = P(None, "gx", "gy", "gz", None)
    return jax.shard_map(
        on_device, mesh=mesh, in_specs=in_specs, out_specs=out_specs, check_vma=False
    )
```

```python
import functools

import jax
import jax.numpy as jnp
from jax import lax
from jax.experimental import pallas as pl
from jax.experimental.pallas import tpu as pltpu
from jax.sharding import PartitionSpec as P

MESH = pl.DeviceIdType.MESH
SIDE = 3.0
SLOTS = 128
FAR = 4096.0
HALF = 64
TURNS = 21
TURNS_Z = 64
UNROLL = 16
UNIT = 5461.0
CENTRE = 32768.0

soft_radius = 0.05
friction = 4.5
noise_amplitude = 15.0
like_repulsion = 25.0
unlike_extra = 15.0
kick_scale = 0.02
root_twelve = 3.4641016151377544


def take(values, index):
    return jnp.take_along_axis(values, index, axis=1, mode="promise_in_bounds")


def cell_of(part):
    return jnp.where(part >= 2.0, 2, jnp.where(part >= 1.0, 1, 0))


def halves(first, second):
    high = (first * UNIT + (CENTRE + 0.5)).astype(jnp.int32)
    low = (second * UNIT + (CENTRE + 0.5)).astype(jnp.int32)
    return high * 65536 + low


def as_own(x, y, z, vx, vy, vz, key):
    return x, y, z, vx * UNIT + CENTRE, vy * UNIT + CENTRE, vz * UNIT, key


def as_other(x, y, z, vx, vy, vz, key):
    return x, y, z, halves(vx, vy), vz * UNIT, key


def pair_force(own, other):
    own_key, other_key = own[6], other[5]
    sep = [own[c] - other[c] for c in range(3)]
    squared = sep[0] * sep[0] + sep[1] * sep[1] + sep[2] * sep[2]
    root = lax.rsqrt(jnp.maximum(squared, 1e-30))
    distance = squared * root
    inverse = jnp.minimum(root, 1.0 / soft_radius)
    weight = jnp.maximum(1.0 - distance, 0.0) * inverse
    other_vx = lax.shift_right_logical(other[3], 16).astype(jnp.float32)
    other_vy = (other[3] & 65535).astype(jnp.float32)
    along = sep[0] * (own[3] - other_vx)
    along = along + sep[1] * (own[4] - other_vy)
    along = along + sep[2] * (own[5] - other[4])
    mixed = own_key ^ other_key
    hashed = mixed * 1103515245 + (own_key + other_key) * 12345
    hashed = hashed ^ lax.shift_right_logical(hashed, 15)
    hashed = hashed * 747796405
    hashed = hashed ^ lax.shift_right_logical(hashed, 13)
    fraction = lax.shift_right_logical(hashed << 1, 8).astype(jnp.float32)
    scale = noise_amplitude * root_twelve / 16777216.0
    base = like_repulsion - 0.5 * noise_amplitude * root_twelve
    level = jnp.where((mixed & 1) == 0, base, base + unlike_extra)
    strength = weight * (fraction * scale + level - (friction / UNIT) * (weight * along))
    return [strength * sep[c] for c in range(3)]


def exchange_kernel(
    groups, pos_hbm, vel_hbm, key_hbm, count_hbm, tiles_ref, order_ref,
    pos_ref, vel_ref, key_ref, count_ref, stage, ranks, mirrored, edged, passing,
    load_sem, send_sem, recv_sem, rank_send, rank_recv, plane_sem, mirror_sem,
):
    n_x, n_y, n_z = groups
    n_half = n_z // 2
    gx, gy, gz = lax.axis_index("gx"), lax.axis_index("gy"), lax.axis_index("gz")
    half, along = gz // n_half, lax.rem(gz, n_half)
    mirror = lax.rem(gz + n_half, n_z)
    first, last = gz == 0, gz == n_z - 1
    start, end = along == 0, along == n_half - 1
    above, below = lax.rem(gy + 1, n_y), lax.rem(gy + n_y - 1, n_y)
    columns = [lax.rem(gx + n_x + dx, n_x) for dx in (-1, 0, 1)]
    peers = [(k, dx) for k in (2, 1, 3, 0) for dx in (-1, 0, 1) if (k, dx) != (0, 0)]

    def slot_at(k):
        return lax.rem(along + k, n_half)

    def device(x, y, z):
        return {"gx": x, "gy": y, "gz": z}

    barrier = pltpu.get_barrier_semaphore()

    def ready(target):
        pl.semaphore_signal(barrier, inc=1, device_id=target, device_id_type=MESH)

    other_half = 1 - half
    opposite = [n_half * other_half + slot_at(k) for k in (2, 1, 3, 0)]
    early, late = half == 0, half == 1

    everyone = peers + [(0, 0)]
    is_top, is_bottom = gy == n_y - 1, gy == 0

    @pl.when(early)
    def _():
        for k, dx in peers:
            ready(device(columns[dx + 1], gy, slot_at(k)))
        for k, dx in everyone:
            ready(device(columns[dx + 1], gy, n_half + slot_at(k)))

        @pl.when(start)
        def _():
            ready(device(gx, above, jnp.int32(0)))
            ready(device(gx, below, jnp.int32(n_half)))

        @pl.when(end)
        def _():
            ready(device(gx, below, jnp.int32(n_z - 1)))

            @pl.when(jnp.logical_not(is_top))
            def _():
                ready(device(gx, above, jnp.int32(n_z - 1)))

    loads = [
        pltpu.make_async_copy(source, target, load_sem.at[i])
        for i, (source, target) in enumerate(
            [(pos_hbm, pos_ref), (count_hbm, count_ref), (key_hbm, key_ref), (vel_hbm, vel_ref)]
        )
    ]
    for load in loads:
        load.start()
    for load in loads[:2]:
        load.wait()

    lane = lax.broadcasted_iota(jnp.int32, (n_z, SLOTS), 1)
    row = lax.broadcasted_iota(jnp.int32, (n_z, SLOTS), 0)
    occupancy = jnp.zeros((n_z, SLOTS), jnp.int32)
    for z in range(n_z):
        occupancy = jnp.where(row == z, count_ref[z], occupancy)
    px, py, pz = pos_ref[0], pos_ref[1], pos_ref[2]
    cell = cell_of(px) * 9 + cell_of(py) * 3 + cell_of(pz)
    cell = jnp.where(lane < occupancy, cell, 27)
    order = cell * SLOTS + lane
    rank = jnp.zeros((n_z, SLOTS), jnp.int32)
    for m in range(SLOTS):
        rank = rank + jnp.where(order[:, m : m + 1] < order, 1, 0)
    source = jnp.zeros((n_z, SLOTS), jnp.int32)
    for m in range(SLOTS):
        source = jnp.where(rank[:, m : m + 1] == lane, m, source)
    real = lane < occupancy
    for load in loads[2:]:
        load.wait()
    key = key_ref[...]
    fields = [
        jnp.where(real, take(px, source), FAR),
        take(py, source),
        take(pz, source),
        take(vel_ref[0], source),
        take(vel_ref[1], source),
        take(vel_ref[2], source),
        take(lax.shift_right_logical(key, 15).astype(jnp.float32), source),
        take((key & 32767).astype(jnp.float32), source),
    ]
    for f, field in enumerate(fields):
        stage[pl.ds(8 + f, n_z, stride=8), :] = field
        stage[pl.ds(f, 1), :] = field[n_z - 1 : n_z]
        stage[pl.ds(8 * (n_z + 1) + f, 1), :] = field[0:1]

    edge = jnp.logical_or(first, last)
    n_peers = len(peers)

    def copy(source, target, send, recv, to):
        return pltpu.make_async_remote_copy(
            src_ref=source, dst_ref=target, send_sem=send, recv_sem=recv,
            device_id=to, device_id_type=MESH,
        )

    def slab(h):
        return stage.at[pl.ds(pl.multiple_of(8 * n_half * h, 8), 8 * (n_half + 2)), :]

    def tell(target):
        pl.semaphore_signal(plane_sem, inc=1, device_id=target, device_id_type=MESH)

    across = copy(slab(1 - half), mirrored, send_sem.at[0], recv_sem.at[0], device(gx, gy, mirror))

    def send_sums(targets):
        for z in targets:
            copy(
                ranks.at[z], order_ref.at[gz], rank_send.at[0], rank_recv.at[0],
                device(gx, gy, z),
            ).start()

    def to_edge(h, y, position):
        return copy(
            slab(h), edged, send_sem.at[1 + h], recv_sem.at[1], device(gx, y, n_half * h + position)
        )

    @pl.when(late)
    def _():
        from_edges = jnp.where(last, jnp.where(is_bottom, 1, 2), jnp.where(start, 1, 0))
        pl.semaphore_wait(barrier, len(everyone) + from_edges)
        across.start()
        @pl.when(last)
        def _():
            to_edge(0, above, n_half - 1).start()

            @pl.when(is_top)
            def _():
                copy(
                    slab(1), passing, send_sem.at[2], recv_sem.at[3],
                    device(gx, above, n_half - 1),
                ).start()

            @pl.when(jnp.logical_not(is_bottom))
            def _():
                tell(device(gx, below, jnp.int32(n_half - 1)))

        pl.semaphore_signal(
            mirror_sem, inc=1, device_id=device(gx, gy, mirror), device_id_type=MESH
        )
        for k, dx in peers:
            tell(device(columns[dx + 1], gy, slot_at(k)))

        @pl.when(start)
        def _():
            tell(device(gx, above, jnp.int32(0)))

    sorted_key = take(key, source)

    own = as_own(*fields[:6], sorted_key)
    words = as_other(*fields[:6], sorted_key)

    def turned(shift):
        return pair_force(own, [pltpu.roll(word, SLOTS - shift, 1) for word in words])

    def some_turns(step, summed):
        for u in range(TURNS):
            shift = step * TURNS + (u + 1)
            push = turned(shift)
            summed = tuple(
                summed[c] + (push[c] - pltpu.roll(push[c], shift, 1)) for c in range(3)
            )
        return summed

    zero = jnp.zeros((n_z, SLOTS), jnp.float32)
    summed = lax.fori_loop(0, (SLOTS // 2 - 1) // TURNS, some_turns, (zero, zero, zero))
    last_push = turned(SLOTS // 2)
    summed = tuple(summed[c] + last_push[c] for c in range(3))

    left = lane < HALF
    inside = fields[0] < 0.5 * FAR
    top = jnp.logical_and(inside, fields[2] >= 2.0)
    bottom = jnp.logical_and(inside, fields[2] < 1.0)
    member = jnp.where(top, 1, jnp.where(bottom, 2 * SLOTS, 0))
    before = jnp.zeros((n_z, SLOTS), jnp.int32)
    for m in range(SLOTS):
        before = before + jnp.where(lane > m, member[:, m : m + 1], 0)
    low, high = before & (2 * SLOTS - 1), lax.shift_right_logical(before, 8)
    seat = jnp.where(jnp.logical_and(bottom, high < HALF), high + HALF, SLOTS)
    seat = jnp.where(jnp.logical_and(top, low < HALF), low, seat)
    origin = jnp.full((n_z, SLOTS), -1, jnp.int32)
    for m in range(SLOTS):
        origin = jnp.where(seat[:, m : m + 1] == lane, m, origin)
    taken = origin >= 0
    origin = jnp.maximum(origin, 0)

    def from_sides(values):
        return jnp.where(left, pltpu.roll(values, 1, 0), pltpu.roll(values, n_z - 1, 0))

    listed = [take(word, origin) for word in words]
    listed[0] = jnp.where(taken, listed[0], FAR)
    listed = [from_sides(values) for values in listed]
    listed[2] = listed[2] + jnp.where(left, -SIDE, SIDE)
    side_at = jnp.where(fields[2] < 1.5, 0, HALF)

    def some_sides(step, summed):
        for u in range(TURNS_Z):
            index = side_at + (step * TURNS_Z + u)
            push = pair_force(own, [take(values, index) for values in listed])
            summed = tuple(summed[c] + push[c] for c in range(3))
        return summed

    summed = some_sides(0, summed)
    for c in range(3):
        ranks[:, c, :] = summed[c]
    ranks[:, 3, :] = jnp.where(real, rank, rank + SLOTS).astype(jnp.float32)

    @pl.when(early)
    def _():
        pl.semaphore_wait(barrier, jnp.where(first, n_peers + 1, n_peers))

        @pl.when(first)
        def _():
            to_edge(0, below, 0).start()

    @pl.when(late)
    def _():
        send_sums(opposite)
        pl.semaphore_wait(plane_sem, 1)

        @pl.when(jnp.logical_and(last, jnp.logical_not(is_top)))
        def _():
            to_edge(1, above, n_half - 1).start()


    def landing(slot):
        return tiles_ref.at[pl.ds(pl.multiple_of(24 * slot, 8), 24), :]

    def spread(buffer, offset, row_at, sem):
        def block(position):
            at = pl.multiple_of(8 * (offset + position), 8)
            return buffer.at[pl.ds(at, 24), :]

        for k, dx in peers:
            copy(
                block(slot_at(k)), landing((1 - dx) * (n_z + 2) + row_at),
                send_sem.at[sem], recv_sem.at[2],
                device(columns[dx + 1], gy, half * n_half + slot_at(k)),
            ).start()
        pltpu.make_async_copy(
            block(along), landing(n_z + 2 + row_at), recv_sem.at[2]
        ).start()

    spread(stage, half * n_half, gz + 1, 3)
    send_sums([half * n_half + slot_at(k) for k in (2, 1, 3)])
    pltpu.make_async_copy(ranks.at[gz], order_ref.at[gz], rank_recv.at[0]).start()

    @pl.when(early)
    def _():
        pl.semaphore_wait(mirror_sem, 1)
        across.start()

    across.wait_recv()
    spread(mirrored, 0, mirror + 1, 4)

    relay = jnp.logical_or(start, end)

    @pl.when(relay)
    def _():
        copy(
            edged, edged, send_sem.at[1], recv_sem.at[1], device(gx, gy, mirror)
        ).wait_recv()
        spread(edged, 0, jnp.where(start, n_z + 1, 0), 5)

    @pl.when(jnp.logical_and(early, jnp.logical_and(end, is_bottom)))
    def _():
        copy(
            passing, passing, send_sem.at[1], recv_sem.at[3], device(gx, gy, mirror)
        ).wait_recv()
        copy(
            passing, edged, send_sem.at[6], recv_sem.at[1], device(gx, gy, mirror)
        ).start()

    @pl.when(early)
    def _():
        extra = jnp.logical_or(start, jnp.logical_and(end, jnp.logical_not(is_top)))
        pl.semaphore_wait(plane_sem, jnp.where(extra, n_peers + 1, n_peers))
        tell(device(gx, gy, mirror))

        @pl.when(first)
        def _():
            to_edge(1, below, 0).start()

        send_sums(opposite)

    def bulk(count, sem):
        part = tiles_ref.at[pl.ds(0, 24 * count)]
        return copy(part, part, send_sem.at[sem], recv_sem.at[2], device(gx, gy, mirror))

    def bulk_rank(count):
        part = order_ref.at[pl.ds(0, count)]
        return copy(part, part, rank_send.at[0], rank_recv.at[0], device(gx, gy, mirror))

    bulk(3 * (n_z + 2), 3).wait_recv()
    bulk_rank(n_z).wait_recv()
    across.wait_send()
    bulk_rank(n_z - 1).wait_send()
    for sem in (3, 4):
        bulk(n_peers, sem).wait_send()

    @pl.when(relay)
    def _():
        bulk(n_peers, 5).wait_send()

    @pl.when(edge)
    def _():
        for h in (0, 1):
            to_edge(h, gy, 0).wait_send()

    @pl.when(jnp.logical_and(early, jnp.logical_and(end, is_bottom)))
    def _():
        copy(
            passing, edged, send_sem.at[6], recv_sem.at[1], device(gx, gy, mirror)
        ).wait_send()


def exchange(groups, positions, velocities, keys, counts):
    n_z = groups[2]
    anywhere = pl.BlockSpec(memory_space=pl.ANY)
    slab = pltpu.VMEM((8 * (n_z // 2 + 2), SLOTS), jnp.float32)
    return pl.pallas_call(
        functools.partial(exchange_kernel, groups),
        out_shape=[
            pltpu.VMEM((72 * (n_z + 2), SLOTS), jnp.float32),
            pltpu.VMEM((n_z, 4, SLOTS), jnp.float32),
        ],
        in_specs=[anywhere] * 4,
        out_specs=[pl.BlockSpec(memory_space=pltpu.VMEM)] * 2,
        scratch_shapes=[
            pltpu.VMEM((3, n_z, SLOTS), jnp.float32),
            pltpu.VMEM((3, n_z, SLOTS), jnp.float32),
            pltpu.VMEM((n_z, SLOTS), jnp.int32),
            pltpu.SMEM((n_z,), jnp.int32),
            pltpu.VMEM((8 * (n_z + 2), SLOTS), jnp.float32),
            pltpu.VMEM((n_z, 4, SLOTS), jnp.float32),
            slab,
            slab,
            slab,
            pltpu.SemaphoreType.DMA((4,)),
            pltpu.SemaphoreType.DMA((7,)),
            pltpu.SemaphoreType.DMA((4,)),
            pltpu.SemaphoreType.DMA((1,)),
            pltpu.SemaphoreType.DMA((1,)),
            pltpu.SemaphoreType.REGULAR,
            pltpu.SemaphoreType.REGULAR,
        ],
        compiler_params=pltpu.CompilerParams(collective_id=0, has_side_effects=True),
        name="sort_exchange",
    )(positions, velocities, keys, counts)


def runs_of(offset):
    spans = [{-1: (2, 3), 0: (0, 3), 1: (0, 1)}[o] for o in offset]
    runs = []
    for a in range(*spans[0]):
        for b in range(*spans[1]):
            low, high = a * 9 + b * 3 + spans[2][0], a * 9 + b * 3 + spans[2][1]
            if runs and runs[-1][1] == low:
                runs[-1] = (runs[-1][0], high)
            else:
                runs.append((low, high))
    return runs


def force_kernel(rows, tiles_ref, order_ref, out_ref):
    lane = lax.broadcasted_iota(jnp.int32, (rows, SLOTS), 1)
    left_half = lane < HALF

    def load(offset, f):
        ox, oy, oz = offset
        start = (((1 + ox) * (rows + 2) + 1 + oy) * 3 + 1 + oz) * 8 + f
        return tiles_ref[pl.ds(start, rows, stride=24), :]

    def join(high, low):
        return high.astype(jnp.int32) * 32768 + low.astype(jnp.int32)

    def beads(offset):
        return [load(offset, f) for f in range(6)] + [join(load(offset, 6), load(offset, 7))]

    own = as_own(*beads((0, 0, 0)))

    def pair(other, summed):
        push = pair_force(own, other)
        return tuple(summed[c] + push[c] for c in range(3))

    zero = jnp.zeros((rows, SLOTS), jnp.float32)
    summed = tuple(order_ref[:, c, :] for c in range(3))

    def count_cells(cells, low, high):
        inside = jnp.logical_and(cells >= low, cells < high)
        return jnp.sum(jnp.where(inside, 1.0, 0.0), axis=1, keepdims=True).astype(jnp.int32)

    def cells_of(x, y, z):
        cells = cell_of(x) * 9 + cell_of(y) * 3 + cell_of(z)
        return jnp.where(x > 0.5 * FAR, 27, cells)

    def tiles_beside(axis, side):
        ranges = [(0,)] * axis + [(side,)] + [(-1, 0, 1)] * (2 - axis)
        return [(ox, oy, oz) for ox in ranges[0] for oy in ranges[1] for oz in ranges[2]]

    def tables(axis, side):
        tiles = []
        total = jnp.zeros((rows, 1), jnp.int32)
        for offset in tiles_beside(axis, side):
            cells = cells_of(*(load(offset, f) for f in range(3)))
            table = []
            for low, high in runs_of(offset):
                begin = count_cells(cells, 0, low) if low else jnp.zeros_like(total)
                length = count_cells(cells, low, high)
                table.append((total, begin - total))
                total = total + length
            tiles.append((offset, table))
        return tiles, total

    def listed(tiles, total, at):
        alive = at < total
        blank = jnp.zeros_like(lane)
        packed = [jnp.full((rows, SLOTS), FAR, jnp.float32), zero, zero, blank, zero, blank]
        for offset, table in tiles:
            index = at
            for base, shift in table:
                index = jnp.where(at >= base, at + shift, index)
            index = index & (SLOTS - 1)
            taken = jnp.logical_and(alive, at >= table[0][0])
            for f, value in enumerate(as_other(*beads(offset))):
                if f < 3 and offset[f]:
                    value = value + SIDE * offset[f]
                packed[f] = jnp.where(taken, take(value, index), packed[f])
        return packed

    def sweep(jobs, first, last, unroll, summed):
        def some_steps(s, summed):
            for u in range(unroll):
                for axis, lists in jobs:
                    index = side_at[axis] + (s * unroll + u)
                    summed = pair([take(values, index) for values in lists], summed)
            return summed

        if unroll == HALF:
            return some_steps(0, summed)
        return lax.fori_loop(first // unroll, (last + unroll - 1) // unroll, some_steps, summed)

    side_at = [jnp.where(own[axis] < 1.5, 0, HALF) for axis in range(3)]

    def merged(lower, upper, half):
        return [
            jnp.where(left_half, a if half == 0 else pltpu.roll(a, HALF, 1),
                      pltpu.roll(b, HALF, 1) if half == 0 else b)
            for a, b in zip(lower, upper)
        ]

    def along_x_and_y(summed):
        sides = [[tables(axis, side) for side in (-1, 1)] for axis in (0, 1)]
        longest = [jnp.maximum(jnp.max(a[1]), jnp.max(b[1])) for a, b in sides]

        def one_pass(p, summed):
            at = lane + p * SLOTS
            packed = [[listed(tiles, total, at) for tiles, total in pairs] for pairs in sides]
            for half in (0, 1):
                jobs = [(axis, merged(*packed[axis], half)) for axis in (0, 1)]
                steps = [
                    jnp.clip(longest[axis] - p * SLOTS - half * HALF, 0, HALF) for axis in (0, 1)
                ]
                if half == 0:
                    summed = sweep(jobs, 0, HALF, HALF, summed)
                else:
                    both = (jnp.minimum(steps[0], steps[1]) + UNROLL - 1) // UNROLL * UNROLL
                    summed = sweep(jobs, 0, both, UNROLL, summed)
                    for axis in (0, 1):
                        summed = sweep(jobs[axis : axis + 1], both, steps[axis], UNROLL, summed)
            return summed

        passes = (jnp.maximum(longest[0], longest[1]) + SLOTS - 1) // SLOTS
        return lax.fori_loop(0, passes, one_pass, summed)

    def rest_along_z(summed):
        lengths = [
            count_layer(load((0, 0, side), 0), load((0, 0, side), 2), side) for side in (-1, 1)
        ]
        longest = jnp.maximum(jnp.max(lengths[0]), jnp.max(lengths[1]))

        def second_half(_, summed):
            lists = merged(*(listed(*tables(2, side), lane) for side in (-1, 1)), 1)
            return sweep([(2, lists)], 0, longest - HALF, UNROLL, summed)

        return lax.fori_loop(0, jnp.where(longest > HALF, 1, 0), second_half, summed)

    def count_layer(x, z, side):
        inside = jnp.logical_and(x < 0.5 * FAR, z >= 2.0 if side < 0 else z < 1.0)
        return jnp.sum(jnp.where(inside, 1.0, 0.0), axis=1, keepdims=True).astype(jnp.int32)

    summed = along_x_and_y(summed)
    summed = rest_along_z(summed)

    order = order_ref[:, 3, :].astype(jnp.int32)
    scale = jnp.where(order < SLOTS, kick_scale, 0.0)
    order = order & (SLOTS - 1)
    for c in range(3):
        out_ref[c] = scale * take(summed[c], order)


def forces(n_z, tiles, order):
    vmem = pl.BlockSpec(memory_space=pltpu.VMEM)
    return pl.pallas_call(
        functools.partial(force_kernel, n_z),
        out_shape=jax.ShapeDtypeStruct((3, n_z, SLOTS), jnp.float32),
        in_specs=[vmem, vmem],
        out_specs=vmem,
        name="pair_forces",
    )(*(pltpu.with_memory_space_constraint(x, pltpu.VMEM) for x in (tiles, order)))


def solution(mesh):
    groups = tuple(mesh.shape[a] for a in ("gx", "gy", "gz"))
    n_z = groups[2]

    def on_device(positions, velocities, bead_keys, counts):
        tiles, order = exchange(
            groups,
            positions.reshape(3, n_z, SLOTS),
            velocities.reshape(3, n_z, SLOTS),
            bead_keys.reshape(n_z, SLOTS),
            counts.reshape(n_z),
        )
        kick = forces(n_z, tiles, order)
        return kick.reshape(3, 1, n_z, 1, SLOTS)

    in_specs = (
        P(None, "gx", ("gy", "gz"), None, None),
        P(None, "gx", ("gy", "gz"), None, None),
        P("gx", ("gy", "gz"), None, None),
        P("gx", ("gy", "gz"), None),
    )
    out_specs = P(None, "gx", "gy", "gz", None)
    return jax.shard_map(
        on_device, mesh=mesh, in_specs=in_specs, out_specs=out_specs, check_vma=False
    )
```
